256 devices in a mesh: dp: 8 (over z), replica: 4 (over y), fsdp: 8 (over x, core).
Axes of the slice: x: 4, y: 4, z: 8, core: 2. Of those that a mesh axis runs over, the one named last changes fastest.
Arguments:
- x_tokens: bfloat16 [32768, 1024], P(('dp', 'replica', 'fsdp'))
- dy_tokens: bfloat16 [32768, 1024], P(('dp', 'replica', 'fsdp'))
- w_gate: bfloat16 [3, 1024, 4096], P(None, 'fsdp')
- w_up: bfloat16 [3, 1024, 4096], P(None, 'fsdp')
- w_down: bfloat16 [3, 4096, 1024], P(None, 'fsdp')
- norm_gain: float32 [3, 1024], replicated
Outputs:
- output 1: bfloat16 [32768, 1024], P(('dp', 'replica', 'fsdp'))
- output 2: float32 [3, 1024, 4096], P(None, 'fsdp')
- output 3: float32 [3, 1024, 4096], P(None, 'fsdp')
- output 4: float32 [3, 4096, 1024], P(None, 'fsdp')
- output 5: float32 [3, 1024], replicated
All inputs are finite; a program needn't handle non-finite values.
Results may differ from the reference program's by a relative error of at most 0.02.
Values are sent between devices in bfloat16 or wider.
A program may use at most 768 MiB of HBM per device.

```python
import jax
import jax.numpy as jnp
from jax import lax

D = 1024
FF = 4096
LAYERS = 3
BLOCK_TOK = 128
N_BLOCKS = 256
NORM_EPS = 1e-6
TOKENS = BLOCK_TOK * N_BLOCKS


def setup_inputs(seed: int = 0) -> dict:
    root_key = jax.random.key(seed)
    subkeys = jax.random.split(root_key, 6)
    in_scale = D ** -0.5
    inner_scale = FF ** -0.5
    x_tokens = jax.random.normal(subkeys[0], (TOKENS, D), jnp.float32).astype(jnp.bfloat16)
    dy_tokens = jax.random.normal(subkeys[1], (TOKENS, D), jnp.float32).astype(jnp.bfloat16)
    w_gate = (jax.random.normal(subkeys[2], (LAYERS, D, FF), jnp.float32) * in_scale).astype(jnp.bfloat16)
    w_up = (jax.random.normal(subkeys[3], (LAYERS, D, FF), jnp.float32) * in_scale).astype(jnp.bfloat16)
    w_down = (jax.random.normal(subkeys[4], (LAYERS, FF, D), jnp.float32) * inner_scale).astype(jnp.bfloat16)
    norm_gain = jax.random.uniform(subkeys[5], (LAYERS, D), jnp.float32, 0.5, 1.5)
    return {"x_tokens": x_tokens, "dy_tokens": dy_tokens, "w_gate": w_gate, "w_up": w_up, "w_down": w_down, "norm_gain": norm_gain}


def snap_bf16(values):
    return values.astype(jnp.bfloat16).astype(jnp.float32)


def layer_apply(hidden, layer_params):
    w_gate, w_up, w_down, gain_row = layer_params
    inv_rms = lax.rsqrt(jnp.mean(hidden * hidden, axis=-1, keepdims=True) + NORM_EPS)
    normed = snap_bf16(hidden * inv_rms * gain_row)
    gate_act = snap_bf16(jnp.dot(normed, w_gate, preferred_element_type=jnp.float32))
    up_act = snap_bf16(jnp.dot(normed, w_up, preferred_element_type=jnp.float32))
    prod_act = snap_bf16(jax.nn.silu(gate_act) * up_act)
    layer_out = snap_bf16(hidden + jnp.dot(prod_act, w_down, preferred_element_type=jnp.float32))
    return layer_out, None


def stack_apply(params, x_block):
    return lax.scan(layer_apply, x_block, params)[0]


def reference(x_tokens, dy_tokens, w_gate, w_up, w_down, norm_gain):
    params = (w_gate.astype(jnp.float32), w_up.astype(jnp.float32), w_down.astype(jnp.float32), norm_gain)
    x_blocks = x_tokens.reshape(N_BLOCKS, BLOCK_TOK, D)
    dy_blocks = dy_tokens.reshape(N_BLOCKS, BLOCK_TOK, D)

    def block_step(grad_sum, block_pair):
        x_block = block_pair[0].astype(jnp.float32)
        dy_block = block_pair[1].astype(jnp.float32)
        y_block, pull_back = jax.vjp(lambda weights: stack_apply(weights, x_block), params)
        block_grads = pull_back(dy_block)[0]
        return jax.tree.map(jnp.add, grad_sum, block_grads), y_block.astype(jnp.bfloat16)

    grad_zero = jax.tree.map(jnp.zeros_like, params)
    grad_sum, y_blocks = lax.scan(block_step, grad_zero, (x_blocks, dy_blocks))
    y_tokens = y_blocks.reshape(TOKENS, D)
    return (y_tokens, grad_sum[0], grad_sum[1], grad_sum[2], grad_sum[3])
```

```python
import functools
import jax
import jax.numpy as jnp
from jax import lax
from jax.sharding import PartitionSpec as P
from jax.experimental import pallas as pl
from jax.experimental.pallas import tpu as pltpu

F32 = jnp.float32
BF16 = jnp.bfloat16
MESH = pl.DeviceIdType.MESH
RS = 16
LN = 128


def wrap(value, size):
    return lax.rem(value + 4 * size, size)


def split_units(units):
    a = (units * 7 + 12) // 24
    b = (units - 2 * a) // 2
    sizes = (a, a, b, units - 2 * a - b)
    starts = (0, a, 2 * a, 2 * a + b)
    return tuple(zip(starts, sizes))


class Hop:
    def __init__(self, axis, size, pos, sign, chunk, stage, send, recv, base, layers):
        self.axis, self.size, self.pos, self.sign = axis, size, pos, sign
        self.chunk, self.stage, self.send_sem, self.recv_sem = chunk, stage, send, recv
        self.base, self.layers = base, layers

    def copy(self, step, layer, index, dst):
        slot = self.base + step * self.layers + layer
        return pltpu.make_async_remote_copy(
            src_ref=self.chunk(layer, index), dst_ref=dst,
            send_sem=self.send_sem.at[slot], recv_sem=self.recv_sem.at[slot],
            device_id={self.axis: wrap(self.pos + self.sign, self.size)}, device_id_type=MESH)

    def rs_copy(self, step, layer):
        return self.copy(step, layer, wrap(self.pos - self.sign * (step + 1), self.size), self.stage(step, layer))

    def rs_add(self, step, layer):
        self.rs_copy(step, layer).wait_recv()
        dst = self.chunk(layer, wrap(self.pos - self.sign * (step + 2), self.size))
        src = self.stage(step, layer)
        if len(dst.shape) == 4:
            def body(i, carry):
                dst[i] += src[i]
                return carry
            lax.fori_loop(0, dst.shape[0], body, 0)
        else:
            dst[...] += src[...]

    def ag_copy(self, step, layer):
        index = wrap(self.pos - self.sign * step, self.size)
        return self.copy(step, layer, index, self.chunk(layer, index))

    def ag_wait(self, step, layer):
        index = wrap(self.pos - self.sign * (step + 1), self.size)
        self.copy(step, layer, index, self.chunk(layer, index)).wait_recv()
        return self.chunk(layer, index)


def ar_kernel(dims, *refs):
    layers, ny, nz, nf = dims
    units = 3 * nf
    grads = refs[:3 * layers]
    gain_ref = refs[3 * layers]
    out_ref, gain_out = refs[3 * layers + 1:3 * layers + 3]
    (G, st_ay, st_bz, st_az, st_by, R, gain_buf, rs_send, rs_recv, ag_send, ag_recv,
     x_send, x_recv, g_send, g_recv, in_sem, out_sem, ready) = refs[3 * layers + 3:]
    y, z, f = lax.axis_index("replica"), lax.axis_index("dp"), lax.axis_index("fsdp")

    barrier = pltpu.get_barrier_semaphore()
    peers = [("fsdp", f, nf), ("replica", y, ny), ("dp", z, nz)]
    count = 0
    for axis, pos, size in peers:
        for j in range(1, size):
            pl.semaphore_signal(barrier, inc=1, device_id={axis: wrap(pos + j, size)}, device_id_type=MESH)
            count += 1

    def load(i, carry):
        yy, zz = i // nz, i % nz
        for layer in range(layers):
            for m in range(2):
                src = grads[3 * layer + m].at[:, zz, :, pl.ds(pl.multiple_of(yy * LN, LN), LN)]
                pltpu.make_async_copy(src, G.at[layer, yy, zz, pl.ds(m * nf, nf)], in_sem).start()
            for h in range(2):
                src = grads[3 * layer + 2].at[zz, :, :, pl.ds(pl.multiple_of((2 * yy + h) * LN, LN), LN)]
                pltpu.make_async_copy(src, G.at[layer, yy, zz, pl.ds(2 * nf + h * (nf // 2), nf // 2)], in_sem).start()
        return carry
    lax.fori_loop(0, ny * nz, load, 0)
    pl.semaphore_wait(barrier, count)
    pltpu.make_async_copy(out_ref, G, in_sem).wait()

    streams = split_units(units)
    hops, base = [], 0
    for phase in range(2):
        row = []
        for k, (start, size) in enumerate(streams):
            sign = 1 if k % 2 == 0 else -1
            first_y = k < 2
            along_y = first_y == (phase == 0)
            sub = pl.ds(start, size)
            if along_y:
                chunk = (lambda sub: lambda layer, i: G.at[layer, i, :, sub])(sub) if phase == 0 else (lambda sub: lambda layer, i: G.at[layer, i, z, sub])(sub)
            else:
                chunk = (lambda sub: lambda layer, i: G.at[layer, :, i, sub])(sub) if phase == 0 else (lambda sub: lambda layer, i: G.at[layer, y, i, sub])(sub)
            buf = ((st_ay, st_bz) if phase == 0 else (st_az, st_by))[0 if first_y else 1]
            stage = (lambda buf, d, size: lambda step, layer: buf.at[d, step, layer, :, pl.ds(0, size)] if len(buf.shape) == 7 else buf.at[d, step, layer, pl.ds(0, size)])(buf, k % 2, size)
            axis, n, pos = ("replica", ny, y) if along_y else ("dp", nz, z)
            row.append(Hop(axis, n, pos, sign, chunk, stage, rs_send, rs_recv, base, layers))
            base += (n - 1) * layers
        hops.append(row)

    def gain_copy(stage, axis, pos, size, j):
        return pltpu.make_async_remote_copy(
            src_ref=gain_buf.at[stage, pos], dst_ref=gain_buf.at[stage, pos],
            send_sem=g_send.at[stage, j], recv_sem=g_recv.at[stage, pos],
            device_id={axis: wrap(pos + j, size)}, device_id_type=MESH)

    def gain_send(stage, value):
        axis, pos, size = peers[stage]
        gain_buf[stage, pos] = value
        for j in range(1, size):
            gain_copy(stage, axis, pos, size, j).start()

    def gain_sum(stage):
        axis, pos, size = peers[stage]
        for j in range(1, size):
            other = wrap(pos + j, size)
            pltpu.make_async_remote_copy(
                src_ref=gain_buf.at[stage, other], dst_ref=gain_buf.at[stage, other],
                send_sem=g_send.at[stage, j], recv_sem=g_recv.at[stage, other],
                device_id={axis: other}, device_id_type=MESH).wait_recv()
        total = gain_buf[stage, 0]
        for i in range(1, size):
            total = total + gain_buf[stage, i]
        return total

    gain_send(0, gain_ref[...])

    def steps(rows, link_us, reduce):
        events = []
        for k, hop in enumerate(rows):
            for step in range(hop.size - 1):
                for layer in range(layers):
                    events.append(((step * layers + layer + 1) * link_us[k], k, step, layer))
        return sorted(events)

    big = [1.4 * ny * 0 + streams[k][1] * (nz if k < 2 else ny) for k in range(4)]
    small = [max(streams[k][1], 8) for k in range(4)]

    for hop in hops[0]:
        for layer in range(layers):
            hop.rs_copy(0, layer).start()
    for phase in range(2):
        order = steps(hops[phase], big if phase == 0 else small, True)
        for n, (_, k, step, layer) in enumerate(order):
            hop = hops[phase][k]
            hop.rs_add(step, layer)
            if step + 1 < hop.size - 1:
                hop.rs_copy(step + 1, layer).start()
            elif phase == 0:
                hops[1][k].rs_copy(0, layer).start()
            if phase == 0 and n == len(order) // 3:
                gain_send(1, gain_sum(0))
            if phase == 0 and n == 2 * len(order) // 3:
                gain_send(2, gain_sum(1))

    def x_copy(m, j, peer, sender):
        return pltpu.make_async_remote_copy(
            src_ref=G.at[:, y, z, m * nf + peer], dst_ref=R.at[:, m * nf + sender],
            send_sem=x_send.at[m, j], recv_sem=x_recv.at[m, sender],
            device_id={"fsdp": peer}, device_id_type=MESH)

    for j in range(1, nf):
        for m in range(2):
            x_copy(m, j, wrap(f + j, nf), f).start()
    for m in range(2):
        R[:, m * nf + f] = G[:, y, z, m * nf + f]
    gain_out[...] = gain_sum(2)
    for phase in range(2):
        for hop in hops[phase]:
            for step in range(hop.size - 1):
                for layer in range(layers):
                    hop.rs_copy(step, layer).wait_send()
    for axis, pos, size in peers[1:]:
        for sign in (1, -1):
            pl.semaphore_signal(ready, inc=1, device_id={axis: wrap(pos + sign, size)}, device_id_type=MESH)
    for j in range(1, nf):
        for m in range(2):
            x_copy(m, j, wrap(f + j, nf), f).wait_send()
            x_copy(m, j, wrap(f + j, nf), wrap(f + j, nf)).wait_recv()
    G[:, y, z, pl.ds(0, 2 * nf)] = R[...]
    pl.semaphore_wait(ready, 4)

    for row in hops:
        for hop in row:
            hop.send_sem, hop.recv_sem = ag_send, ag_recv

    pltpu.make_async_copy(G.at[:, y, z], out_ref.at[:, y, z], out_sem).start()

    def emit(hop, step, layer, k, phase):
        index = wrap(hop.pos - hop.sign * (step + 1), hop.size)
        sub = pl.ds(*streams[k])
        if phase == 0:
            dst = out_ref.at[layer, index, :, sub] if k < 2 else out_ref.at[layer, :, index, sub]
        else:
            dst = out_ref.at[layer, y, index, sub] if k < 2 else out_ref.at[layer, index, z, sub]
        pltpu.make_async_copy(hop.chunk(layer, index), dst, out_sem).start()

    for hop in hops[1]:
        for layer in range(layers):
            hop.ag_copy(0, layer).start()
    for phase in (1, 0):
        order = steps(hops[phase], big if phase == 0 else small, False)
        for _, k, step, layer in order:
            hop = hops[phase][k]
            hop.ag_wait(step, layer)
            if step + 1 < hop.size - 1:
                hop.ag_copy(step + 1, layer).start()
            elif phase == 1:
                hops[0][k].ag_copy(0, layer).start()
            emit(hop, step, layer, k, phase)
    for phase in range(2):
        for hop in hops[phase]:
            for step in range(hop.size - 1):
                for layer in range(layers):
                    hop.ag_copy(step, layer).wait_send()
    for stage, (axis, pos, size) in enumerate(peers):
        for j in range(1, size):
            gain_copy(stage, axis, pos, size, j).wait_send()
    pltpu.make_async_copy(G, out_ref, out_sem).wait()


def all_reduce(grads, gain, dims):
    layers, ny, nz, nf = dims
    units = 3 * nf
    streams = split_units(units)
    a, b = streams[0][1], max(streams[2][1], streams[3][1])
    copies = layers * 2 * 2 * ((ny - 1) + (nz - 1))
    views = []
    for i, g in enumerate(grads):
        if i % 3 < 2:
            views.append(g.reshape(nf, nz, RS, ny * LN))
        else:
            views.append(g.reshape(nz, nf // 2, RS, 2 * ny * LN))
    gr = gain.reshape(-1, LN)
    out, gain_out = pl.pallas_call(
        functools.partial(ar_kernel, dims),
        out_shape=(jax.ShapeDtypeStruct((layers, ny, nz, units, RS, LN), F32), jax.ShapeDtypeStruct(gr.shape, F32)),
        in_specs=[pl.BlockSpec(memory_space=pl.ANY)] * len(views) + [pl.BlockSpec(memory_space=pltpu.VMEM)],
        out_specs=(pl.BlockSpec(memory_space=pl.ANY), pl.BlockSpec(memory_space=pltpu.VMEM)),
        scratch_shapes=[
            pltpu.VMEM((layers, ny, nz, units, RS, LN), F32),
            pltpu.VMEM((2, ny - 1, layers, nz, a, RS, LN), F32),
            pltpu.VMEM((2, nz - 1, layers, ny, b, RS, LN), F32),
            pltpu.VMEM((2, nz - 1, layers, a, RS, LN), F32),
            pltpu.VMEM((2, ny - 1, layers, b, RS, LN), F32),
            pltpu.VMEM((layers, 2 * nf, RS, LN), F32),
            pltpu.VMEM((3, max(nf, ny, nz)) + gr.shape, F32),
            pltpu.SemaphoreType.DMA((copies,)), pltpu.SemaphoreType.DMA((copies,)),
            pltpu.SemaphoreType.DMA((copies,)), pltpu.SemaphoreType.DMA((copies,)),
            pltpu.SemaphoreType.DMA((2, nf)), pltpu.SemaphoreType.DMA((2, nf)),
            pltpu.SemaphoreType.DMA((3, max(nf, ny, nz))), pltpu.SemaphoreType.DMA((3, max(nf, ny, nz))),
            pltpu.SemaphoreType.DMA, pltpu.SemaphoreType.DMA, pltpu.SemaphoreType.REGULAR,
        ],
        compiler_params=pltpu.CompilerParams(collective_id=0, has_side_effects=True, vmem_limit_bytes=52 * 2**20),
        name="grad_all_reduce",
    )(*views, gr)
    return out, gain_out


def unpack_kernel(g_ref, o_ref):
    ny, nf = g_ref.shape[0], g_ref.shape[1]
    for j in range(nf):
        for i in range(ny):
            o_ref[:, (j * ny + i) * LN:(j * ny + i + 1) * LN] = g_ref[i, j]


def unpack_down_kernel(g_ref, o_ref):
    ny, nf = g_ref.shape[0], g_ref.shape[1]
    for i in range(ny):
        for h in range(2):
            for r in range(nf // 2):
                o_ref[r * RS:(r + 1) * RS, (2 * i + h) * LN:(2 * i + h + 1) * LN] = g_ref[i, h * (nf // 2) + r]


def unpack(out, dims):
    layers, ny, nz, nf = dims
    res = []
    for m in range(3):
        spec_in = pl.BlockSpec((None, ny, None, nf, RS, LN), functools.partial(lambda m, l, z: (l, 0, z, m, 0, 0), m))
        if m < 2:
            shape, block, body = (layers, nz * RS, nf * ny * LN), (None, RS, nf * ny * LN), unpack_kernel
        else:
            shape, block, body = (layers, nz * (nf // 2) * RS, 2 * ny * LN), (None, (nf // 2) * RS, 2 * ny * LN), unpack_down_kernel
        res.append(pl.pallas_call(
            body, grid=(layers, nz), in_specs=[spec_in],
            out_specs=pl.BlockSpec(block, lambda l, z: (l, z, 0)),
            out_shape=jax.ShapeDtypeStruct(shape, F32), name="unpack_%d" % m)(out))
    return res


NORM_EPS = 1e-6
TOKEN_AXES = ("dp", "replica", "fsdp")
CONTRACT_ROWS = (((0,), (0,)), ((), ()))
CONTRACT_COLS = (((1,), (1,)), ((), ()))


def dot(a, b, dims=(((1,), (0,)), ((), ()))):
    return lax.dot_general(a, b, dims, preferred_element_type=F32)


def solution(mesh):
    shards = mesh.shape["fsdp"]
    tok_spec = P(TOKEN_AXES, None)
    shard_spec = P(None, "fsdp", None)
    full_spec = P(None, None)

    def to_columns(w_rows):
        layers, rows, cols = w_rows.shape
        split = w_rows.reshape(layers, rows, shards, cols // shards)
        moved = lax.all_to_all(split, "fsdp", split_axis=2, concat_axis=1, tiled=True)
        return moved.reshape(layers, rows * shards, cols // shards)

    def device_step(x_local, dy_local, w_gate_sh, w_up_sh, w_down_sh, norm_gain):
        layers = w_gate_sh.shape[0]
        both = to_columns(jnp.concatenate([w_gate_sh, w_up_sh], axis=0))
        w_gate, w_up, w_down = both[:layers], both[layers:], w_down_sh
        hidden = x_local
        saved = []
        for layer in range(layers):
            hidden_f = hidden.astype(F32)
            inv_rms = lax.rsqrt(jnp.mean(hidden_f * hidden_f, axis=-1, keepdims=True) + NORM_EPS)
            normed = (hidden_f * inv_rms * norm_gain[layer]).astype(BF16)
            normed = lax.all_gather(normed, "fsdp", axis=0, tiled=True)
            gate = dot(normed, w_gate[layer]).astype(BF16)
            up = dot(normed, w_up[layer]).astype(BF16)
            prod = (jax.nn.silu(gate.astype(F32)) * up.astype(F32)).astype(BF16)
            out = lax.psum_scatter(dot(prod, w_down[layer]), "fsdp", scatter_dimension=0, tiled=True)
            saved.append((hidden_f, inv_rms, normed, gate, up, prod))
            hidden = (hidden_f + out).astype(BF16)
        cot = dy_local
        grads = [None] * layers
        for layer in reversed(range(layers)):
            hidden_f, inv_rms, normed, gate, up, prod = saved[layer]
            cot_all = lax.all_gather(cot, "fsdp", axis=0, tiled=True)
            d_prod = dot(cot_all, w_down[layer], CONTRACT_COLS).astype(BF16).astype(F32)
            gate_f = gate.astype(F32)
            sig = jax.nn.sigmoid(gate_f)
            d_gate = (d_prod * up.astype(F32) * sig * (1.0 + gate_f * (1.0 - sig))).astype(BF16)
            d_up = (d_prod * gate_f * sig).astype(BF16)
            part = dot(d_gate, w_gate[layer], CONTRACT_COLS) + dot(d_up, w_up[layer], CONTRACT_COLS)
            d_normed = lax.psum_scatter(part, "fsdp", scatter_dimension=0, tiled=True).astype(BF16).astype(F32)
            d_gain = jnp.sum(d_normed * hidden_f * inv_rms, axis=0)
            scaled = d_normed * norm_gain[layer]
            d_hidden = cot.astype(F32) + inv_rms * scaled - hidden_f * (inv_rms * inv_rms * inv_rms) * jnp.mean(scaled * hidden_f, axis=-1, keepdims=True)
            cot = d_hidden.astype(BF16)
            grads[layer] = (
                dot(normed, d_gate, CONTRACT_ROWS),
                dot(normed, d_up, CONTRACT_ROWS),
                dot(prod, cot_all, CONTRACT_ROWS),
                d_gain,
            )
        flat = [grads[layer][part] for layer in range(layers) for part in range(3)]
        gain = jnp.stack([grads[layer][3] for layer in range(layers)])
        dims = (layers, mesh.shape["replica"], mesh.shape["dp"], shards)
        blocks, gain_sum = all_reduce(flat, gain, dims)
        dw_gate, dw_up, dw_down = unpack(blocks, dims)
        return (hidden, dw_gate, dw_up, dw_down, gain_sum.reshape(gain.shape))

    return jax.shard_map(device_step, mesh=mesh, in_specs=(tok_spec, tok_spec, shard_spec, shard_spec, shard_spec, full_spec), out_specs=(tok_spec, shard_spec, shard_spec, shard_spec, full_spec), check_vma=False)
```

```python
import functools
import jax
import jax.numpy as jnp
from jax import lax
from jax.sharding import PartitionSpec as P
from jax.experimental import pallas as pl
from jax.experimental.pallas import tpu as pltpu

F32 = jnp.float32
BF16 = jnp.bfloat16
MESH = pl.DeviceIdType.MESH
RS = 16
LN = 128


def wrap(value, size):
    return lax.rem(value + 4 * size, size)


def split_units(units):
    a = (units * 7 + 12) // 24
    b = (units - 2 * a) // 2
    sizes = (a, a, b, units - 2 * a - b)
    starts = (0, a, 2 * a, 2 * a + b)
    return tuple(zip(starts, sizes))


class Hop:
    def __init__(self, axis, size, pos, sign, chunk, stage, send, recv, base, layers):
        self.axis, self.size, self.pos, self.sign = axis, size, pos, sign
        self.chunk, self.stage, self.send_sem, self.recv_sem = chunk, stage, send, recv
        self.base, self.layers = base, layers

    def copy(self, step, layer, index, dst):
        slot = self.base + step * self.layers + layer
        return pltpu.make_async_remote_copy(
            src_ref=self.chunk(layer, index), dst_ref=dst,
            send_sem=self.send_sem.at[slot], recv_sem=self.recv_sem.at[slot],
            device_id={self.axis: wrap(self.pos + self.sign, self.size)}, device_id_type=MESH)

    def rs_copy(self, step, layer):
        return self.copy(step, layer, wrap(self.pos - self.sign * (step + 1), self.size), self.stage(step, layer))

    def rs_add(self, step, layer):
        self.rs_copy(step, layer).wait_recv()
        dst = self.chunk(layer, wrap(self.pos - self.sign * (step + 2), self.size))
        src = self.stage(step, layer)
        if len(dst.shape) == 4:
            def body(i, carry):
                dst[i] += src[i]
                return carry
            lax.fori_loop(0, dst.shape[0], body, 0)
        else:
            dst[...] += src[...]

    def ag_copy(self, step, layer):
        index = wrap(self.pos - self.sign * step, self.size)
        return self.copy(step, layer, index, self.chunk(layer, index))

    def ag_wait(self, step, layer):
        index = wrap(self.pos - self.sign * (step + 1), self.size)
        self.copy(step, layer, index, self.chunk(layer, index)).wait_recv()
        return self.chunk(layer, index)


def ar_kernel(dims, *refs):
    layers, ny, nz, nf = dims
    units = 3 * nf
    grad_ref, gain_ref, out_ref, gain_out = refs[:4]
    (G, st_ay, st_bz, st_az, st_by, R, gain_buf, rs_send, rs_recv, ag_send, ag_recv,
     x_send, x_recv, g_send, g_recv, in_sem, out_sem, ready) = refs[4:]
    y, z, f = lax.axis_index("replica"), lax.axis_index("dp"), lax.axis_index("fsdp")

    barrier = pltpu.get_barrier_semaphore()
    peers = [("fsdp", f, nf), ("replica", y, ny), ("dp", z, nz)]
    count = 0
    for axis, pos, size in peers:
        for j in range(1, size):
            pl.semaphore_signal(barrier, inc=1, device_id={axis: wrap(pos + j, size)}, device_id_type=MESH)
            count += 1

    load = pltpu.make_async_copy(grad_ref, G, in_sem)
    load.start()
    pl.semaphore_wait(barrier, count)
    load.wait()

    streams = split_units(units)
    hops, base = [], 0
    for phase in range(2):
        row = []
        for k, (start, size) in enumerate(streams):
            sign = 1 if k % 2 == 0 else -1
            first_y = k < 2
            along_y = first_y == (phase == 0)
            sub = pl.ds(start, size)
            if along_y:
                chunk = (lambda sub: lambda layer, i: G.at[layer, i, :, sub])(sub) if phase == 0 else (lambda sub: lambda layer, i: G.at[layer, i, z, sub])(sub)
            else:
                chunk = (lambda sub: lambda layer, i: G.at[layer, :, i, sub])(sub) if phase == 0 else (lambda sub: lambda layer, i: G.at[layer, y, i, sub])(sub)
            buf = ((st_ay, st_bz) if phase == 0 else (st_az, st_by))[0 if first_y else 1]
            stage = (lambda buf, d, size: lambda step, layer: buf.at[d, step, layer, :, pl.ds(0, size)] if len(buf.shape) == 7 else buf.at[d, step, layer, pl.ds(0, size)])(buf, k % 2, size)
            axis, n, pos = ("replica", ny, y) if along_y else ("dp", nz, z)
            row.append(Hop(axis, n, pos, sign, chunk, stage, rs_send, rs_recv, base, layers))
            base += (n - 1) * layers
        hops.append(row)

    def gain_copy(stage, axis, pos, size, j):
        return pltpu.make_async_remote_copy(
            src_ref=gain_buf.at[stage, pos], dst_ref=gain_buf.at[stage, pos],
            send_sem=g_send.at[stage, j], recv_sem=g_recv.at[stage, pos],
            device_id={axis: wrap(pos + j, size)}, device_id_type=MESH)

    def gain_send(stage, value):
        axis, pos, size = peers[stage]
        gain_buf[stage, pos] = value
        for j in range(1, size):
            gain_copy(stage, axis, pos, size, j).start()

    def gain_sum(stage):
        axis, pos, size = peers[stage]
        for j in range(1, size):
            other = wrap(pos + j, size)
            pltpu.make_async_remote_copy(
                src_ref=gain_buf.at[stage, other], dst_ref=gain_buf.at[stage, other],
                send_sem=g_send.at[stage, j], recv_sem=g_recv.at[stage, other],
                device_id={axis: other}, device_id_type=MESH).wait_recv()
        total = gain_buf[stage, 0]
        for i in range(1, size):
            total = total + gain_buf[stage, i]
        return total

    gain_send(0, gain_ref[...])

    def steps(rows, link_us, reduce):
        events = []
        for k, hop in enumerate(rows):
            for step in range(hop.size - 1):
                for layer in range(layers):
                    events.append(((step * layers + layer + 1) * link_us[k], k, step, layer))
        return sorted(events)

    big = [1.4 * ny * 0 + streams[k][1] * (nz if k < 2 else ny) for k in range(4)]
    small = [max(streams[k][1], 8) for k in range(4)]

    for hop in hops[0]:
        for layer in range(layers):
            hop.rs_copy(0, layer).start()
    for phase in range(2):
        order = steps(hops[phase], big if phase == 0 else small, True)
        for n, (_, k, step, layer) in enumerate(order):
            hop = hops[phase][k]
            hop.rs_add(step, layer)
            if step + 1 < hop.size - 1:
                hop.rs_copy(step + 1, layer).start()
            elif phase == 0:
                hops[1][k].rs_copy(0, layer).start()
            if phase == 0 and n == len(order) // 3:
                gain_send(1, gain_sum(0))
            if phase == 0 and n == 2 * len(order) // 3:
                gain_send(2, gain_sum(1))

    def x_copy(m, j, peer, sender):
        return pltpu.make_async_remote_copy(
            src_ref=G.at[:, y, z, m * nf + peer], dst_ref=R.at[:, m * nf + sender],
            send_sem=x_send.at[m, j], recv_sem=x_recv.at[m, sender],
            device_id={"fsdp": peer}, device_id_type=MESH)

    for j in range(1, nf):
        for m in range(2):
            x_copy(m, j, wrap(f + j, nf), f).start()
    for m in range(2):
        R[:, m * nf + f] = G[:, y, z, m * nf + f]
    gain_out[...] = gain_sum(2)
    for phase in range(2):
        for hop in hops[phase]:
            for step in range(hop.size - 1):
                for layer in range(layers):
                    hop.rs_copy(step, layer).wait_send()
    for axis, pos, size in peers[1:]:
        for sign in (1, -1):
            pl.semaphore_signal(ready, inc=1, device_id={axis: wrap(pos + sign, size)}, device_id_type=MESH)
    for j in range(1, nf):
        for m in range(2):
            x_copy(m, j, wrap(f + j, nf), f).wait_send()
            x_copy(m, j, wrap(f + j, nf), wrap(f + j, nf)).wait_recv()
    G[:, y, z, pl.ds(0, 2 * nf)] = R[...]
    pl.semaphore_wait(ready, 4)

    for row in hops:
        for hop in row:
            hop.send_sem, hop.recv_sem = ag_send, ag_recv

    pltpu.make_async_copy(G.at[:, y, z], out_ref.at[:, y, z], out_sem).start()

    def emit(hop, step, layer, k, phase):
        index = wrap(hop.pos - hop.sign * (step + 1), hop.size)
        sub = pl.ds(*streams[k])
        if phase == 0:
            dst = out_ref.at[layer, index, :, sub] if k < 2 else out_ref.at[layer, :, index, sub]
        else:
            dst = out_ref.at[layer, y, index, sub] if k < 2 else out_ref.at[layer, index, z, sub]
        pltpu.make_async_copy(hop.chunk(layer, index), dst, out_sem).start()

    for hop in hops[1]:
        for layer in range(layers):
            hop.ag_copy(0, layer).start()
    for phase in (1, 0):
        order = steps(hops[phase], big if phase == 0 else small, False)
        for _, k, step, layer in order:
            hop = hops[phase][k]
            hop.ag_wait(step, layer)
            if step + 1 < hop.size - 1:
                hop.ag_copy(step + 1, layer).start()
            elif phase == 1:
                hops[0][k].ag_copy(0, layer).start()
            emit(hop, step, layer, k, phase)
    for phase in range(2):
        for hop in hops[phase]:
            for step in range(hop.size - 1):
                for layer in range(layers):
                    hop.ag_copy(step, layer).wait_send()
    for stage, (axis, pos, size) in enumerate(peers):
        for j in range(1, size):
            gain_copy(stage, axis, pos, size, j).wait_send()
    pltpu.make_async_copy(G, out_ref, out_sem).wait()


def all_reduce(grads, gain, dims):
    layers, ny, nz, nf = dims
    units = 3 * nf
    streams = split_units(units)
    a, b = streams[0][1], max(streams[2][1], streams[3][1])
    copies = layers * 2 * 2 * ((ny - 1) + (nz - 1))
    gr = gain.reshape(-1, LN)
    out, gain_out = pl.pallas_call(
        functools.partial(ar_kernel, dims),
        out_shape=(jax.ShapeDtypeStruct((layers, ny, nz, units, RS, LN), F32), jax.ShapeDtypeStruct(gr.shape, F32)),
        in_specs=[pl.BlockSpec(memory_space=pl.ANY), pl.BlockSpec(memory_space=pltpu.VMEM)],
        out_specs=(pl.BlockSpec(memory_space=pl.ANY), pl.BlockSpec(memory_space=pltpu.VMEM)),
        scratch_shapes=[
            pltpu.VMEM((layers, ny, nz, units, RS, LN), F32),
            pltpu.VMEM((2, ny - 1, layers, nz, a, RS, LN), F32),
            pltpu.VMEM((2, nz - 1, layers, ny, b, RS, LN), F32),
            pltpu.VMEM((2, nz - 1, layers, a, RS, LN), F32),
            pltpu.VMEM((2, ny - 1, layers, b, RS, LN), F32),
            pltpu.VMEM((layers, 2 * nf, RS, LN), F32),
            pltpu.VMEM((3, max(nf, ny, nz)) + gr.shape, F32),
            pltpu.SemaphoreType.DMA((copies,)), pltpu.SemaphoreType.DMA((copies,)),
            pltpu.SemaphoreType.DMA((copies,)), pltpu.SemaphoreType.DMA((copies,)),
            pltpu.SemaphoreType.DMA((2, nf)), pltpu.SemaphoreType.DMA((2, nf)),
            pltpu.SemaphoreType.DMA((3, max(nf, ny, nz))), pltpu.SemaphoreType.DMA((3, max(nf, ny, nz))),
            pltpu.SemaphoreType.DMA, pltpu.SemaphoreType.DMA, pltpu.SemaphoreType.REGULAR,
        ],
        compiler_params=pltpu.CompilerParams(collective_id=0, has_side_effects=True, vmem_limit_bytes=52 * 2**20),
        name="grad_all_reduce",
    )(grads, gr)
    return out, gain_out


def unpack_kernel(g_ref, gate_ref, up_ref, down_ref):
    ny, nzb, units = g_ref.shape[:3]
    nf = units // 3
    for k in range(nzb):
        for i in range(ny):
            for m, ref in enumerate((gate_ref, up_ref)):
                for j in range(nf):
                    col = (j * ny + i) * LN
                    ref[k * RS:(k + 1) * RS, col:col + LN] = g_ref[i, k, m * nf + j]
            for h in range(2):
                for r in range(nf // 2):
                    row, col = (k * (nf // 2) + r) * RS, (2 * i + h) * LN
                    down_ref[row:row + RS, col:col + LN] = g_ref[i, k, 2 * nf + h * (nf // 2) + r]


def unpack(out, dims, steps=2):
    layers, ny, nz, nf = dims
    nzb = nz // steps
    wide, tall = nf * ny * LN, (nf // 2) * RS
    return pl.pallas_call(
        unpack_kernel, grid=(layers, steps),
        in_specs=[pl.BlockSpec((None, ny, nzb, 3 * nf, RS, LN), lambda l, z: (l, 0, z, 0, 0, 0))],
        out_specs=[pl.BlockSpec((None, nzb * RS, wide), lambda l, z: (l, z, 0))] * 2
        + [pl.BlockSpec((None, nzb * tall, 2 * ny * LN), lambda l, z: (l, z, 0))],
        out_shape=[jax.ShapeDtypeStruct((layers, nz * RS, wide), F32)] * 2
        + [jax.ShapeDtypeStruct((layers, nz * tall, 2 * ny * LN), F32)],
        name="unpack")(out)


NORM_EPS = 1e-6
NN = (((1,), (0,)), ((), ()))
NT = (((1,), (1,)), ((), ()))
TN = (((0,), (0,)), ((), ()))


def dot(a, b, dims=NN):
    return lax.dot_general(a, b, dims, preferred_element_type=F32)


def fb_kernel(dims, x_ref, dy_ref, wg_ref, wu_ref, wd_ref, gain_ref, y_ref, grad_ref, dgain_ref,
              WB, WD, N, GA, UA, PA, DH, O, DS, MS, H, DGU, GL,
              ag_send, ag_recv, rs_send, rs_recv, wx_send, wx_recv, wy_send, wy_recv, w_sem, wd_sem, out_sem):
    layers, ny, nz, nf, tok, depth, hid = dims
    nx, half, q = nf // 2, tok // 2, depth // nf // ny
    f, y = lax.axis_index("fsdp"), lax.axis_index("replica")
    x, c = f // 2, f % 2
    partner = 2 * x + (1 - c)
    tile = min(256, depth)

    def dev(off, core=None):
        return 2 * wrap(x + off, nx) + (c if core is None else core)

    h0, h1 = pl.ds(0, half), pl.ds(half, half)
    whole = pl.ds(0, tok)

    barrier = pltpu.get_barrier_semaphore()
    for j in range(1, nf):
        pl.semaphore_signal(barrier, inc=1, device_id={"fsdp": wrap(f + j, nf)}, device_id_type=MESH)
    for j in (1, ny - 1):
        pl.semaphore_signal(barrier, inc=1, device_id={"replica": wrap(y + j, ny)}, device_id_type=MESH)

    wd_copies = [pltpu.make_async_copy(wd_ref.at[l], WD.at[l], wd_sem.at[l]) for l in range(layers)]
    mine = pl.ds(y * q, q)
    weights = (wg_ref, wu_ref)

    def own_rows(l, m):
        src = weights[m].at[l, mine, pl.ds(pl.multiple_of(f * hid, hid), hid)]
        return pltpu.make_async_copy(src, WB.at[l, m, f, mine], w_sem.at[l, m])

    for l in range(layers):
        for m in range(2):
            own_rows(l, m).start()
        wd_copies[l].start()
    pl.semaphore_wait(barrier, nf + 1)

    def wx_copy(l, m, j, peer, sender):
        return pltpu.make_async_remote_copy(
            src_ref=weights[m].at[l, mine, pl.ds(pl.multiple_of(peer * hid, hid), hid)], dst_ref=WB.at[l, m, sender, mine],
            send_sem=wx_send.at[l, m, j], recv_sem=wx_recv.at[l, m, sender], device_id={"fsdp": peer}, device_id_type=MESH)

    def wx_start(l):
        for m in range(2):
            for j in range(1, nf):
                wx_copy(l, m, j, wrap(f + j, nf), f).start()

    parts = (pl.ds(0, nf // 2), pl.ds(nf // 2, nf // 2))

    def wy_copy(l, m, k, owner, part, step):
        view = WB.at[l, m, parts[part], pl.ds(wrap(owner, ny) * q, q)]
        return pltpu.make_async_remote_copy(
            src_ref=view, dst_ref=view, send_sem=wy_send.at[l, m, k], recv_sem=wy_recv.at[l, m, k],
            device_id={"replica": wrap(y + step, ny)}, device_id_type=MESH)

    def wy_sends(l, m):
        args = [(0, y, 0, 1), (2, y, 1, -1), (1, y, 1, 1), (3, y, 0, -1), (4, y - 1, 0, 1), (5, y + 1, 1, -1)]
        return [functools.partial(wy_copy, l, m, *a) for a in args]

    def wy_start(l):
        for m in range(2):
            own_rows(l, m).wait()
            for j in range(1, nf):
                wx_copy(l, m, j, wrap(f + j, nf), wrap(f + j, nf)).wait_recv()
            for copy in wy_sends(l, m)[:4]:
                copy().start()

    def wy_mid(l):
        for m in range(2):
            sends = wy_sends(l, m)
            wy_copy(l, m, 0, y - 1, 0, 1).wait_recv()
            sends[4]().start()
            wy_copy(l, m, 2, y + 1, 1, -1).wait_recv()
            sends[5]().start()

    def wy_end(l):
        for m in range(2):
            wy_copy(l, m, 1, y - 1, 1, 1).wait_recv()
            wy_copy(l, m, 3, y + 1, 0, -1).wait_recv()
            wy_copy(l, m, 4, y - 2, 0, 1).wait_recv()
            wy_copy(l, m, 5, y + 2, 1, -1).wait_recv()

    class Gather:
        def __init__(self, r, buf):
            self.r, self.buf = r, buf

        def copy(self, k, block, rows, target):
            view = self.buf.at[block, rows]
            return pltpu.make_async_remote_copy(
                src_ref=view, dst_ref=view, send_sem=ag_send.at[self.r, k], recv_sem=ag_recv.at[self.r, k],
                device_id={"fsdp": target}, device_id_type=MESH)

        def sends(self):
            args = [(0, f, whole, partner), (1, f, h0, dev(1)), (2, f, h1, dev(1)), (3, f, h1, dev(-1)), (4, f, h0, dev(-1)),
                    (5, dev(-1), h0, dev(1)), (6, dev(1), h1, dev(-1)), (7, dev(-1), whole, partner), (8, dev(1), whole, partner),
                    (9, dev(2), h0, partner), (10, dev(2), h1, partner)]
            return [functools.partial(self.copy, *a) for a in args]

        def wait(self, k):
            o = 1 - c
            block, rows = [(partner, whole), (dev(-1), h0), (dev(-1), h1), (dev(1), h1), (dev(1), h0), (dev(2), h0), (dev(2), h1),
                           (dev(-1, o), whole), (dev(1, o), whole), (dev(2, o), h0), (dev(2, o), h1)][k]
            self.copy(k, block, rows, partner).wait_recv()

        def start(self):
            sends = self.sends()
            for k in (1, 3, 0, 2, 4):
                sends[k]().start()

        def mid(self):
            sends = self.sends()
            for k, nxt in ((1, 5), (3, 6), (2, 7), (4, 8)):
                self.wait(k)
                sends[nxt]().start()

        def end(self):
            sends = self.sends()
            for k, nxt in ((5, 9), (6, 10)):
                self.wait(k)
                sends[nxt]().start()

        def near(self):
            self.wait(7)
            self.wait(8)

        def far(self):
            self.wait(9)
            self.wait(10)

        def drain(self):
            for copy in self.sends():
                copy().wait_send()

    def rs_d2d(r, i, xp, core):
        return pltpu.make_async_remote_copy(
            src_ref=O.at[xp, core], dst_ref=DS.at[r % 2, xp], send_sem=rs_send.at[r, i], recv_sem=rs_recv.at[r, i],
            device_id={"fsdp": partner}, device_id_type=MESH)

    quarter = half // 2

    def rs_msg(r, k, d):
        off, side = (2, d) if k == 0 else (1 - 2 * d, d if k == 3 else 1 - d)
        start, size, slot, at = side * half, half, (0 if k == 0 else 2), 0
        if k in (1, 2):
            at = (k - 1) * quarter
            start, size, slot = side * half + at, quarter, 1
        return pltpu.make_async_remote_copy(
            src_ref=O.at[wrap(x + off, nx), c, pl.ds(start, size)], dst_ref=MS.at[r % 2, d, slot, pl.ds(at, size)],
            send_sem=rs_send.at[r, 4 + 2 * k + d], recv_sem=rs_recv.at[r, 4 + 2 * k + d],
            device_id={"fsdp": dev(1 - 2 * d)}, device_id_type=MESH)

    def combine(r, i, off):
        xp = wrap(x + off, nx)
        rs_d2d(r, i, xp, c).wait_recv()
        O[xp, c] += DS[r % 2, xp]

    def rs_start(r):
        combine(r, 1, 1)
        rs_msg(r, 1, 0).start()
        combine(r, 2, 3)
        rs_msg(r, 1, 1).start()
        combine(r, 3, 2)
        for k in (0, 2):
            for d in range(2):
                rs_msg(r, k, d).start()
        combine(r, 0, 0)

    def rs_mid(r):
        for d in range(2):
            rs_msg(r, 0, d).wait_recv()
            O[wrap(x + 1 - 2 * d, nx), c, pl.ds(d * half, half)] += MS[r % 2, d, 0]
            rs_msg(r, 3, d).start()

    def rs_end(r):
        for k in (1, 2, 3):
            for d in range(2):
                rs_msg(r, k, d).wait_recv()
        s = r % 2
        top = O[x, c, h0] + (MS[s, 0, 2] + MS[s, 1, 1])
        bottom = O[x, c, h1] + (MS[s, 0, 1] + MS[s, 1, 2])
        for i in range(nx):
            rs_d2d(r, i, x, 1 - c).wait_send()
        for k in range(4):
            for d in range(2):
                rs_msg(r, k, d).wait_send()
        return jnp.concatenate([top, bottom], axis=0)

    def pairs(r, gather, body, waited):
        def step(i, carry):
            if not waited:
                @pl.when(i == 1)
                def _():
                    gather.mid()
                    gather.near()

                @pl.when(i == 3)
                def _():
                    gather.end()
                    gather.far()
            xp = wrap(x + i + i // 2 - 2 * (i // 3), nx)
            body(xp)
            rs_d2d(r, i, xp, 1 - c).start()
            return carry
        lax.fori_loop(0, nx, step, 0)

    def rms(hidden):
        return lax.rsqrt(jnp.mean(hidden * hidden, axis=-1, keepdims=True) + NORM_EPS)

    fwd = [Gather(l, N.at[l]) for l in range(layers)]
    bwd = [Gather(2 * layers - 1 - l, DH.at[l]) for l in range(layers)]
    last = layers - 1

    H[0] = x_ref[...]
    DH[last, f] = dy_ref[...]
    wx_start(0)
    for l in range(layers):
        hidden = H[l].astype(F32)
        N[l, f] = (hidden * rms(hidden) * gain_ref[l:l + 1]).astype(BF16)
        gather = fwd[l]
        gather.start()
        if l == 0:
            for other in range(1, layers):
                wx_start(other)
            bwd[last].start()
            wy_start(0)
            gather.mid()
            wy_mid(0)
            for other in range(1, layers):
                wy_start(other)
            gather.near()
            gather.end()
            gather.far()
            bwd[last].mid()
            gather.wait(0)
            wy_end(0)
        else:
            wy_end(l)
            gather.wait(0)
        wd_copies[l].wait()

        def forward(xp, l=l):
            tokens = N[l, pl.ds(2 * xp, 2)].reshape(2 * tok, depth)
            for j in range(hid // tile):
                cols = pl.ds(j * tile, tile)
                gate = dot(tokens, WB[l, 0, :, :, cols].reshape(depth, tile)).astype(BF16)
                up = dot(tokens, WB[l, 1, :, :, cols].reshape(depth, tile)).astype(BF16)
                GA[l, xp, :, cols] = gate
                UA[l, xp, :, cols] = up
                PA[l, xp, :, cols] = (jax.nn.silu(gate.astype(F32)) * up.astype(F32)).astype(BF16)
            prod = PA[l, xp]
            for j in range(depth // tile):
                cols = pl.ds(j * tile, tile)
                O[xp, :, :, cols] = dot(prod, WD[l, :, cols]).reshape(2, tok, tile)

        pairs(l, gather, forward, l == 0)
        rs_start(l)
        if l == 0:
            bwd[last].near()
            bwd[last].end()
            bwd[last].far()
            bwd[last].wait(0)
            for other in range(1, layers):
                wy_mid(other)
        rs_mid(l)
        hidden = (H[l].astype(F32) + rs_end(l)).astype(BF16)
        if l < last:
            H[l + 1] = hidden
        else:
            y_ref[...] = hidden

    grad_copy = None
    for l in reversed(range(layers)):
        r = 2 * layers - 1 - l
        gather = bwd[l]
        if l != last:
            gather.start()
            gather.wait(0)

        def backward(xp, l=l):
            cot = DH[l, pl.ds(2 * xp, 2)].reshape(2 * tok, depth)
            for j in range(hid // tile):
                cols = pl.ds(j * tile, tile)
                d_prod = dot(cot, WD[l, cols, :], NT).astype(BF16).astype(F32)
                gate = GA[l, xp, :, cols].astype(F32)
                sig = jax.nn.sigmoid(gate)
                d_up = d_prod * gate * sig
                d_gate = d_prod * UA[l, xp, :, cols].astype(F32) * sig * (1.0 + gate * (1.0 - sig))
                DGU[0, xp, :, cols] = d_gate.astype(BF16)
                DGU[1, xp, :, cols] = d_up.astype(BF16)
            d_gate, d_up = DGU[0, xp], DGU[1, xp]
            rows = depth // nf
            for j in range(depth // tile):
                sub = pl.ds(j * tile // rows, tile // rows)
                part = dot(d_gate, WB[l, 0, sub].reshape(tile, hid), NT) + dot(d_up, WB[l, 1, sub].reshape(tile, hid), NT)
                O[xp, :, :, pl.ds(j * tile, tile)] = part.reshape(2, tok, tile)

        pairs(r, gather, backward, l == last)
        rs_start(r)

        if grad_copy is not None:
            grad_copy.wait()
        group = nf // 2
        zs = tile // (group * RS)

        def down_grad(j, carry, l=l):
            lhs = PA[l, :, :, pl.ds(pl.multiple_of(j * tile, tile), tile)].reshape(nf * tok, tile)
            for i in range(depth // tile):
                res = dot(lhs, DH[l, :, :, pl.ds(i * tile, tile)].reshape(nf * tok, tile), TN)
                for h in range(tile // LN):
                    col = i * (tile // LN) + h
                    for zi in range(zs):
                        for g in range(group):
                            row = (zi * group + g) * RS
                            GL[col // 2, j * zs + zi, 2 * nf + (col % 2) * group + g] = res[row:row + RS, h * LN:(h + 1) * LN]
            return carry
        lax.fori_loop(0, hid // tile, down_grad, 0)
        rs_mid(r)

        fs = tile // (nz * RS)

        def up_grad(j, carry, l=l):
            lhs = N[l, :, :, pl.ds(pl.multiple_of(j * tile, tile), tile)].reshape(nf * tok, tile)
            for m in range(2):
                for i in range(hid // tile):
                    res = dot(lhs, DGU[m, :, :, pl.ds(i * tile, tile)].reshape(nf * tok, tile), TN)
                    for h in range(tile // LN):
                        for fi in range(fs):
                            for zi in range(nz):
                                row = (fi * nz + zi) * RS
                                GL[i * (tile // LN) + h, zi, m * nf + j * fs + fi] = res[row:row + RS, h * LN:(h + 1) * LN]
            return carry
        lax.fori_loop(0, depth // tile, up_grad, 0)
        grad_copy = pltpu.make_async_copy(GL, grad_ref.at[l], out_sem)
        grad_copy.start()

        d_normed = rs_end(r).astype(BF16).astype(F32)
        hidden = H[l].astype(F32)
        inv = rms(hidden)
        dgain_ref[l:l + 1] = jnp.sum(d_normed * hidden * inv, axis=0, keepdims=True)
        if l > 0:
            scaled = d_normed * gain_ref[l:l + 1]
            cot = DH[l, f].astype(F32)
            d_hidden = cot + inv * scaled - hidden * (inv * inv * inv) * jnp.mean(scaled * hidden, axis=-1, keepdims=True)
            DH[l - 1, f] = d_hidden.astype(BF16)

    for gather in fwd + bwd:
        gather.drain()
    for l in range(layers):
        for m in range(2):
            for j in range(1, nf):
                wx_copy(l, m, j, wrap(f + j, nf), f).wait_send()
            for copy in wy_sends(l, m):
                copy().wait_send()
    grad_copy.wait()


def forward_backward(x, dy, wg, wu, wd, gain, dims):
    layers, ny, nz, nf, tok, depth, hid = dims
    nx = nf // 2
    vm, hbm = pl.BlockSpec(memory_space=pltpu.VMEM), pl.BlockSpec(memory_space=pl.ANY)
    dma = pltpu.SemaphoreType.DMA
    return pl.pallas_call(
        functools.partial(fb_kernel, dims),
        out_shape=(jax.ShapeDtypeStruct((tok, depth), BF16),
                   jax.ShapeDtypeStruct((layers, ny, nz, 3 * nf, RS, LN), F32),
                   jax.ShapeDtypeStruct((layers, depth), F32)),
        in_specs=[vm, vm, hbm, hbm, hbm, vm],
        out_specs=(vm, hbm, vm),
        scratch_shapes=[
            pltpu.VMEM((layers, 2, nf, depth // nf, hid), BF16),
            pltpu.VMEM((layers, hid, depth), BF16),
            pltpu.VMEM((layers, nf, tok, depth), BF16),
            pltpu.VMEM((layers, nx, 2 * tok, hid), BF16),
            pltpu.VMEM((layers, nx, 2 * tok, hid), BF16),
            pltpu.VMEM((layers, nx, 2 * tok, hid), BF16),
            pltpu.VMEM((layers, nf, tok, depth), BF16),
            pltpu.VMEM((nx, 2, tok, depth), F32),
            pltpu.VMEM((2, nx, tok, depth), F32),
            pltpu.VMEM((2, 2, 3, tok // 2, depth), F32),
            pltpu.VMEM((layers, tok, depth), BF16),
            pltpu.VMEM((2, nx, 2 * tok, hid), BF16),
            pltpu.VMEM((ny, nz, 3 * nf, RS, LN), F32),
            dma((2 * layers, 11)), dma((2 * layers, 11)),
            dma((2 * layers, 12)), dma((2 * layers, 12)),
            dma((layers, 2, nf)), dma((layers, 2, nf)),
            dma((layers, 2, 6)), dma((layers, 2, 6)),
            dma((layers, 2)), dma((layers,)), dma,
        ],
        compiler_params=pltpu.CompilerParams(collective_id=1, has_side_effects=True, vmem_limit_bytes=60 * 2**20),
        name="forward_backward",
    )(x, dy, wg, wu, wd, gain)


TOKEN_AXES = ("dp", "replica", "fsdp")


def solution(mesh):
    ny, nz, nf = mesh.shape["replica"], mesh.shape["dp"], mesh.shape["fsdp"]
    tok_spec, shard_spec, full_spec = P(TOKEN_AXES, None), P(None, "fsdp", None), P(None, None)

    def device_step(x, dy, wg, wu, wd, gain):
        layers, depth = gain.shape
        dims = (layers, ny, nz, nf)
        out, grads, d_gain = forward_backward(x, dy, wg, wu, wd, gain, dims + (x.shape[0], depth, wd.shape[1]))
        blocks, gain_sum = all_reduce(grads, d_gain, dims)
        dw_gate, dw_up, dw_down = unpack(blocks, dims)
        return out, dw_gate, dw_up, dw_down, gain_sum.reshape(gain.shape)

    return jax.shard_map(
        device_step, mesh=mesh, in_specs=(tok_spec, tok_spec, shard_spec, shard_spec, shard_spec, full_spec),
        out_specs=(tok_spec, shard_spec, shard_spec, shard_spec, full_spec), check_vma=False)
```

```python
import functools
import heapq
import jax
import jax.numpy as jnp
from jax import lax
from jax.sharding import PartitionSpec as P
from jax.experimental import pallas as pl
from jax.experimental.pallas import tpu as pltpu

F32 = jnp.float32
BF16 = jnp.bfloat16
LOGICAL = pl.DeviceIdType.LOGICAL
RS, LN = 16, 128
UNIT_BYTES = RS * LN * 4
NORM_EPS = 1e-6
NN = (((1,), (0,)), ((), ()))
NT = (((1,), (1,)), ((), ()))
TN = (((0,), (0,)), ((), ()))
LINK_RATE, CORE_RATE, HOP, CORE_HOP, STEP_COST = 46.6e3, 500e3, 2.2, 0.9, 0.15
CORES = "cores"
BOTH, SIGN, BF16_BYTES = (0, 1), (1, -1), 2
FIRST, SECOND, PASS, RELAY, FAR, OWN = range(6)
FORWARD, BACKWARD, DOWN, ADD, EXCHANGE = 1.2, 1.7, 2.2, 0.2, 5.0


def dot(a, b, dims=NN):
    return lax.dot_general(a, b, dims, preferred_element_type=F32)


def repeat(start, stop, work):
    def step(i, carry):
        work(i)
        return carry
    lax.fori_loop(start, stop, step, 0)


def wrap(value, size):
    return lax.rem(value + 4 * size, size)


class Clock:
    def __init__(self):
        self.now, self.queue, self.count, self.links = 0.0, [], 0, {}

    def send(self, link, size):
        near = link == CORES
        start = max(self.now, self.links.get(link, 0.0))
        self.links[link] = start + size / (CORE_RATE if near else LINK_RATE)
        return self.links[link] + (CORE_HOP if near else HOP)

    def after(self, ready, work):
        self.count += 1
        heapq.heappush(self.queue, (ready, self.count, work))

    def step(self):
        ready, _, work = heapq.heappop(self.queue)
        self.now = max(self.now, ready) + STEP_COST
        work()

    def run(self, until):
        while self.queue and self.queue[0][0] <= until:
            self.step()

    def busy(self, spent):
        self.now += spent
        self.run(self.now)

    def idle(self, until):
        self.run(until)
        self.now = max(self.now, until)


class Job:
    def __init__(self, env, layer, part, start, offsets, swap):
        sizes = PART_SIZES[part]
        self.env, self.layer, self.part, self.swap = env, layer, part, swap
        self.sizes, self.offsets, self.starts = sizes, offsets, (start, start + sizes[0])
        self.units = pl.ds(start, sum(sizes))
        self.left, self.arrived, self.early = 2, {}, {}
        rings = (env.ny // 2, env.nz // 2)
        self.slots = {}
        for gather in (False, True):
            for phase in BOTH:
                for k in BOTH:
                    for d in BOTH:
                        half = rings[phase ^ k]
                        self.slots[gather, phase, k, d] = env.slots[gather]
                        env.slots[gather] += half if gather else half + 1

    def ring(self, phase, k):
        return ("replica", "dp")[phase ^ k]

    def half_ring(self, phase, k):
        return self.env.size[self.ring(phase, k)] // 2

    def block(self, phase, k, index, side=None):
        env, G, layer = self.env, self.env.G, self.layer
        start, size = self.starts[k], self.sizes[k]
        if side is not None:
            start, size = start + side * (size // 2), size // 2
        units = pl.ds(start, size)
        if phase == 0:
            return G.at[layer, index, :, units] if k == 0 else G.at[layer, :, index, units]
        return G.at[layer, env.y, index, units] if k == 0 else G.at[layer, index, env.z, units]

    def stage(self, phase, k, d, step, side=None):
        env = self.env
        buf = env.G.at[0] if self.layer == env.last else env.S
        first = 0 if k == 0 else env.split
        offset, size = self.offsets[k], self.sizes[k]
        half_total = ((env.units - env.split) if k else env.split) // 2
        at = 2 * (step - 1) + d
        if step == 0:
            units = pl.ds(first + d * half_total + offset // 2, size // 2)
            at = env.nz - 2 if self.ring(phase, k) == "dp" else 2
        elif side is None:
            units = pl.ds(first + offset, size)
        else:
            units = pl.ds(first + offset + side * (size // 2), size // 2)
        if phase == 0:
            return buf.at[at, :, units] if k == 0 else buf.at[:, at, units]
        return buf.at[env.ny - 1, at, units] if k == 0 else buf.at[at, env.nz - 1, units]

    def copy(self, gather, phase, k, d, slot, src, dst):
        env = self.env
        send, recv = (env.ag_send, env.ag_recv) if gather else (env.rs_send, env.rs_recv)
        slot = self.slots[gather, phase, k, d] + slot
        return pltpu.make_async_remote_copy(
            src_ref=src, dst_ref=dst, send_sem=send.at[slot], recv_sem=recv.at[slot],
            device_id=env.device(self.ring(phase, k), SIGN[d]), device_id_type=LOGICAL)

    def send_time(self, phase, k, d, units):
        env = self.env
        other = (env.nz if k == 0 else env.ny) if phase == 0 else 1
        return env.clock.send((self.ring(phase, k), d), units * other * UNIT_BYTES)

    def piece(self, phase, k, d, step, early):
        if step == 0:
            return 0, d
        if step == 1:
            return (1, 1 - d) if early else (2, d)
        return step + 1, None

    def reduce_copy(self, phase, k, d, step, early=False):
        slot, side = self.piece(phase, k, d, step, early)
        index = self.env.near(self.ring(phase, k), SIGN[d] * (self.half_ring(phase, k) - step))
        stage = self.stage(phase, k, d, step, None if step == 0 else side)
        return self.copy(False, phase, k, d, slot, self.block(phase, k, index, side), stage)

    def reduce_send(self, phase, k, d, step, early=False):
        self.reduce_copy(phase, k, d, step, early).start()
        ready = self.send_time(phase, k, d, self.sizes[k] if step > 1 else self.sizes[k] // 2)
        if early:
            self.early[phase, k, d] = ready
        else:
            if step == 1:
                ready = max(ready, self.early[phase, k, d])
            self.env.clock.after(ready, functools.partial(self.reduce_step, phase, k, d, step))

    def reduce_start(self, phase, k):
        for d in BOTH:
            self.reduce_send(phase, k, d, 0)
        for d in BOTH:
            self.reduce_send(phase, k, d, 1, True)

    def start(self):
        for k in BOTH:
            self.reduce_start(0, k)

    def reduce_step(self, phase, k, d, step):
        half = self.half_ring(phase, k)
        if step == 1:
            self.reduce_copy(phase, k, d, step, True).wait_recv()
        self.reduce_copy(phase, k, d, step).wait_recv()
        index = self.env.near(self.ring(phase, k), SIGN[d] * (half - 1 - step))
        self.block(phase, k, index, d if step == 0 else None)[...] += self.stage(phase, k, d, step)[...]
        if step + 1 < half:
            self.reduce_send(phase, k, d, step + 1)
        elif self.both(False, phase, k):
            if phase == 0:
                self.reduce_start(1, k)
            else:
                self.left -= 1
                if self.left == 0:
                    self.reduced()

    def both(self, gather, phase, k):
        key = gather, phase, k
        self.arrived[key] = self.arrived.get(key, 0) + 1
        return self.arrived[key] == 2

    def wait_sends(self, gather):
        for phase in BOTH:
            for k in BOTH:
                half = self.half_ring(phase, k)
                for d in BOTH:
                    some, all_units = self.block(phase, k, 0, d), self.block(phase, k, 0)

                    def done(slot, view):
                        self.copy(gather, phase, k, d, slot, view, view).wait_send()
                    if gather:
                        repeat(0, half - 1, lambda slot: done(slot, all_units))
                        done(half - 1, some)
                    else:
                        repeat(0, 3, lambda slot: done(slot, some))
                        if half > 2:
                            repeat(3, half + 1, lambda slot: done(slot, all_units))

    def x_copy(self, m, j, peer, sender):
        env = self.env
        return pltpu.make_async_remote_copy(
            src_ref=env.G.at[self.layer, env.y, env.z, m * env.nf + peer], dst_ref=env.R.at[self.layer, m * env.nf + sender],
            send_sem=env.x_send.at[self.layer, m, j], recv_sem=env.x_recv.at[self.layer, m, sender],
            device_id=env.row + peer, device_id_type=LOGICAL)

    def reduced(self):
        env = self.env
        self.wait_sends(False)
        for axis in ("replica", "dp"):
            for sign in (1, -1):
                pl.semaphore_signal(env.ready.at[self.layer, self.part], device_id=env.device(axis, sign), device_id_type=LOGICAL)
        for m in self.swap:
            repeat(1, env.nf, lambda j: self.x_copy(m, j, wrap(env.f + j, env.nf), env.f).start())
        env.reduced.add((self.layer, self.part))
        env.clock.after(env.clock.now + (EXCHANGE if self.swap else HOP), self.exchanged)

    def exchanged(self):
        env = self.env
        f, nf = env.f, env.nf
        for m in self.swap:
            env.R[self.layer, m * nf + f] = env.G[self.layer, env.y, env.z, m * nf + f]
        for m in self.swap:
            repeat(1, nf, lambda j: self.x_copy(m, j, wrap(f + j, nf), f).wait_send())
            repeat(1, nf, lambda j: self.x_copy(m, j, wrap(f + j, nf), wrap(f + j, nf)).wait_recv())
        for m in self.swap:
            env.G[self.layer, env.y, env.z, pl.ds(m * nf, nf)] = env.R[self.layer, pl.ds(m * nf, nf)]
        pl.semaphore_wait(env.ready.at[self.layer, self.part], 4)
        self.left = 2
        for k in BOTH:
            self.gather_start(1, k)
        env.exchanged.add((self.layer, self.part))
        env.begin_waiting()

    def gather_copy(self, phase, k, d, step, index):
        side = d if step + 1 == self.half_ring(phase, k) else None
        view = self.block(phase, k, self.env.near(self.ring(phase, k), index), side)
        return self.copy(True, phase, k, d, step, view, view)

    def gather_send(self, phase, k, d, step):
        self.gather_copy(phase, k, d, step, -SIGN[d] * step).start()
        units = self.sizes[k] if step + 1 < self.half_ring(phase, k) else self.sizes[k] // 2
        ready = self.send_time(phase, k, d, units)
        self.env.clock.after(ready, functools.partial(self.gather_step, phase, k, d, step))

    def gather_start(self, phase, k):
        for d in BOTH:
            self.gather_send(phase, k, d, 0)

    def gather_step(self, phase, k, d, step):
        env = self.env
        self.gather_copy(phase, k, d, step, -SIGN[d] * (step + 1)).wait_recv()
        if step + 1 < self.half_ring(phase, k):
            self.gather_send(phase, k, d, step + 1)
        elif self.both(True, phase, k):
            if phase == 1:
                self.gather_start(0, k)
            else:
                self.left -= 1
                if self.left == 0:
                    here = (self.layer, slice(None), slice(None), self.units)
                    pltpu.make_async_copy(env.G.at[here], env.out_ref.at[here], env.out_sem).start()


class Env:
    def __init__(self, dims):
        self.exchanged, self.reduced, self.waiting, self.clock = set(), set(), [], Clock()
        self.slots = {False: 0, True: 0}
        self.ny, self.nz, self.nf = dims[1:4]
        self.last = dims[0] - 1
        self.f, self.y, self.z = lax.axis_index("fsdp"), lax.axis_index("replica"), lax.axis_index("dp")
        self.size = {"fsdp": self.nf, "replica": self.ny, "dp": self.nz}
        self.pos = {"fsdp": self.f, "replica": self.y, "dp": self.z}
        stride = {"fsdp": 1, "replica": self.nf, "dp": self.nf * self.ny}
        me = self.f + stride["replica"] * self.y + stride["dp"] * self.z
        self.row = me - self.f
        self.shift = {a: [wrap(self.pos[a] + k, n) for k in range(n)] for a, n in self.size.items()}
        self.ids = {a: [me + (p - self.pos[a]) * stride[a] for p in self.shift[a]] for a in self.size}

    def near(self, axis, k):
        return self.shift[axis][k % self.size[axis]]

    def device(self, axis, k):
        return self.ids[axis][k % self.size[axis]]

    def begin(self, job):
        self.waiting.append(job)
        self.begin_waiting()

    def begin_waiting(self):
        for job in list(self.waiting):
            above = job.layer + 1, job.part
            if above[0] >= self.last or above in self.exchanged:
                self.waiting.remove(job)
                job.start()

    def settle(self, layer):
        while not {(layer, part) for part in BOTH} <= self.reduced:
            self.clock.step()


PART_SIZES = ((10, 6), (4, 4))
GATE_UP, DOWN_PART = BOTH


def step_kernel(dims, x_ref, dy_ref, wg_ref, wu_ref, wd_ref, gain_ref, y_ref, out_ref, gain_out,
                WB, WD, N, GA, UA, DH, O, DS, MS, H, DGU, G, S, R, gain_buf, gain_row,
                ag_send, ag_recv, rs_send, rs_recv, wx_send, wx_recv, wy_send, wy_recv, w_sem, wd_sem,
                jr_send, jr_recv, jg_send, jg_recv, x_send, x_recv, g_send, g_recv, out_sem, io_sem, ready, credit):
    layers, ny, nz, nf, tok, depth, hid = dims
    nx, half, q = nf // 2, tok // 2, depth // nf // ny
    tile = min(256, depth)
    last = layers - 1

    env = Env(dims)
    f, y, z = env.f, env.y, env.z
    x, c = f // 2, f % 2
    env.G, env.S, env.R, env.out_ref = G, S, R, out_ref
    env.rs_send, env.rs_recv, env.ag_send, env.ag_recv = jr_send, jr_recv, jg_send, jg_recv
    env.x_send, env.x_recv, env.ready, env.out_sem = x_send, x_recv, ready, out_sem
    env.units, env.split = 3 * nf, sum(sizes[0] for sizes in PART_SIZES)
    clock = env.clock
    jobs = {}
    for l in reversed(range(layers)):
        jobs[l, GATE_UP] = Job(env, l, GATE_UP, 0, (0, 0), BOTH)
        jobs[l, DOWN_PART] = Job(env, l, DOWN_PART, sum(PART_SIZES[GATE_UP]), PART_SIZES[GATE_UP], ())

    chips = [wrap(x + k, nx) for k in range(nx)]
    same, opposite_core = [2 * p + c for p in chips], [2 * p + (1 - c) for p in chips]
    fid = {id(v): env.row + v for v in same + opposite_core}

    def dev(off, opposite=False):
        return (opposite_core if opposite else same)[off % nx]

    partner = dev(0, True)
    halves = (pl.ds(0, half), pl.ds(half, half))
    whole = pl.ds(0, tok)
    axes = [("fsdp", f, nf), ("replica", y, ny), ("dp", z, nz)]

    barrier = pltpu.get_barrier_semaphore()
    for axis, pos, size in axes:
        for j in range(1, size):
            pl.semaphore_signal(barrier, device_id=env.device(axis, j), device_id_type=LOGICAL)

    x_copy = pltpu.make_async_copy(x_ref, H.at[0], io_sem.at[0])
    dy_copy = pltpu.make_async_copy(dy_ref, DH.at[last % 2, f], io_sem.at[1])
    x_copy.start()
    dy_copy.start()
    wd_copies = [pltpu.make_async_copy(wd_ref.at[l], WD.at[l], wd_sem.at[l]) for l in range(layers)]
    mine = pl.ds(y * q, q)
    weights = (wg_ref, wu_ref)

    def own_rows(l, m):
        src = weights[m].at[l, mine, pl.ds(pl.multiple_of(f * hid, hid), hid)]
        return pltpu.make_async_copy(src, WB.at[l, m, f, mine], w_sem.at[l, m])

    for l in range(layers):
        for m in BOTH:
            own_rows(l, m).start()
        wd_copies[l].start()
    pl.semaphore_wait(barrier, nf + ny + nz - 3)

    def wx_copy(l, m, j, peer, sender):
        return pltpu.make_async_remote_copy(
            src_ref=weights[m].at[l, mine, pl.ds(pl.multiple_of(peer * hid, hid), hid)], dst_ref=WB.at[l, m, sender, mine],
            send_sem=wx_send.at[l, m, j], recv_sem=wx_recv.at[l, m, sender], device_id=env.row + peer, device_id_type=LOGICAL)

    def wx_start(l):
        for m in BOTH:
            repeat(1, nf, lambda j: wx_copy(l, m, j, wrap(f + j, nf), f).start())

    y_rows = [env.near("replica", k) * q for k in range(ny)]
    parts = (pl.ds(0, nf // 2), pl.ds(nf // 2, nf // 2))

    def wy_copy(l, m, kind, d, arrived=False):
        hops = (kind == PASS) + arrived
        part = parts[BOTH[d - (kind == SECOND)]]
        view = WB.at[l, m, part, pl.ds(y_rows[-SIGN[d] * hops % ny], q)]
        return pltpu.make_async_remote_copy(
            src_ref=view, dst_ref=view, send_sem=wy_send.at[l, m, kind, d], recv_sem=wy_recv.at[l, m, kind, d],
            device_id=env.device("replica", SIGN[d]), device_id_type=LOGICAL)

    def wy_each(l, kinds, work):
        for m in BOTH:
            for kind in kinds:
                for d in BOTH:
                    work(l, m, kind, d)

    def wy_send_one(*args):
        wy_copy(*args).start()

    def wy_take(*args):
        wy_copy(*args, True).wait_recv()

    def wy_start(l):
        for m in BOTH:
            own_rows(l, m).wait()
            repeat(1, nf, lambda j: wx_copy(l, m, j, wrap(f + j, nf), wrap(f + j, nf)).wait_recv())
            for kind in (FIRST, SECOND):
                for d in BOTH:
                    wy_send_one(l, m, kind, d)

    def wy_mid(l):
        for m in BOTH:
            for d in BOTH:
                wy_take(l, m, FIRST, d)
                wy_send_one(l, m, PASS, d)

    def wy_end(l):
        wy_each(l, (SECOND, PASS), wy_take)

    class Gather:
        def __init__(self, r, buf):
            self.r, self.buf, self.ready = r, buf, {}

        def copy(self, kind, d, arrived=False):
            hops = (kind in (PASS, RELAY)) + (kind == FAR) * nx // len(BOTH)
            local = kind in (RELAY, FAR, OWN)
            block = dev(-SIGN[d] * (hops + (arrived and not local)), arrived and local)
            rows = whole if kind in (RELAY, OWN) else halves[d - (kind == SECOND)]
            target = partner if local else dev(SIGN[d])
            view = self.buf.at[block, rows]
            return rows.size, pltpu.make_async_remote_copy(
                src_ref=view, dst_ref=view, send_sem=ag_send.at[self.r, kind, d], recv_sem=ag_recv.at[self.r, kind, d],
                device_id=fid[id(target)], device_id_type=LOGICAL)

        def send(self, kind, d):
            size, copy = self.copy(kind, d)
            copy.start()
            self.ready[kind, d] = clock.send(CORES if kind in (RELAY, FAR, OWN) else d, size * depth * BF16_BYTES)

        def wait(self, kind, d=0):
            clock.idle(self.ready[kind, d])
            self.copy(kind, d, True)[-1].wait_recv()

        def start(self):
            for kind in (FIRST, OWN, SECOND):
                for d in BOTH[:1] if kind == OWN else BOTH:
                    self.send(kind, d)

        def forward(self, kind, onward):
            for d in BOTH:
                self.wait(kind, d)
                self.send(onward, d)

        def mid(self):
            self.forward(FIRST, PASS)
            self.forward(SECOND, RELAY)

        def end(self):
            self.forward(PASS, FAR)

        def take(self, kind):
            for d in BOTH:
                self.wait(kind, d)

        def near(self):
            self.take(RELAY)

        def far(self):
            self.take(FAR)

        def drain(self):
            for kind, d in self.ready:
                self.copy(kind, d)[-1].wait_send()

    def rs_d2d(r, i, xp, core):
        return pltpu.make_async_remote_copy(
            src_ref=O.at[xp, core], dst_ref=DS.at[xp], send_sem=rs_send.at[r, i], recv_sem=rs_recv.at[r, i],
            device_id=fid[id(partner)], device_id_type=LOGICAL)

    quarter = half // 2
    chunk = min(16, half)
    arrive = {}

    def rs_msg(r, k, d):
        off, side = (2, d) if k == 0 else (SIGN[d], d if k == 3 else 1 - d)
        start, size, slot, at = side * half, half, (0 if k == 0 else 2), 0
        if k in (1, 2):
            at = (k - 1) * quarter
            start, size, slot = side * half + at, quarter, 1
        return pltpu.make_async_remote_copy(
            src_ref=O.at[chips[off % nx], c, pl.ds(start, size)], dst_ref=MS.at[d, slot, pl.ds(at, size)],
            send_sem=rs_send.at[r, 4 + 2 * k + d], recv_sem=rs_recv.at[r, 4 + 2 * k + d],
            device_id=fid[id(dev(SIGN[d]))], device_id_type=LOGICAL)

    def rs_post(r, k, d):
        rs_msg(r, k, d).start()
        arrive[k, d] = clock.send(d, (quarter if k in (1, 2) else half) * depth * 4)

    def rs_take(r, k, d):
        clock.idle(arrive[k, d])
        rs_msg(r, k, d).wait_recv()

    def rows_at(start, j):
        return pl.ds(pl.multiple_of(start + j * chunk, chunk), chunk)

    def combine(r, i, off):
        xp = chips[off % nx]
        clock.idle(arrive[i])
        rs_d2d(r, i, xp, c).wait_recv()

        def add(j):
            rows = rows_at(0, j)
            O[xp, c, rows] += DS[xp, rows]
        repeat(0, tok // chunk, add)
        clock.busy(ADD)

    def rs_start(r):
        for i, d in ((1, 0), (2, 1)):
            combine(r, i, SIGN[d])
            rs_post(r, 1, d)
        combine(r, 3, 2)
        for k in (0, 2):
            for d in BOTH:
                rs_post(r, k, d)
        combine(r, 0, 0)

    def rs_mid(r):
        for d in BOTH:
            rs_take(r, 0, d)

            def add(j):
                rows = rows_at(d * half, j)
                O[chips[SIGN[d] % nx], c, rows] += MS[d, 0, rows_at(0, j)]
            repeat(0, half // chunk, add)
            rs_post(r, 3, d)

    def rs_end(r, body):
        for k in (1, 2, 3):
            for d in BOTH:
                rs_take(r, k, d)
        for side in BOTH:
            def step(j):
                rows, local = rows_at(side * half, j), rows_at(0, j)
                body(rows, O[x, c, rows] + (MS[0, 2 - side, local] + MS[1, 1 + side, local]))
            repeat(0, half // chunk, step)
        clock.busy(5 * ADD)
        for i in range(nx):
            rs_d2d(r, i, x, 1 - c).wait_send()
        for k in range(4):
            for d in BOTH:
                rs_msg(r, k, d).wait_send()

    def pairs(r, gather, body, cost):
        def step(i):
            xp = wrap(x + i + i // 2 - 2 * (i // 3), nx)
            body(xp)
            rs_d2d(r, i, xp, 1 - c).start()

        def go(first, stop):
            repeat(first, stop, step)
            for i in range(first, stop):
                clock.now += cost
                arrive[i] = clock.send(CORES, tok * depth * 4)
            clock.busy(0.0)

        if gather is None:
            go(0, nx)
            return
        go(0, 1)
        gather.mid()
        gather.near()
        go(1, 3)
        gather.end()
        gather.far()
        go(3, nx)

    def rms(hidden):
        return lax.rsqrt(jnp.mean(hidden * hidden, axis=-1, keepdims=True) + NORM_EPS)

    def down_grad(l):
        group = nf // 2
        zs = tile // (group * RS)

        def body(j, carry):
            lhs = GA[l, :, :, pl.ds(pl.multiple_of(j * tile, tile), tile)].reshape(-1, tile)
            for i in range(depth // tile):
                res = dot(lhs, DH[l % 2, :, :, pl.ds(i * tile, tile)].reshape(-1, tile), TN)
                for h in range(tile // LN):
                    col = i * (tile // LN) + h
                    for zi in range(zs):
                        rows = res[zi * group * RS:(zi + 1) * group * RS, h * LN:(h + 1) * LN]
                        G[l, col // 2, j * zs + zi, pl.ds(2 * nf + (col % 2) * group, group)] = rows.reshape(group, RS, LN)
            return carry
        lax.fori_loop(0, hid // tile, body, 0)

    def up_grad(l):
        fs = tile // (nz_rows * RS)

        def body(j, carry):
            lhs = N[l, :, :, pl.ds(pl.multiple_of(j * tile, tile), tile)].reshape(-1, tile)
            for m in BOTH:
                for i in range(hid // tile):
                    res = dot(lhs, DGU[m, :, :, pl.ds(i * tile, tile)].reshape(-1, tile), TN)
                    for h in range(tile // LN):
                        for fi in range(fs):
                            rows = res[fi * nz_rows * RS:(fi + 1) * nz_rows * RS, h * LN:(h + 1) * LN]
                            G[l, i * (tile // LN) + h, :, m * nf + j * fs + fi] = rows.reshape(nz_rows, RS, LN)
            return carry
        lax.fori_loop(0, depth // tile, body, 0)

    nz_rows = depth // nf // RS
    fwd = [Gather(l, N.at[l]) for l in range(layers)]
    bwd = [Gather(2 * layers - 1 - l, DH.at[l % 2]) for l in range(layers)]

    def activations(l, xp, cols):
        tokens = N[l, pl.ds(2 * xp, 2)].reshape(-1, depth)
        gate = dot(tokens, WB[l, 0, :, :, cols].reshape(depth, tile)).astype(BF16)
        up = dot(tokens, WB[l, 1, :, :, cols].reshape(depth, tile)).astype(BF16)
        return gate, up

    def product(xp, prod, l):
        for j in range(depth // tile):
            cols = pl.ds(j * tile, tile)
            O[xp, :, :, cols] = dot(prod, WD[l, :, cols]).reshape(-1, tok, tile)

    def forward(l, xp):
        for j in range(hid // tile):
            cols = pl.ds(j * tile, tile)
            gate, up = activations(l, xp, cols)
            GA[l, xp, :, cols] = gate
            UA[l, xp, :, cols] = up
            DGU[0, xp, :, cols] = (jax.nn.silu(gate.astype(F32)) * up.astype(F32)).astype(BF16)
        product(xp, DGU[0, xp], l)

    def backward(l, xp):
        cot = DH[l % 2, pl.ds(2 * xp, 2)].reshape(-1, depth)
        for j in range(hid // tile):
            cols = pl.ds(j * tile, tile)
            gate, up = activations(l, xp, cols) if l == last else (GA[l, xp, :, cols], UA[l, xp, :, cols])
            gate, up = gate.astype(F32), up.astype(F32)
            d_prod = dot(cot, WD[l, cols, :], NT).astype(BF16).astype(F32)
            sig = jax.nn.sigmoid(gate)
            GA[l, xp, :, cols] = (gate * sig * up).astype(BF16)
            DGU[0, xp, :, cols] = (d_prod * up * sig * (1.0 + gate * (1.0 - sig))).astype(BF16)
            DGU[1, xp, :, cols] = (d_prod * gate * sig).astype(BF16)
        d_gate, d_up = DGU[0, xp], DGU[1, xp]
        rows = depth // nf
        for j in range(depth // tile):
            sub = pl.ds(j * tile // rows, tile // rows)
            part = dot(d_gate, WB[l, 0, sub].reshape(tile, hid), NT) + dot(d_up, WB[l, 1, sub].reshape(tile, hid), NT)
            O[xp, :, :, pl.ds(j * tile, tile)] = part.reshape(-1, tok, tile)

    wx_start(0)
    x_copy.wait()
    dy_copy.wait()

    def normalize(l, rows, hidden):
        N[l, f, rows] = (hidden * rms(hidden) * gain_ref[l:l + 1]).astype(BF16)
    repeat(0, tok // chunk, lambda j: normalize(0, rows_at(0, j), H[0, rows_at(0, j)].astype(F32)))
    for l in range(last):
        gather = fwd[l]
        gather.start()
        if l == 0:
            for k in range(1, layers):
                wx_start(k)
            bwd[last].start()
            wy_start(0)
            gather.mid()
            wy_mid(0)
            for k in range(1, layers):
                wy_start(k)
            gather.near()
            gather.end()
            gather.far()
            bwd[last].mid()
        gather.wait(OWN)
        wy_end(l)
        wd_copies[l].wait()
        pairs(l, None if l == 0 else gather, functools.partial(forward, l), FORWARD)
        rs_start(l)
        if l == 0:
            bwd[last].near()
            bwd[last].end()
            bwd[last].far()
            bwd[last].wait(OWN)
            for k in range(1, layers):
                wy_mid(k)
        rs_mid(l)

        def next_hidden(rows, total, l=l):
            hidden = (H[l, rows].astype(F32) + total).astype(BF16)
            H[l + 1, rows] = hidden
            normalize(l + 1, rows, hidden.astype(F32))
        rs_end(l, next_hidden)

    for l in reversed(range(layers)):
        r = 2 * last - l
        gather = fwd[l] if l == last else bwd[l]
        gather.start()
        gather.wait(OWN)
        if l == last:
            wy_end(l)
            wd_copies[l].wait()
        pairs(r, gather, functools.partial(backward, l), FORWARD + BACKWARD if l == last else BACKWARD)
        rs_start(r)
        if l == 0:
            env.settle(last)
        down_grad(l)
        clock.busy(DOWN)
        env.begin(jobs[l, DOWN_PART])
        up_grad(l)
        clock.busy(2 * DOWN)
        env.begin(jobs[l, GATE_UP])
        rs_mid(r)
        bwd[l].drain()

        def next_cot(rows, total, l=l):
            d_normed = total.astype(BF16).astype(F32)
            hidden = H[l, rows].astype(F32)
            inv = rms(hidden)
            if l > 0:
                scaled = d_normed * gain_ref[l:l + 1]
                cot = DH[l % 2, f, rows].astype(F32)
                d_hidden = cot + inv * scaled - hidden * (inv * inv * inv) * jnp.mean(scaled * hidden, axis=-1, keepdims=True)
                DH[(l - 1) % 2, f, rows] = d_hidden.astype(BF16)
            gain_row[...] += jnp.sum(d_normed * hidden * inv, axis=0, keepdims=True)
        gain_row[...] = jnp.zeros((1, depth), F32)
        rs_end(r, next_cot)
        lanes = depth // LN
        for j in range(lanes):
            gain_buf[0, f, l * lanes + j:l * lanes + j + 1] = gain_row[:, j * LN:(j + 1) * LN]

    def gain_copy(stage, j):
        axis, pos, size = axes[stage]
        return pltpu.make_async_remote_copy(
            src_ref=gain_buf.at[stage, pos], dst_ref=gain_buf.at[stage, pos],
            send_sem=g_send.at[stage, j], recv_sem=g_recv.at[stage, pos],
            device_id=env.device(axis, j), device_id_type=LOGICAL)

    def gain_send(stage):
        for j in range(1, axes[stage][2]):
            gain_copy(stage, j).start()
        clock.after(clock.now + 2 * EXCHANGE, functools.partial(gain_sum, stage))

    def gain_sum(stage):
        axis, pos, size = axes[stage]
        for j in range(1, size):
            peer = env.near(axis, j)
            pltpu.make_async_remote_copy(
                src_ref=gain_buf.at[stage, peer], dst_ref=gain_buf.at[stage, peer],
                send_sem=g_send.at[stage, j], recv_sem=g_recv.at[stage, peer],
                device_id=env.device(axis, j), device_id_type=LOGICAL).wait_recv()
        total = gain_buf[stage, 0]
        for i in range(1, size):
            total = total + gain_buf[stage, i]
        if stage == 2:
            gain_out[...] = total
        else:
            gain_buf[stage + 1, axes[stage + 1][1]] = total
            gain_send(stage + 1)

    gain_send(0)

    for target in (partner, dev(1), dev(-1)):
        pl.semaphore_signal(credit, device_id=fid[id(target)], device_id_type=LOGICAL)
    r = 2 * layers - 1
    pl.semaphore_wait(credit, 3)
    pairs(r, None, lambda xp: product(xp, GA[last, xp], last), FORWARD)
    rs_start(r)
    rs_mid(r)

    def output(rows, total):
        H[0, rows] = (H[last, rows].astype(F32) + total).astype(BF16)
    rs_end(r, output)
    y_copy = pltpu.make_async_copy(H.at[0], y_ref, io_sem.at[2])
    y_copy.start()
    while clock.queue:
        clock.step()

    y_copy.wait()
    for gather in fwd:
        gather.drain()
    for l in range(layers):
        for m in BOTH:
            repeat(1, nf, lambda j: wx_copy(l, m, j, wrap(f + j, nf), f).wait_send())
            for kind in (FIRST, SECOND, PASS):
                for d in BOTH:
                    wy_copy(l, m, kind, d).wait_send()
    for job in jobs.values():
        job.wait_sends(True)
    for stage in range(3):
        for j in range(1, axes[stage][2]):
            gain_copy(stage, j).wait_send()
    pltpu.make_async_copy(G, out_ref, out_sem).wait()


def fused_step(x, dy, wg, wu, wd, gain, dims):
    layers, ny, nz, nf, tok, depth, hid = dims
    nx = nf // 2
    vm, hbm = pl.BlockSpec(memory_space=pltpu.VMEM), pl.BlockSpec(memory_space=pl.ANY)
    dma = pltpu.SemaphoreType.DMA
    blocks = (layers, ny, nz, 3 * nf, RS, LN)
    lines = layers * depth // LN
    steps = layers * 2 * 2 * (ny + nz)
    wide = max(nf, ny, nz)
    return pl.pallas_call(
        functools.partial(step_kernel, dims),
        out_shape=(jax.ShapeDtypeStruct((tok, depth), BF16), jax.ShapeDtypeStruct(blocks, F32), jax.ShapeDtypeStruct((lines, LN), F32)),
        in_specs=[hbm, hbm, hbm, hbm, hbm, vm],
        out_specs=(hbm, hbm, vm),
        scratch_shapes=[
            pltpu.VMEM((layers, 2, nf, depth // nf, hid), BF16),
            pltpu.VMEM((layers, hid, depth), BF16),
            pltpu.VMEM((layers, nf, tok, depth), BF16),
            pltpu.VMEM((layers, nx, 2 * tok, hid), BF16),
            pltpu.VMEM((layers, nx, 2 * tok, hid), BF16),
            pltpu.VMEM((2, nf, tok, depth), BF16),
            pltpu.VMEM((nx, 2, tok, depth), F32),
            pltpu.VMEM((nx, tok, depth), F32),
            pltpu.VMEM((2, 3, tok // 2, depth), F32),
            pltpu.VMEM((layers, tok, depth), BF16),
            pltpu.VMEM((2, nx, 2 * tok, hid), BF16),
            pltpu.VMEM(blocks, F32),
            pltpu.VMEM(blocks[1:], F32),
            pltpu.VMEM((layers, 2 * nf, RS, LN), F32),
            pltpu.VMEM((3, wide, lines, LN), F32),
            pltpu.VMEM((1, depth), F32),
            dma((2 * layers, OWN + 1, 2)), dma((2 * layers, OWN + 1, 2)),
            dma((2 * layers, 12)), dma((2 * layers, 12)),
            dma((layers, 2, nf)), dma((layers, 2, nf)),
            dma((layers, 2, PASS + 1, 2)), dma((layers, 2, PASS + 1, 2)),
            dma((layers, 2)), dma((layers,)),
            dma((steps + 8 * layers * 2,)), dma((steps + 8 * layers * 2,)), dma((steps,)), dma((steps,)),
            dma((layers, 2, nf)), dma((layers, 2, nf)),
            dma((3, wide)), dma((3, wide)), dma, dma((3,)),
            pltpu.SemaphoreType.REGULAR((layers, 2)), pltpu.SemaphoreType.REGULAR,
        ],
        compiler_params=pltpu.CompilerParams(collective_id=0, has_side_effects=True, vmem_limit_bytes=67043328),
        name="fused_step",
    )(x, dy, wg, wu, wd, gain)


def unpack_kernel(g_ref, gate_ref, up_ref, down_ref):
    ny, nzb, units = g_ref.shape[:3]
    nf = units // 3
    for k in range(nzb):
        for i in range(ny):
            for m, ref in enumerate((gate_ref, up_ref)):
                for j in range(nf):
                    col = (j * ny + i) * LN
                    ref[k * RS:(k + 1) * RS, col:col + LN] = g_ref[i, k, m * nf + j]
            for h in BOTH:
                for r in range(nf // 2):
                    row, col = (k * (nf // 2) + r) * RS, (2 * i + h) * LN
                    down_ref[row:row + RS, col:col + LN] = g_ref[i, k, 2 * nf + h * (nf // 2) + r]


def unpack(out, dims, steps=2):
    layers, ny, nz, nf = dims
    nzb = nz // steps
    wide, tall = nf * ny * LN, (nf // 2) * RS
    return pl.pallas_call(
        unpack_kernel, grid=(layers, steps),
        in_specs=[pl.BlockSpec((None, ny, nzb, 3 * nf, RS, LN), lambda l, z: (l, 0, z, 0, 0, 0))],
        out_specs=[pl.BlockSpec((None, nzb * RS, wide), lambda l, z: (l, z, 0))] * 2
        + [pl.BlockSpec((None, nzb * tall, 2 * ny * LN), lambda l, z: (l, z, 0))],
        out_shape=[jax.ShapeDtypeStruct((layers, nz * RS, wide), F32)] * 2
        + [jax.ShapeDtypeStruct((layers, nz * tall, 2 * ny * LN), F32)],
        name="unpack")(out)


TOKEN_AXES = ("dp", "replica", "fsdp")


def solution(mesh):
    ny, nz, nf = mesh.shape["replica"], mesh.shape["dp"], mesh.shape["fsdp"]
    tok_spec, shard_spec, full_spec = P(TOKEN_AXES, None), P(None, "fsdp", None), P(None, None)

    def device_step(x, dy, wg, wu, wd, gain):
        layers, depth = gain.shape
        dims = (layers, ny, nz, nf)
        out, blocks, gain_sum = fused_step(x, dy, wg, wu, wd, gain, dims + (x.shape[0], depth, wd.shape[1]))
        dw_gate, dw_up, dw_down = unpack(blocks, dims)
        return out, dw_gate, dw_up, dw_down, gain_sum.reshape(gain.shape)

    return jax.shard_map(
        device_step, mesh=mesh, in_specs=(tok_spec, tok_spec, shard_spec, shard_spec, shard_spec, full_spec),
        out_specs=(tok_spec, shard_spec, shard_spec, shard_spec, full_spec), check_vma=False)
```

```python
import functools
import heapq
import jax
import jax.numpy as jnp
from jax import lax
from jax.sharding import PartitionSpec as P
from jax.experimental import pallas as pl
from jax.experimental.pallas import tpu as pltpu

F32 = jnp.float32
BF16 = jnp.bfloat16
LOGICAL = pl.DeviceIdType.LOGICAL
RS, LN = 16, 128
UNIT_BYTES = RS * LN * 4
NORM_EPS = 1e-6
NN = (((1,), (0,)), ((), ()))
NT = (((1,), (1,)), ((), ()))
TN = (((0,), (0,)), ((), ()))
LINK_RATE, CORE_RATE, HOP, CORE_HOP, STEP_COST, HBM_READ, ENTRY = 46.6e3, 500e3, 2.2, 0.9, 0.15, 1.1, 3.5
CORES = "cores"
BOTH, SIGN, BF16_BYTES = (0, 1), (1, -1), 2
FIRST, SECOND, PASS, RELAY, FAR, OWN = range(6)
DIRECT = "direct"
FORWARD, BACKWARD, WEIGHT, ADD, EXCHANGE = 1.2, 1.7, 2.2, 0.2, 5.0


def dot(a, b, dims=NN):
    return lax.dot_general(a, b, dims, preferred_element_type=F32)


def repeat(start, stop, work):
    def step(i, carry):
        work(i)
        return carry
    lax.fori_loop(start, stop, step, 0)


def wrap(value, size):
    return lax.rem(value + 4 * size, size)


class Clock:
    def __init__(self):
        self.now, self.queue, self.count, self.links = 0.0, [], 0, {}

    def send(self, link, size):
        near = link == CORES
        start = max(self.now, self.links.get(link, 0.0))
        self.links[link] = start + size / (CORE_RATE if near else LINK_RATE)
        return self.links[link] + (CORE_HOP if near else HOP)

    def after(self, ready, work):
        self.count += 1
        heapq.heappush(self.queue, (ready, self.count, work))

    def step(self):
        ready, _, work = heapq.heappop(self.queue)
        self.now = max(self.now, ready) + STEP_COST
        work()

    def run(self, until):
        while self.queue and self.queue[0][0] <= until:
            self.step()

    def busy(self, spent):
        self.now += spent
        self.run(self.now)

    def idle(self, until):
        self.run(until)
        self.now = max(self.now, until)


class Job:
    def __init__(self, env, layer, part):
        sizes = PART_SIZES[part]
        start = part * env.nf
        offsets = [sum(p[k] for p in PART_SIZES[:part]) for k in BOTH]
        swap = () if part == DOWN else (part,)
        self.env, self.layer, self.part, self.swap = env, layer, part, swap
        self.sizes, self.offsets, self.starts = sizes, offsets, (start, start + sizes[0])
        self.units = pl.ds(start, sum(sizes))
        self.left, self.turned, self.arrived, self.early = 2, 0, {}, {}
        rings = (env.ny // 2, env.nz // 2)
        self.slots = {}
        for gather in (False, True):
            for phase in BOTH:
                for k in BOTH:
                    for d in BOTH:
                        half = rings[phase ^ k]
                        self.slots[gather, phase, k, d] = env.slots[gather]
                        env.slots[gather] += half if gather else half + 1

    def ring(self, phase, k):
        return ("replica", "dp")[phase ^ k]

    def half_ring(self, phase, k):
        return self.env.size[self.ring(phase, k)] // 2

    def block(self, phase, k, index, side=None):
        env, G, layer = self.env, self.env.G, self.layer
        start, size = self.starts[k], self.sizes[k]
        if side is not None:
            start, size = start + side * (size // 2), size // 2
        units = pl.ds(start, size)
        if phase == 0:
            return G.at[layer, index, :, units] if k == 0 else G.at[layer, :, index, units]
        return G.at[layer, env.y, index, units] if k == 0 else G.at[layer, index, env.z, units]

    def stage(self, phase, k, d, step, side=None):
        env = self.env
        ref, lead = (env.G, (0,)) if self.layer == env.last else (env.S, ())
        first = 0 if k == 0 else env.split
        offset, size = self.offsets[k], self.sizes[k]
        half_total = ((env.units - env.split) if k else env.split) // 2
        at = 2 * (step - 1) + d
        if step == 0:
            units = pl.ds(first + d * half_total + offset // 2, size // 2)
            at = env.nz - 2 if self.ring(phase, k) == "dp" else 2
        elif side is None:
            units = pl.ds(first + offset, size)
        else:
            units = pl.ds(first + offset + side * (size // 2), size // 2)
        every = slice(None)
        if phase == 0:
            place = (at, every) if k == 0 else (every, at)
        else:
            place = (env.ny - 1, at) if k == 0 else (at, env.nz - 1)
        return ref.at[(*lead, *place, units)]

    def copy(self, gather, phase, k, d, slot, src, dst):
        env = self.env
        send, recv = (env.ag_send, env.ag_recv) if gather else (env.rs_send, env.rs_recv)
        slot = self.slots[gather, phase, k, d] + slot
        return pltpu.make_async_remote_copy(
            src_ref=src, dst_ref=dst, send_sem=send.at[slot], recv_sem=recv.at[slot],
            device_id=env.device(self.ring(phase, k), SIGN[d]), device_id_type=LOGICAL)

    def send_time(self, phase, k, d, units):
        env = self.env
        other = (env.nz if k == 0 else env.ny) if phase == 0 else 1
        return env.clock.send((self.ring(phase, k), d), units * other * UNIT_BYTES)

    def piece(self, phase, k, d, step, early):
        if step == 0:
            return 0, d
        if step == 1:
            return (1, 1 - d) if early else (2, d)
        return step + 1, None

    def reduce_copy(self, phase, k, d, step, early=False):
        slot, side = self.piece(phase, k, d, step, early)
        index = self.env.near(self.ring(phase, k), SIGN[d] * (self.half_ring(phase, k) - step))
        stage = self.stage(phase, k, d, step, None if step == 0 else side)
        return self.copy(False, phase, k, d, slot, self.block(phase, k, index, side), stage)

    def reduce_send(self, phase, k, d, step, early=False):
        self.reduce_copy(phase, k, d, step, early).start()
        ready = self.send_time(phase, k, d, self.sizes[k] if step > 1 else self.sizes[k] // 2)
        if early:
            self.early[phase, k, d] = ready
        else:
            if step == 1:
                ready = max(ready, self.early[phase, k, d])
            self.env.clock.after(ready, functools.partial(self.reduce_step, phase, k, d, step))

    def reduce_start(self, phase, k):
        for d in BOTH:
            self.reduce_send(phase, k, d, 0)
        for d in BOTH:
            self.reduce_send(phase, k, d, 1, True)

    def start(self, phase, k):
        env = self.env
        if phase == 0 and k == 0 and env.above(self):
            pl.semaphore_wait(env.freed.at[env.above(self)], 4)
        self.reduce_start(phase, k)

    def reduce_step(self, phase, k, d, step):
        half = self.half_ring(phase, k)
        if step == 1:
            self.reduce_copy(phase, k, d, step, True).wait_recv()
        self.reduce_copy(phase, k, d, step).wait_recv()
        index = self.env.near(self.ring(phase, k), SIGN[d] * (half - 1 - step))
        self.block(phase, k, index, d if step == 0 else None)[...] += self.stage(phase, k, d, step)[...]
        if step + 1 < half:
            self.reduce_send(phase, k, d, step + 1)
        elif self.both(False, phase, k):
            if phase == 0:
                self.halfway()
                self.env.begin(self, 1, k)
            else:
                self.left -= 1
                if self.left == 0:
                    self.reduced()

    def halfway(self):
        env, here = self.env, (self.layer, self.part)
        self.turned += 1
        if self.turned == len(BOTH):
            if 0 < self.layer < env.last:
                self.tell(env.freed)
            env.half.add(here)
            env.begin_waiting()

    def tell(self, flags):
        for axis in ("replica", "dp"):
            for sign in SIGN:
                pl.semaphore_signal(flags.at[self.layer, self.part], device_id=self.env.device(axis, sign), device_id_type=LOGICAL)

    def both(self, gather, phase, k):
        key = gather, phase, k
        self.arrived[key] = self.arrived.get(key, 0) + 1
        return self.arrived[key] == 2

    def wait_sends(self, gather):
        for phase in BOTH:
            for k in BOTH:
                half = self.half_ring(phase, k)
                for d in BOTH:
                    some, all_units = self.block(phase, k, 0, d), self.block(phase, k, 0)

                    def done(slot, view):
                        self.copy(gather, phase, k, d, slot, view, view).wait_send()
                    if gather:
                        repeat(0, half - 1, lambda slot: done(slot, all_units))
                        done(half - 1, some)
                    else:
                        repeat(0, 3, lambda slot: done(slot, some))
                        if half > 2:
                            repeat(3, half + 1, lambda slot: done(slot, all_units))

    def x_copy(self, m, j, peer, sender):
        env = self.env
        lane = (2 * self.layer + m) * env.nf
        return pltpu.make_async_remote_copy(
            src_ref=env.G.at[self.layer, env.y, env.z, m * env.nf + peer], dst_ref=env.R.at[self.layer, m * env.nf + sender],
            send_sem=env.x_send.at[lane + j], recv_sem=env.x_recv.at[lane + sender],
            device_id=env.row + peer, device_id_type=LOGICAL)

    def reduced(self):
        env = self.env
        self.wait_sends(False)
        self.tell(env.ready)
        for m in self.swap:
            repeat(1, env.nf, lambda j: self.x_copy(m, j, wrap(env.f + j, env.nf), env.f).start())
        env.reduced.add((self.layer, self.part))
        env.clock.after(env.clock.now + (EXCHANGE if self.swap else HOP), self.exchanged)

    def exchanged(self):
        env = self.env
        f, nf = env.f, env.nf
        for m in self.swap:
            env.R[self.layer, m * nf + f] = env.G[self.layer, env.y, env.z, m * nf + f]
        for m in self.swap:
            repeat(1, nf, lambda j: self.x_copy(m, j, wrap(f + j, nf), f).wait_send())
            repeat(1, nf, lambda j: self.x_copy(m, j, wrap(f + j, nf), wrap(f + j, nf)).wait_recv())
        for m in self.swap:
            env.G[self.layer, env.y, env.z, pl.ds(m * nf, nf)] = env.R[self.layer, pl.ds(m * nf, nf)]
        pl.semaphore_wait(env.ready.at[self.layer, self.part], 4)
        self.left = 2
        for k in BOTH:
            self.gather_start(1, k)
        env.exchanged.add((self.layer, self.part))
        env.begin_waiting()

    def gather_copy(self, phase, k, d, step, index):
        side = d if step + 1 == self.half_ring(phase, k) else None
        view = self.block(phase, k, self.env.near(self.ring(phase, k), index), side)
        return self.copy(True, phase, k, d, step, view, view)

    def gather_send(self, phase, k, d, step):
        self.gather_copy(phase, k, d, step, -SIGN[d] * step).start()
        units = self.sizes[k] if step + 1 < self.half_ring(phase, k) else self.sizes[k] // 2
        ready = self.send_time(phase, k, d, units)
        self.env.clock.after(ready, functools.partial(self.gather_step, phase, k, d, step))

    def gather_start(self, phase, k):
        for d in BOTH:
            self.gather_send(phase, k, d, 0)

    def gather_step(self, phase, k, d, step):
        env = self.env
        self.gather_copy(phase, k, d, step, -SIGN[d] * (step + 1)).wait_recv()
        if step + 1 < self.half_ring(phase, k):
            self.gather_send(phase, k, d, step + 1)
        elif self.both(True, phase, k):
            if phase == 1:
                self.gather_start(0, k)
            else:
                self.left -= 1
                if self.left == 0:
                    here = (self.layer, slice(None), slice(None), self.units)
                    pltpu.make_async_copy(env.G.at[here], env.out_ref.at[here], env.out_sem).start()


class Env:
    def __init__(self, dims):
        self.exchanged, self.reduced, self.half, self.waiting, self.clock = set(), set(), set(), [], Clock()
        self.slots = {False: 0, True: 0}
        self.ny, self.nz, self.nf = dims[1:4]
        self.last = dims[0] - 1
        self.f, self.y, self.z = lax.axis_index("fsdp"), lax.axis_index("replica"), lax.axis_index("dp")
        self.size = {"fsdp": self.nf, "replica": self.ny, "dp": self.nz}
        self.pos = {"fsdp": self.f, "replica": self.y, "dp": self.z}
        stride = {"fsdp": 1, "replica": self.nf, "dp": self.nf * self.ny}
        me = self.f + stride["replica"] * self.y + stride["dp"] * self.z
        self.row = me - self.f
        self.shift = {a: [wrap(self.pos[a] + k, n) for k in range(n)] for a, n in self.size.items()}
        self.ids = {a: [me + (p - self.pos[a]) * stride[a] for p in self.shift[a]] for a in self.size}

    def near(self, axis, k):
        return self.shift[axis][k % self.size[axis]]

    def device(self, axis, k):
        return self.ids[axis][k % self.size[axis]]

    def above(self, job):
        return (job.layer + 1, job.part) if job.layer + 1 < self.last else None

    def begin(self, job, phase, k):
        self.waiting.append((job, phase, k))
        self.begin_waiting()

    def begin_job(self, job):
        for k in BOTH:
            self.begin(job, 0, k)

    def begin_waiting(self):
        for item in list(self.waiting):
            job, phase, k = item
            if item in self.waiting and (not self.above(job) or self.above(job) in (self.exchanged if phase else self.half)):
                self.waiting.remove(item)
                job.start(phase, k)

    def settle(self, layer):
        while not {(layer, part) for part in (GATE, UP, DOWN)} <= self.reduced:
            self.clock.step()


GATE, UP, DOWN = range(3)
PART_SIZES = ((6, 2), (4, 4), (4, 4))


def step_kernel(dims, x_ref, dy_ref, wg_ref, wu_ref, wd_ref, gain_ref, y_ref, out_ref, gain_out,
                WB, WD, N, GA, UA, DH, O, DS, MS, H, DGU, G, S, R, gain_buf, gain_row,
                ag_send, ag_recv, rs_send, rs_recv, wx_send, wx_recv, wy_send, wy_recv, w_sem, wd_sem,
                jr_send, jr_recv, jg_send, jg_recv, x_send, x_recv, g_send, g_recv, out_sem, io_sem, ready, freed, credit):
    layers, ny, nz, nf, tok, depth, hid = dims
    nx, half, q = nf // 2, tok // 2, depth // nf // ny
    tile = min(256, depth)
    last = layers - 1

    env = Env(dims)
    f, y, z = env.f, env.y, env.z
    x, c = f // 2, f % 2
    env.G, env.S, env.R, env.out_ref = G, S, R, out_ref
    env.rs_send, env.rs_recv, env.ag_send, env.ag_recv = jr_send, jr_recv, jg_send, jg_recv
    env.x_send, env.x_recv, env.ready, env.freed, env.out_sem = x_send, x_recv, ready, freed, out_sem
    env.units, env.split = 3 * nf, sum(sizes[0] for sizes in PART_SIZES)
    clock = env.clock
    jobs = {}
    for l in reversed(range(layers)):
        for part in (GATE, UP, DOWN):
            jobs[l, part] = Job(env, l, part)

    chips = [wrap(x + k, nx) for k in range(nx)]
    same, opposite_core = [2 * p + c for p in chips], [2 * p + (1 - c) for p in chips]
    fid = {id(v): env.row + v for v in same + opposite_core}

    def dev(off, opposite=False):
        return (opposite_core if opposite else same)[off % nx]

    partner = dev(0, True)
    halves = (pl.ds(0, half), pl.ds(half, half))
    whole = pl.ds(0, tok)
    axes = [("fsdp", f, nf), ("replica", y, ny), ("dp", z, nz)]

    barrier = pltpu.get_barrier_semaphore()
    for axis, pos, size in axes:
        for j in range(1, size):
            pl.semaphore_signal(barrier, device_id=env.device(axis, j), device_id_type=LOGICAL)

    x_copy = pltpu.make_async_copy(x_ref, H.at[0], io_sem.at[0])
    dy_copy = pltpu.make_async_copy(dy_ref, DH.at[last % 2, f], io_sem.at[1])
    x_copy.start()
    dy_copy.start()
    wd_copies = [pltpu.make_async_copy(wd_ref.at[l], WD.at[l], wd_sem.at[l]) for l in range(layers)]
    weights = (wg_ref, wu_ref)
    y_at = [env.near("replica", k) for k in range(ny)]
    parts = (pl.ds(0, nf // 2), pl.ds(nf // 2, nf // 2))
    direct = pl.ds(ny * q // 2, ny * q // 2)
    direct_lane = 2 * layers * nf
    shared = {}

    def share(l, m, hops=0):
        size = q // 2 if (l, m) == BOTH else q
        return pl.ds(y_at[hops % ny] * size, size)

    def own_rows(l, m, rows, sem):
        src = weights[m].at[l, rows, pl.ds(pl.multiple_of(f * hid, hid), hid)]
        return pltpu.make_async_copy(src, WB.at[l, m, f, rows], w_sem.at[sem])

    own_copies = {(l, m): own_rows(l, m, share(l, m), 2 * l + m) for l in range(layers) for m in BOTH}
    own_copies[DIRECT] = own_rows(*BOTH, direct, 2 * layers)
    for copy in own_copies.values():
        copy.start()
    for copy in wd_copies:
        copy.start()
    pl.semaphore_wait(barrier, nf + ny + nz - 3)
    clock.busy(ENTRY)

    def wx_copy(l, m, j, peer, sender, rows, lane):
        return pltpu.make_async_remote_copy(
            src_ref=weights[m].at[l, rows, pl.ds(pl.multiple_of(peer * hid, hid), hid)], dst_ref=WB.at[l, m, sender, rows],
            send_sem=wx_send.at[lane + j], recv_sem=wx_recv.at[lane + sender], device_id=env.row + peer, device_id_type=LOGICAL)

    def wx_sets(l):
        return [(l, m, share(l, m), (2 * l + m) * nf) for m in BOTH]

    def wx_post(key, l, m, rows, lane):
        repeat(1, nf, lambda j: wx_copy(l, m, j, wrap(f + j, nf), f, rows, lane).start())
        for d in BOTH:
            shared[key] = clock.send(d, nx * rows.size * hid * BF16_BYTES) + HBM_READ

    def wx_take(key, l, m, rows, lane):
        clock.idle(shared[key])
        own_copies[key].wait()
        repeat(1, nf, lambda j: wx_copy(l, m, j, wrap(f + j, nf), wrap(f + j, nf), rows, lane).wait_recv())

    def wx_start(l):
        for args in wx_sets(l):
            wx_post(args[:2], *args)

    def wy_copy(l, m, kind, d, arrived=False):
        hops = (kind == PASS) + arrived
        lane = ((2 * l + m) * (PASS + 1) + kind) * 2 + d
        part = parts[BOTH[d - (kind == SECOND)]]
        view = WB.at[l, m, part, share(l, m, -SIGN[d] * hops)]
        return pltpu.make_async_remote_copy(
            src_ref=view, dst_ref=view, send_sem=wy_send.at[lane], recv_sem=wy_recv.at[lane],
            device_id=env.device("replica", SIGN[d]), device_id_type=LOGICAL)

    def wy_each(l, kinds, work):
        for m in BOTH:
            for kind in kinds:
                for d in BOTH:
                    work(l, m, kind, d)

    def wy_send_one(l, m, kind, d):
        wy_copy(l, m, kind, d).start()
        shared[l, m, kind, d] = clock.send(("replica", d), nf // 2 * share(l, m).size * hid * BF16_BYTES)

    def wy_take(*args):
        clock.idle(shared[args])
        wy_copy(*args, True).wait_recv()

    def wy_start(l):
        for args in wx_sets(l):
            wx_take(args[:2], *args)
            for kind in (FIRST, SECOND):
                for d in BOTH:
                    wy_send_one(*args[:2], kind, d)

    def wy_mid(l):
        for m in BOTH:
            for d in BOTH:
                wy_take(l, m, FIRST, d)
                wy_send_one(l, m, PASS, d)

    def wy_end(l):
        wy_each(l, (SECOND, PASS), wy_take)

    class Gather:
        def __init__(self, r, buf, slot):
            self.r, self.buf, self.slot, self.ready = r, buf, slot, {}

        def copy(self, kind, d, arrived=False):
            hops = (kind in (PASS, RELAY)) + (kind == FAR) * nx // len(BOTH)
            local = kind in (RELAY, FAR, OWN)
            block = dev(-SIGN[d] * (hops + (arrived and not local)), arrived and local)
            rows = whole if kind in (RELAY, OWN) else halves[d - (kind == SECOND)]
            target = partner if local else dev(SIGN[d])
            lane = (self.r * (OWN + 1) + kind) * 2 + d
            view = self.buf.at[self.slot, block, rows]
            return rows.size, pltpu.make_async_remote_copy(
                src_ref=view, dst_ref=view, send_sem=ag_send.at[lane], recv_sem=ag_recv.at[lane],
                device_id=fid[id(target)], device_id_type=LOGICAL)

        def send(self, kind, d):
            size, copy = self.copy(kind, d)
            copy.start()
            self.ready[kind, d] = clock.send(CORES if kind in (RELAY, FAR, OWN) else d, size * depth * BF16_BYTES)

        def wait(self, kind, d=0):
            clock.idle(self.ready[kind, d])
            self.copy(kind, d, True)[-1].wait_recv()

        def start(self):
            for kind in (FIRST, OWN, SECOND):
                for d in BOTH[:1] if kind == OWN else BOTH:
                    self.send(kind, d)

        def forward(self, kind, onward):
            for d in BOTH:
                self.wait(kind, d)
                self.send(onward, d)

        def mid(self):
            self.forward(FIRST, PASS)
            self.forward(SECOND, RELAY)

        def end(self):
            self.forward(PASS, FAR)

        def take(self, kind):
            for d in BOTH:
                self.wait(kind, d)

        def near(self):
            self.take(RELAY)

        def far(self):
            self.take(FAR)

        def drain(self):
            for kind, d in self.ready:
                self.copy(kind, d)[-1].wait_send()

    def rs_d2d(r, i, xp, core):
        return pltpu.make_async_remote_copy(
            src_ref=O.at[xp, core], dst_ref=DS.at[xp], send_sem=rs_send.at[12 * r + i], recv_sem=rs_recv.at[12 * r + i],
            device_id=fid[id(partner)], device_id_type=LOGICAL)

    quarter = half // 2
    chunk = min(16, half)
    arrive = {}

    def rs_msg(r, k, d):
        lane = 12 * r + 4 + 2 * k + d
        off, side = (2, d) if k == 0 else (SIGN[d], d if k == 3 else 1 - d)
        start, size, slot, at = side * half, half, (0 if k == 0 else 2), 0
        if k in (1, 2):
            at = (k - 1) * quarter
            start, size, slot = side * half + at, quarter, 1
        return pltpu.make_async_remote_copy(
            src_ref=O.at[chips[off % nx], c, pl.ds(start, size)], dst_ref=MS.at[d, slot, pl.ds(at, size)],
            send_sem=rs_send.at[lane], recv_sem=rs_recv.at[lane],
            device_id=fid[id(dev(SIGN[d]))], device_id_type=LOGICAL)

    def rs_post(r, k, d):
        rs_msg(r, k, d).start()
        arrive[k, d] = clock.send(d, (quarter if k in (1, 2) else half) * depth * 4)

    def rs_take(r, k, d):
        clock.idle(arrive[k, d])
        rs_msg(r, k, d).wait_recv()

    def rows_at(start, j):
        return pl.ds(pl.multiple_of(start + j * chunk, chunk), chunk)

    def combine(r, i, off):
        xp = chips[off % nx]
        clock.idle(arrive[i])
        rs_d2d(r, i, xp, c).wait_recv()

        def add(j):
            rows = rows_at(0, j)
            O[xp, c, rows] += DS[xp, rows]
        repeat(0, tok // chunk, add)
        clock.busy(ADD)

    def rs_near(r):
        for i, d in ((1, 0), (2, 1)):
            combine(r, i, SIGN[d])
            rs_post(r, 1, d)

    def rs_start(r):
        combine(r, 3, 2)
        for k in (0, 2):
            for d in BOTH:
                rs_post(r, k, d)
        combine(r, 0, 0)

    def rs_mid(r):
        for d in BOTH:
            rs_take(r, 0, d)

            def add(j):
                rows = rows_at(d * half, j)
                O[chips[SIGN[d] % nx], c, rows] += MS[d, 0, rows_at(0, j)]
            repeat(0, half // chunk, add)
            rs_post(r, 3, d)

    def rs_end(r, body):
        for k in (1, 2, 3):
            for d in BOTH:
                rs_take(r, k, d)
        for side in BOTH:
            def step(j):
                rows, local = rows_at(side * half, j), rows_at(0, j)
                body(rows, O[x, c, rows] + (MS[0, 2 - side, local] + MS[1, 1 + side, local]))
            repeat(0, half // chunk, step)
        clock.busy(5 * ADD)
        for i in range(nx):
            rs_d2d(r, i, x, 1 - c).wait_send()
        for k in range(4):
            for d in BOTH:
                rs_msg(r, k, d).wait_send()

    def pairs(r, gather, body, cost, after_mid=None):
        def step(i):
            xp = wrap(x + i + i // 2 - 2 * (i // 3), nx)
            body(xp)
            rs_d2d(r, i, xp, 1 - c).start()

        def go(first, stop):
            repeat(first, stop, step)
            for i in range(first, stop):
                clock.now += cost
                arrive[i] = clock.send(CORES, tok * depth * 4)
            clock.busy(0.0)

        go(0, 1)
        if gather:
            gather.mid()
            if after_mid:
                after_mid()
            gather.near()
        go(1, 3)
        if gather:
            gather.end()
        rs_near(r)
        if gather:
            gather.far()
        go(3, nx)

    def rms(hidden):
        return lax.rsqrt(jnp.mean(hidden * hidden, axis=-1, keepdims=True) + NORM_EPS)

    def down_grad(l):
        group = nf // 2
        zs = tile // (group * RS)

        def body(j, carry):
            lhs = GA[l, :, :, pl.ds(pl.multiple_of(j * tile, tile), tile)].reshape(-1, tile)
            for i in range(depth // tile):
                res = dot(lhs, DH[l % 2, :, :, pl.ds(i * tile, tile)].reshape(-1, tile), TN)
                for h in range(tile // LN):
                    col = i * (tile // LN) + h
                    for zi in range(zs):
                        rows = res[zi * group * RS:(zi + 1) * group * RS, h * LN:(h + 1) * LN]
                        G[l, col // 2, j * zs + zi, pl.ds(2 * nf + (col % 2) * group, group)] = rows.reshape(group, RS, LN)
            return carry
        lax.fori_loop(0, hid // tile, body, 0)

    def up_grad(l):
        fs = tile // (nz_rows * RS)

        def body(j, carry):
            lhs = N[l, :, :, pl.ds(pl.multiple_of(j * tile, tile), tile)].reshape(-1, tile)
            for m in BOTH:
                for i in range(hid // tile):
                    res = dot(lhs, DGU[m, :, :, pl.ds(i * tile, tile)].reshape(-1, tile), TN)
                    for h in range(tile // LN):
                        for fi in range(fs):
                            rows = res[fi * nz_rows * RS:(fi + 1) * nz_rows * RS, h * LN:(h + 1) * LN]
                            G[l, i * (tile // LN) + h, :, m * nf + j * fs + fi] = rows.reshape(nz_rows, RS, LN)
            return carry
        lax.fori_loop(0, depth // tile, body, 0)

    nz_rows = depth // nf // RS
    fwd = [Gather(l, N, l) for l in range(layers)]
    bwd = [Gather(2 * layers - 1 - l, DH, l % 2) for l in range(layers)]

    def activations(l, xp, cols):
        tokens = N[l, pl.ds(2 * xp, 2)].reshape(-1, depth)
        gate = dot(tokens, WB[l, 0, :, :, cols].reshape(depth, tile)).astype(BF16)
        up = dot(tokens, WB[l, 1, :, :, cols].reshape(depth, tile)).astype(BF16)
        return gate, up

    def product(xp, prod, l):
        for j in range(depth // tile):
            cols = pl.ds(j * tile, tile)
            O[xp, :, :, cols] = dot(prod, WD[l, :, cols]).reshape(-1, tok, tile)

    def forward(l, xp):
        for j in range(hid // tile):
            cols = pl.ds(j * tile, tile)
            gate, up = activations(l, xp, cols)
            GA[l, xp, :, cols] = gate
            UA[l, xp, :, cols] = up
            DGU[0, xp, :, cols] = (jax.nn.silu(gate.astype(F32)) * up.astype(F32)).astype(BF16)
        product(xp, DGU[0, xp], l)

    def backward(l, xp):
        cot = DH[l % 2, pl.ds(2 * xp, 2)].reshape(-1, depth)
        for j in range(hid // tile):
            cols = pl.ds(j * tile, tile)
            gate, up = activations(l, xp, cols) if l == last else (GA[l, xp, :, cols], UA[l, xp, :, cols])
            gate, up = gate.astype(F32), up.astype(F32)
            d_prod = dot(cot, WD[l, cols, :], NT).astype(BF16).astype(F32)
            sig = jax.nn.sigmoid(gate)
            GA[l, xp, :, cols] = (gate * sig * up).astype(BF16)
            DGU[0, xp, :, cols] = (d_prod * up * sig * (1.0 + gate * (1.0 - sig))).astype(BF16)
            DGU[1, xp, :, cols] = (d_prod * gate * sig).astype(BF16)
        d_gate, d_up = DGU[0, xp], DGU[1, xp]
        rows = depth // nf
        for j in range(depth // tile):
            sub = pl.ds(j * tile // rows, tile // rows)
            part = dot(d_gate, WB[l, 0, sub].reshape(tile, hid), NT) + dot(d_up, WB[l, 1, sub].reshape(tile, hid), NT)
            O[xp, :, :, pl.ds(j * tile, tile)] = part.reshape(-1, tok, tile)

    wx_start(0)
    x_copy.wait()
    dy_copy.wait()

    def normalize(l, rows, hidden):
        N[l, f, rows] = (hidden * rms(hidden) * gain_ref[l:l + 1]).astype(BF16)
    repeat(0, tok // chunk, lambda j: normalize(0, rows_at(0, j), H[0, rows_at(0, j)].astype(F32)))
    clock.busy(5 * ADD)
    straight = DIRECT, *BOTH, direct, direct_lane
    for l in range(last):
        gather = fwd[l]
        gather.start()
        if l == 0:
            wx_post(*straight)
            wy_start(0)
            gather.mid()
            wy_mid(0)
            for k in range(1, layers):
                wx_start(k)
            gather.near()
            gather.end()
            gather.far()
            wx_take(*straight)
        gather.wait(OWN)
        wy_end(l)
        wd_copies[l].wait()
        pairs(l, gather if l else None, functools.partial(forward, l), FORWARD, bwd[last].start if l == last - 1 else None)
        rs_start(l)
        wy_start(l + 1)
        rs_mid(l)
        wy_mid(l + 1)
        if l == last - 1:
            bwd[last].mid()

        def next_hidden(rows, total, l=l):
            hidden = (H[l, rows].astype(F32) + total).astype(BF16)
            H[l + 1, rows] = hidden
            normalize(l + 1, rows, hidden.astype(F32))
        rs_end(l, next_hidden)

    for l in reversed(range(layers)):
        r = 2 * last - l
        gather = fwd[l] if l == last else bwd[l]
        gather.start()
        gather.wait(OWN)
        if l == last:
            bwd[l].near()
            bwd[l].end()
            bwd[l].far()
            bwd[l].wait(OWN)
            wy_end(l)
            wd_copies[l].wait()
        pairs(r, gather, functools.partial(backward, l), FORWARD + BACKWARD if l == last else BACKWARD)
        rs_start(r)
        if l == 0:
            env.settle(last)
        down_grad(l)
        clock.busy(WEIGHT)
        env.begin_job(jobs[l, DOWN])
        up_grad(l)
        clock.busy(2 * WEIGHT)
        env.begin_job(jobs[l, GATE])
        env.begin_job(jobs[l, UP])
        rs_mid(r)
        bwd[l].drain()

        def next_cot(rows, total, l=l):
            d_normed = total.astype(BF16).astype(F32)
            hidden = H[l, rows].astype(F32)
            inv = rms(hidden)
            if l > 0:
                scaled = d_normed * gain_ref[l:l + 1]
                cot = DH[l % 2, f, rows].astype(F32)
                d_hidden = cot + inv * scaled - hidden * (inv * inv * inv) * jnp.mean(scaled * hidden, axis=-1, keepdims=True)
                DH[(l - 1) % 2, f, rows] = d_hidden.astype(BF16)
            gain_row[...] += jnp.sum(d_normed * hidden * inv, axis=0, keepdims=True)
        gain_row[...] = jnp.zeros((1, depth), F32)
        rs_end(r, next_cot)
        lanes = depth // LN
        for j in range(lanes):
            gain_buf[0, f, l * lanes + j:l * lanes + j + 1] = gain_row[:, j * LN:(j + 1) * LN]

    def gain_copy(stage, j):
        axis, pos, size = axes[stage]
        return pltpu.make_async_remote_copy(
            src_ref=gain_buf.at[stage, pos], dst_ref=gain_buf.at[stage, pos],
            send_sem=g_send.at[stage, j], recv_sem=g_recv.at[stage, pos],
            device_id=env.device(axis, j), device_id_type=LOGICAL)

    def gain_send(stage):
        for j in range(1, axes[stage][2]):
            gain_copy(stage, j).start()
        clock.after(clock.now + 2 * EXCHANGE, functools.partial(gain_sum, stage))

    def gain_sum(stage):
        axis, pos, size = axes[stage]
        for j in range(1, size):
            peer = env.near(axis, j)
            pltpu.make_async_remote_copy(
                src_ref=gain_buf.at[stage, peer], dst_ref=gain_buf.at[stage, peer],
                send_sem=g_send.at[stage, j], recv_sem=g_recv.at[stage, peer],
                device_id=env.device(axis, j), device_id_type=LOGICAL).wait_recv()
        total = gain_buf[stage, 0]
        for i in range(1, size):
            total = total + gain_buf[stage, i]
        if stage == 2:
            gain_out[...] = total
        else:
            gain_buf[stage + 1, axes[stage + 1][1]] = total
            gain_send(stage + 1)

    gain_send(0)

    for target in (partner, dev(1), dev(-1)):
        pl.semaphore_signal(credit, device_id=fid[id(target)], device_id_type=LOGICAL)
    r = 2 * layers - 1
    pl.semaphore_wait(credit, 3)
    pairs(r, None, lambda xp: product(xp, GA[last, xp], last), FORWARD)
    rs_start(r)
    rs_mid(r)

    def output(rows, total):
        H[0, rows] = (H[last, rows].astype(F32) + total).astype(BF16)
    rs_end(r, output)
    y_copy = pltpu.make_async_copy(H.at[0], y_ref, io_sem.at[2])
    y_copy.start()
    while clock.queue:
        clock.step()

    y_copy.wait()
    for gather in fwd:
        gather.drain()
    for l, m, rows, lane in [straight[1:]] + [args for l in range(layers) for args in wx_sets(l)]:
        repeat(1, nf, lambda j: wx_copy(l, m, j, wrap(f + j, nf), f, rows, lane).wait_send())
    for l in range(layers):
        wy_each(l, (FIRST, SECOND, PASS), lambda *args: wy_copy(*args).wait_send())
    for job in jobs.values():
        job.wait_sends(True)
    for stage in range(3):
        for j in range(1, axes[stage][2]):
            gain_copy(stage, j).wait_send()
    pltpu.make_async_copy(G, out_ref, out_sem).wait()


def fused_step(x, dy, wg, wu, wd, gain, dims):
    layers, ny, nz, nf, tok, depth, hid = dims
    nx = nf // 2
    vm, hbm = pl.BlockSpec(memory_space=pltpu.VMEM), pl.BlockSpec(memory_space=pl.ANY)
    dma = pltpu.SemaphoreType.DMA
    blocks = (layers, ny, nz, 3 * nf, RS, LN)
    lines = layers * depth // LN
    steps = layers * 3 * 2 * (ny + nz)
    wide = max(nf, ny, nz)
    return pl.pallas_call(
        functools.partial(step_kernel, dims),
        out_shape=(jax.ShapeDtypeStruct((tok, depth), BF16), jax.ShapeDtypeStruct(blocks, F32), jax.ShapeDtypeStruct((lines, LN), F32)),
        in_specs=[hbm, hbm, hbm, hbm, hbm, vm],
        out_specs=(hbm, hbm, vm),
        scratch_shapes=[
            pltpu.VMEM((layers, 2, nf, depth // nf, hid), BF16),
            pltpu.VMEM((layers, hid, depth), BF16),
            pltpu.VMEM((layers, nf, tok, depth), BF16),
            pltpu.VMEM((layers, nx, 2 * tok, hid), BF16),
            pltpu.VMEM((layers, nx, 2 * tok, hid), BF16),
            pltpu.VMEM((2, nf, tok, depth), BF16),
            pltpu.VMEM((nx, 2, tok, depth), F32),
            pltpu.VMEM((nx, tok, depth), F32),
            pltpu.VMEM((2, 3, tok // 2, depth), F32),
            pltpu.VMEM((layers, tok, depth), BF16),
            pltpu.VMEM((2, nx, 2 * tok, hid), BF16),
            pltpu.VMEM(blocks, F32),
            pltpu.VMEM(blocks[1:], F32),
            pltpu.VMEM((layers, 2 * nf, RS, LN), F32),
            pltpu.VMEM((3, wide, lines, LN), F32),
            pltpu.VMEM((1, depth), F32),
            dma((24 * layers,)), dma((24 * layers,)), dma((24 * layers,)), dma((24 * layers,)),
            dma(((2 * layers + 1) * nf,)), dma(((2 * layers + 1) * nf,)), dma((12 * layers,)), dma((12 * layers,)),
            dma((2 * layers + 1,)), dma((layers,)),
            dma((2 * steps,)), dma((2 * steps,)), dma((steps,)), dma((steps,)),
            dma((2 * layers * nf,)), dma((2 * layers * nf,)),
            dma((3, wide)), dma((3, wide)), dma, dma((3,)),
            pltpu.SemaphoreType.REGULAR((layers, 3)), pltpu.SemaphoreType.REGULAR((layers, 3)), pltpu.SemaphoreType.REGULAR,
        ],
        compiler_params=pltpu.CompilerParams(collective_id=0, has_side_effects=True, vmem_limit_bytes=67043328),
        name="fused_step",
    )(x, dy, wg, wu, wd, gain)


def unpack_kernel(g_ref, gate_ref, up_ref, down_ref):
    ny, nzb, units = g_ref.shape[:3]
    nf = units // 3
    for k in range(nzb):
        for i in range(ny):
            for m, ref in enumerate((gate_ref, up_ref)):
                for j in range(nf):
                    col = (j * ny + i) * LN
                    ref[k * RS:(k + 1) * RS, col:col + LN] = g_ref[i, k, m * nf + j]
            for h in BOTH:
                for r in range(nf // 2):
                    row, col = (k * (nf // 2) + r) * RS, (2 * i + h) * LN
                    down_ref[row:row + RS, col:col + LN] = g_ref[i, k, 2 * nf + h * (nf // 2) + r]


def unpack(out, dims, steps=2):
    layers, ny, nz, nf = dims
    nzb = nz // steps
    wide, tall = nf * ny * LN, (nf // 2) * RS
    return pl.pallas_call(
        unpack_kernel, grid=(layers, steps),
        in_specs=[pl.BlockSpec((None, ny, nzb, 3 * nf, RS, LN), lambda l, z: (l, 0, z, 0, 0, 0))],
        out_specs=[pl.BlockSpec((None, nzb * RS, wide), lambda l, z: (l, z, 0))] * 2
        + [pl.BlockSpec((None, nzb * tall, 2 * ny * LN), lambda l, z: (l, z, 0))],
        out_shape=[jax.ShapeDtypeStruct((layers, nz * RS, wide), F32)] * 2
        + [jax.ShapeDtypeStruct((layers, nz * tall, 2 * ny * LN), F32)],
        name="unpack")(out)


TOKEN_AXES = ("dp", "replica", "fsdp")


def solution(mesh):
    ny, nz, nf = mesh.shape["replica"], mesh.shape["dp"], mesh.shape["fsdp"]
    tok_spec, shard_spec, full_spec = P(TOKEN_AXES, None), P(None, "fsdp", None), P(None, None)

    def device_step(x, dy, wg, wu, wd, gain):
        layers, depth = gain.shape
        dims = (layers, ny, nz, nf)
        out, blocks, gain_sum = fused_step(x, dy, wg, wu, wd, gain, dims + (x.shape[0], depth, wd.shape[1]))
        dw_gate, dw_up, dw_down = unpack(blocks, dims)
        return out, dw_gate, dw_up, dw_down, gain_sum.reshape(gain.shape)

    return jax.shard_map(
        device_step, mesh=mesh, in_specs=(tok_spec, tok_spec, shard_spec, shard_spec, shard_spec, full_spec),
        out_specs=(tok_spec, shard_spec, shard_spec, shard_spec, full_spec), check_vma=False)
```

```python
import functools
import heapq
import jax
import jax.numpy as jnp
from jax import lax
from jax.sharding import PartitionSpec as P
from jax.experimental import pallas as pl
from jax.experimental.pallas import tpu as pltpu

F32 = jnp.float32
BF16 = jnp.bfloat16
LOGICAL = pl.DeviceIdType.LOGICAL
RS, LN = 16, 128
UNIT_BYTES = RS * LN * 4
NORM_EPS = 1e-6
NN = (((1,), (0,)), ((), ()))
NT = (((1,), (1,)), ((), ()))
TN = (((0,), (0,)), ((), ()))
LINK_RATE, CORE_RATE, HOP, CORE_HOP, STEP_COST, HBM_READ, ENTRY = 46.6e3, 500e3, 2.2, 0.9, 0.15, 1.1, 3.5
CORES = "cores"
BOTH, SIGN, BF16_BYTES = (0, 1), (1, -1), 2
FIRST, SECOND, PASS, RELAY, FAR, OWN = range(6)
DIRECT = "direct"
FORWARD, BACKWARD, WEIGHT, ADD, EXCHANGE = 0.7, 0.95, 0.9, 0.15, 5.0


def dot(a, b, dims=NN):
    return lax.dot_general(a, b, dims, preferred_element_type=F32)


def loop(count, work):
    repeat(0, count, work)


def repeat(start, stop, work):
    def step(i, carry):
        work(i)
        return carry
    lax.fori_loop(start, stop, step, 0)


def wait_for(view, sem, device, sent=False):
    copy = pltpu.make_async_remote_copy(
        src_ref=view, dst_ref=view, send_sem=sem, recv_sem=sem, device_id=device, device_id_type=LOGICAL)
    if sent:
        copy.wait_send()
    else:
        copy.wait_recv()


def first(count):
    return pl.ds(0, count)


def wrap(value, size):
    return lax.rem(value + 4 * size, size)


class Clock:
    def __init__(self):
        self.now, self.queue, self.count, self.links = 0.0, [], 0, {}

    def send(self, link, size):
        near = link == CORES
        start = max(self.now, self.links.get(link, 0.0))
        self.links[link] = start + size / (CORE_RATE if near else LINK_RATE)
        return self.links[link] + (CORE_HOP if near else HOP)

    def after(self, ready, work):
        self.count += 1
        heapq.heappush(self.queue, (ready, self.count, work))

    def step(self):
        ready, _, work = heapq.heappop(self.queue)
        self.now = max(self.now, ready) + STEP_COST
        work()

    def run(self, until):
        while self.queue and self.queue[0][0] <= until:
            self.step()

    def busy(self, spent):
        self.now += spent
        self.run(self.now)

    def idle(self, until):
        self.run(until)
        self.now = max(self.now, until)

    def play(self, task):
        for ready in task:
            self.idle(ready)

    def spawn(self, task):
        ready = next(task, None)
        if ready is not None:
            self.after(ready, functools.partial(self.spawn, task))

    def until(self, done):
        while not done():
            self.step()

    def known(self, times, key):
        while key not in times:
            yield self.now + STEP_COST
        yield times[key]


class Job:
    def __init__(self, env, layer, part):
        parts = LAST_SIZES if layer == env.last else PART_SIZES
        sizes, start = (parts[part], env.nf - parts[part]), part * env.nf
        before = sum(parts[:part])
        offsets = before, start - before
        self.split = sum(parts)
        swap = () if part == DOWN else (part,)
        self.env, self.layer, self.part, self.swap = env, layer, part, swap
        self.sizes, self.offsets, self.starts = sizes, offsets, (start, start + sizes[0])
        self.left, self.turned = len(BOTH), 0
        above = env.above(self)
        self.slots = dict(env.jobs[above].slots) if above else {}
        for gather in BOTH[1:] if above else BOTH:
            for phase in BOTH:
                for k in BOTH:
                    self.slots[gather, phase, k] = env.sends, env.receives
                    env.sends += 1
                    env.receives += self.half_ring(phase, k)

    def ring(self, phase, k):
        return ("replica", "dp")[phase ^ k]

    def half_ring(self, phase, k):
        return self.env.size[self.ring(phase, k)] // 2

    def block(self, phase, k, index, side=None):
        env, G, layer = self.env, self.env.G, self.layer
        start, size = self.starts[k], self.sizes[k]
        if side is not None:
            start, size = start + side * (size // 2), size // 2
        units = pl.ds(start, size)
        if phase == 0:
            return G.at[layer, index, :, units] if k == 0 else G.at[layer, :, index, units]
        return G.at[layer, env.y, index, units] if k == 0 else G.at[layer, index, env.z, units]

    def stage(self, phase, k, d, step, side=None):
        env = self.env
        ref, lead = (env.G, (0,)) if self.layer == env.last else (env.S, ())
        base = 0 if k == 0 else self.split
        offset, size = self.offsets[k], self.sizes[k]
        half_total = ((env.units - self.split) if k else self.split) // 2
        at = 2 * (step - 1) + d
        if step == 0:
            units = pl.ds(base + d * half_total + offset // 2, size // 2)
            at = env.nz - 2 if self.ring(phase, k) == "dp" else 2
        elif side is None:
            units = pl.ds(base + offset, size)
        else:
            units = pl.ds(base + offset + side * (size // 2), size // 2)
        every = slice(None)
        if phase == 0:
            place = (at, every) if k == 0 else (every, at)
        else:
            place = (env.ny - 1, at) if k == 0 else (at, env.nz - 1)
        return ref.at[(*lead, *place, units)]

    def many(self, phase, k, count):
        G, some, every = self.env.G, first(count), slice(None)
        units = pl.ds(self.starts[k], self.sizes[k])
        other = every if phase == 0 else 0
        place = (some, other) if phase == k else (other, some)
        return G.at[(self.layer, *place, units)]

    def copy(self, gather, phase, k, d, step, src, dst):
        env = self.env
        send, receive = self.slots[gather, phase, k]
        return pltpu.make_async_remote_copy(
            src_ref=src, dst_ref=dst, send_sem=env.send_sem.at[send], recv_sem=env.recv_sem.at[receive + step],
            device_id=env.device(self.ring(phase, k), SIGN[d]), device_id_type=LOGICAL)

    def take(self, gather, phase, k, step, blocks):
        receive = self.slots[gather, phase, k][1]
        wait_for(self.many(phase, k, blocks), self.env.recv_sem.at[receive + step], self.env.device(self.ring(phase, k), 1))

    def send_time(self, phase, k, d, units):
        env = self.env
        other = (env.nz if k == 0 else env.ny) if phase == 0 else 1
        return env.clock.send((self.ring(phase, k), d), units * other * UNIT_BYTES)

    def reduce_send(self, phase, k, step, early=False):
        size, ready = self.sizes[k], 0.0
        for d in BOTH:
            side = None if step > 1 else BOTH[d - 1] if early else d
            index = self.env.near(self.ring(phase, k), SIGN[d] * (self.half_ring(phase, k) - step))
            stage = self.stage(phase, k, d, step, None if step == 0 else side)
            self.copy(0, phase, k, d, step, self.block(phase, k, index, side), stage).start()
            ready = max(ready, self.send_time(phase, k, d, size if step > 1 else size // 2))
        if not early:
            self.env.clock.after(ready, functools.partial(self.reduce_step, phase, k, step))

    def reduce_start(self, phase, k):
        self.reduce_send(phase, k, 0)
        self.reduce_send(phase, k, 1, True)

    def start(self, phase, k):
        env = self.env
        if phase == 0 and k == 0 and env.above(self):
            pl.semaphore_wait(env.freed.at[env.above(self)], 4)
        self.reduce_start(phase, k)

    def reduce_step(self, phase, k, step):
        half = self.half_ring(phase, k)
        self.take(0, phase, k, step, len(BOTH) if step else 1)
        for d in BOTH:
            index = self.env.near(self.ring(phase, k), SIGN[d] * (half - 1 - step))
            self.block(phase, k, index, None if step else d)[...] += self.stage(phase, k, d, step)[...]
        if step + 1 < half:
            self.reduce_send(phase, k, step + 1)
        elif phase == 0:
            self.halfway()
            self.env.begin(self, 1, k)
        else:
            self.left -= 1
            if self.left == 0:
                self.reduced()

    def halfway(self):
        env, here = self.env, (self.layer, self.part)
        self.turned += 1
        if self.turned == len(BOTH):
            self.wait_sends(0, 0)
            if 0 < self.layer < env.last:
                self.tell(env.freed)
            env.half.add(here)
            env.begin_waiting()

    def tell(self, flags):
        for axis in ("replica", "dp"):
            for sign in SIGN:
                pl.semaphore_signal(flags.at[self.layer, self.part], device_id=self.env.device(axis, sign), device_id_type=LOGICAL)

    def wait_sends(self, gather, phase):
        for k in BOTH:
            ring = self.ring(phase, k)
            send = self.slots[gather, phase, k][0]
            wait_for(self.many(phase, k, self.env.size[ring] - 1), self.env.send_sem.at[send], self.env.device(ring, 1), True)

    def x_copy(self, m, peer, sender):
        env = self.env
        lane = 2 * self.layer + m
        return pltpu.make_async_remote_copy(
            src_ref=env.G.at[self.layer, env.y, env.z, m * env.nf + peer], dst_ref=env.R.at[self.layer, m * env.nf + sender],
            send_sem=env.x_send.at[lane], recv_sem=env.x_recv.at[lane],
            device_id=env.row + peer, device_id_type=LOGICAL)

    def reduced(self):
        env = self.env
        self.wait_sends(0, 1)
        self.tell(env.ready)
        for m in self.swap:
            repeat(1, env.nf, lambda j: self.x_copy(m, wrap(env.f + j, env.nf), env.f).start())
        env.reduced.add((self.layer, self.part))
        env.clock.after(env.clock.now + (EXCHANGE if self.swap else HOP), self.exchanged)

    def exchanged(self):
        env = self.env
        f, nf = env.f, env.nf
        for m in self.swap:
            env.R[self.layer, m * nf + f] = env.G[self.layer, env.y, env.z, m * nf + f]
        for m in self.swap:
            lane, view = 2 * self.layer + m, env.R.at[self.layer, first(nf - 1)]
            wait_for(view, env.x_send.at[lane], env.device("fsdp", 1), True)
            wait_for(view, env.x_recv.at[lane], env.device("fsdp", 1))
        for m in self.swap:
            env.G[self.layer, env.y, env.z, pl.ds(m * nf, nf)] = env.R[self.layer, pl.ds(m * nf, nf)]
        pl.semaphore_wait(env.ready.at[self.layer, self.part], 4)
        self.left = 2
        for k in BOTH:
            self.gather_send(1, k, 0)
        env.exchanged.add((self.layer, self.part))
        env.begin_waiting()

    def gather_send(self, phase, k, step):
        half, ready = self.half_ring(phase, k), 0.0
        for d in BOTH:
            side = d if step + 1 == half else None
            view = self.block(phase, k, self.env.near(self.ring(phase, k), -SIGN[d] * step), side)
            self.copy(1, phase, k, d, step, view, view).start()
            ready = max(ready, self.send_time(phase, k, d, self.sizes[k] if side is None else self.sizes[k] // 2))
        self.env.clock.after(ready, functools.partial(self.gather_step, phase, k, step))

    def gather_step(self, phase, k, step):
        env = self.env
        last = step + 1 == self.half_ring(phase, k)
        self.take(1, phase, k, step, 1 if last else len(BOTH))
        if not last:
            self.gather_send(phase, k, step + 1)
        elif phase == 1:
            self.gather_send(0, k, 0)
        else:
            self.left -= 1
            here = (self.layer, slice(None), slice(None), pl.ds(self.starts[k], self.sizes[k]))
            pltpu.make_async_copy(env.G.at[here], env.out_ref.at[here], env.out_sem).start()


class Env:
    def __init__(self, dims):
        self.exchanged, self.reduced, self.half, self.waiting, self.clock = set(), set(), set(), [], Clock()
        self.sends = self.receives = 0
        self.ny, self.nz, self.nf = dims[1:4]
        self.last = dims[0] - 1
        self.f, self.y, self.z = lax.axis_index("fsdp"), lax.axis_index("replica"), lax.axis_index("dp")
        self.size = {"fsdp": self.nf, "replica": self.ny, "dp": self.nz}
        self.pos = {"fsdp": self.f, "replica": self.y, "dp": self.z}
        stride = {"fsdp": 1, "replica": self.nf, "dp": self.nf * self.ny}
        me = self.f + stride["replica"] * self.y + stride["dp"] * self.z
        self.row = me - self.f
        self.shift = {a: [wrap(self.pos[a] + k, n) for k in range(n)] for a, n in self.size.items()}
        self.ids = {a: [me + (p - self.pos[a]) * stride[a] for p in self.shift[a]] for a in self.size}

    def near(self, axis, k):
        return self.shift[axis][k % self.size[axis]]

    def device(self, axis, k):
        return self.ids[axis][k % self.size[axis]]

    def above(self, job):
        return (job.layer + 1, job.part) if job.layer + 1 < self.last else None

    def begin(self, job, phase, k):
        self.waiting.append((job, phase, k))
        self.begin_waiting()

    def begin_job(self, job):
        for k in BOTH:
            self.begin(job, 0, k)

    def begin_waiting(self):
        for item in list(self.waiting):
            job, phase, k = item
            if item in self.waiting and (not self.above(job) or self.above(job) in (self.exchanged if phase else self.half)):
                self.waiting.remove(item)
                job.start(phase, k)

    def settle(self, layer):
        self.clock.until(lambda: {(layer, part) for part in (GATE, UP, DOWN)} <= self.reduced)


GATE, UP, DOWN = range(3)
PART_SIZES, LAST_SIZES = (4, 4, 6), (6, 4, 6)


def step_kernel(dims, x_ref, dy_ref, wg_ref, wu_ref, wd_ref, gain_ref, y_ref, out_ref, gain_out,
                WB, WD, N, GA, UA, DH, O, DS, MS, H, DGU, G, S, R, gain_buf, gain_row,
                ag_send, ag_recv, rs_send, rs_recv, wx_send, wx_recv, wz_send, wz_recv, wy_send, wy_recv, w_sem, wd_sem,
                j_send, j_recv, x_send, x_recv, g_send, g_recv, out_sem, io_sem, ready, freed, credit):
    layers, ny, nz, nf, tok, depth, hid = dims
    nx, q = nf // 2, depth // nf // ny
    tile = min(256, depth)
    last = layers - 1

    env = Env(dims)
    f, y, z = env.f, env.y, env.z
    x, c = f // 2, f % 2
    env.G, env.S, env.R, env.out_ref = G, S, R, out_ref
    env.send_sem, env.recv_sem = j_send, j_recv
    env.x_send, env.x_recv, env.ready, env.freed, env.out_sem = x_send, x_recv, ready, freed, out_sem
    env.units = 3 * nf
    clock = env.clock
    env.jobs = jobs = {}
    for l in reversed(range(layers)):
        for part in (GATE, UP, DOWN):
            jobs[l, part] = Job(env, l, part)

    chips = [wrap(x + k, nx) for k in range(nx)]
    same, opposite_core = [2 * p + c for p in chips], [2 * p + (1 - c) for p in chips]
    fid = {id(v): env.row + v for v in same + opposite_core}

    def dev(off, opposite=False):
        return (opposite_core if opposite else same)[off % nx]

    partner = dev(0, True)
    axes = [("fsdp", f, nf), ("replica", y, ny), ("dp", z, nz)]

    barrier = pltpu.get_barrier_semaphore()
    for axis, pos, size in axes:
        for j in range(1, size):
            pl.semaphore_signal(barrier, device_id=env.device(axis, j), device_id_type=LOGICAL)

    x_copy = pltpu.make_async_copy(x_ref, H.at[0], io_sem.at[0])
    dy_copy = pltpu.make_async_copy(dy_ref, DH.at[last % 2, f], io_sem.at[1])
    x_copy.start()
    dy_copy.start()
    wd_copies = [pltpu.make_async_copy(wd_ref.at[l], WD.at[l], wd_sem.at[l]) for l in range(layers)]
    weights = (wg_ref, wu_ref)
    y_at = [env.near("replica", k) for k in range(ny)]
    parts = (first(nf // 2), pl.ds(nf // 2, nf // 2))
    direct = pl.ds(ny * q // 2, ny * q // 2)
    direct_lane = 2 * layers
    shared = {}

    def share(l, m, hops=0):
        size = q // 2 if (l, m) == BOTH else q
        return pl.ds(y_at[hops % ny] * size, size)

    odd = lax.rem(z, 2)
    z_partner = env.ids["dp"][0] + (1 - 2 * odd) * nf * ny

    def fetched(l, m, other=False):
        if l == 0:
            return share(l, m)
        return pl.ds(y_at[0] * q + (1 - odd if other else odd) * (q // 2), q // 2)

    def wz_copy(l, m, other=False):
        view = WB.at[l, m, :, fetched(l, m, other)]
        return pltpu.make_async_remote_copy(
            src_ref=view, dst_ref=view, send_sem=wz_send.at[2 * l + m], recv_sem=wz_recv.at[2 * l + m],
            device_id=z_partner, device_id_type=LOGICAL)

    def own_rows(l, m, rows, sem):
        src = weights[m].at[l, rows, pl.ds(pl.multiple_of(f * hid, hid), hid)]
        return pltpu.make_async_copy(src, WB.at[l, m, f, rows], w_sem.at[sem])

    own_copies = {(l, m): own_rows(l, m, fetched(l, m), 2 * l + m) for l in range(layers) for m in BOTH}
    own_copies[DIRECT] = own_rows(*BOTH, direct, 2 * layers)
    for copy in own_copies.values():
        copy.start()
    for copy in wd_copies:
        copy.start()
    pl.semaphore_wait(barrier, nf + ny + nz - 3)
    clock.busy(ENTRY)

    def wx_copy(l, m, peer, sender, rows, lane):
        return pltpu.make_async_remote_copy(
            src_ref=weights[m].at[l, rows, pl.ds(pl.multiple_of(peer * hid, hid), hid)], dst_ref=WB.at[l, m, sender, rows],
            send_sem=wx_send.at[lane], recv_sem=wx_recv.at[lane], device_id=env.row + peer, device_id_type=LOGICAL)

    def wx_sets(l):
        return [(l, m, fetched(l, m), 2 * l + m) for m in BOTH]

    def wx_post(key, l, m, rows, lane):
        repeat(1, nf, lambda j: wx_copy(l, m, wrap(f + j, nf), f, rows, lane).start())
        for d in BOTH:
            shared[key] = clock.send(d, nx * rows.size * hid * BF16_BYTES) + HBM_READ

    def wx_take(key, l, m, rows, lane):
        yield from clock.known(shared, key)
        own_copies[key].wait()
        wait_for(WB.at[l, m, first(nf - 1), rows], wx_recv.at[lane], env.device("fsdp", 1))

    def wx_start(l):
        for args in wx_sets(l):
            wx_post(args[:2], *args)

    def wy_copy(l, m, kind, d, arrived=False):
        hops = (kind == PASS) + arrived
        lane = 2 * l + m
        part = parts[BOTH[d - (kind == SECOND)]]
        view = WB.at[l, m, part, share(l, m, -SIGN[d] * hops)]
        return pltpu.make_async_remote_copy(
            src_ref=view, dst_ref=view, send_sem=wy_send.at[lane], recv_sem=wy_recv.at[2 * lane + (kind > FIRST)],
            device_id=env.device("replica", SIGN[d]), device_id_type=LOGICAL)

    def wy_send_one(l, m, kind, d):
        wy_copy(l, m, kind, d).start()
        shared[l, m, kind, d] = clock.send(("replica", d), nf // 2 * share(l, m).size * hid * BF16_BYTES)

    def wy_take(l, m, later):
        for kind in (SECOND, PASS) if later else (FIRST,):
            for d in BOTH:
                yield from clock.known(shared, (l, m, kind, d))
        rows = first(share(l, m).size * (1 + later))
        wait_for(WB.at[l, m, :, rows], wy_recv.at[2 * (2 * l + m) + later], env.device("replica", 1))

    def weights_task():
        for l in range(layers):
            for args in wx_sets(l):
                yield from wx_take(args[:2], *args)
                if l:
                    wz_copy(*args[:2]).start()
                    yield clock.send(("dp", 0), nf * q // 2 * hid * BF16_BYTES)
                    wz_copy(*args[:2], True).wait_recv()
                for kind in (FIRST, SECOND):
                    for d in BOTH:
                        wy_send_one(*args[:2], kind, d)
            for m in BOTH:
                yield from wy_take(l, m, 0)
                for d in BOTH:
                    wy_send_one(l, m, PASS, d)

    def weights_here(l):
        while l in claimed and l not in arrived:
            yield clock.now + STEP_COST
        if l in arrived:
            return
        claimed.add(l)
        if l == 0:
            yield from wx_take(*straight)
        for m in BOTH:
            yield from wy_take(l, m, 1)
        wd_copies[l].wait()
        arrived.add(l)

    claimed, arrived = set(), set()
    straight = DIRECT, *BOTH, direct, direct_lane

    class Gather:
        def __init__(self, lanes, buf, slot, base, size):
            self.lanes, self.buf, self.slot, self.ready = lanes, buf, slot, {}
            self.whole = pl.ds(base, size)
            self.halves = (pl.ds(base, size // 2), pl.ds(base + size // 2, size // 2))

        def copy(self, kind, d):
            hops = (kind in (PASS, RELAY)) + (kind == FAR) * nx // len(BOTH)
            block = dev(-SIGN[d] * hops)
            rows = self.whole if kind in (RELAY, OWN) else self.halves[d - (kind == SECOND)]
            target = partner if kind in (RELAY, FAR, OWN) else dev(SIGN[d])
            view = self.buf.at[self.slot, block, rows]
            return rows.size, pltpu.make_async_remote_copy(
                src_ref=view, dst_ref=view, send_sem=ag_send.at[self.lanes], recv_sem=ag_recv.at[self.lanes * (OWN + 1) + kind],
                device_id=fid[id(target)], device_id_type=LOGICAL)

        def send(self, *kinds):
            for kind in kinds:
                ready = 0.0
                for d in BOTH[:1] if kind == OWN else BOTH:
                    size, copy = self.copy(kind, d)
                    copy.start()
                    ready = max(ready, clock.send(CORES if kind in (RELAY, FAR, OWN) else d, size * depth * BF16_BYTES))
                self.ready[kind] = ready

        def blocks(self, count):
            return self.buf.at[self.slot, first(count), self.whole]

        def take(self, *kinds):
            for kind in kinds:
                yield from clock.known(self.ready, kind)
                wait_for(self.blocks(2 if kind == RELAY else 1), ag_recv.at[self.lanes * (OWN + 1) + kind], fid[id(partner)])

        def start(self):
            self.send(FIRST, OWN, SECOND)

        def mid(self):
            for kind, onward in ((FIRST, PASS), (SECOND, RELAY)):
                yield from self.take(kind)
                self.send(onward)

        def end(self):
            yield from self.take(PASS)
            self.send(FAR)

        def drain(self):
            wait_for(self.blocks(nf - 1), ag_send.at[self.lanes], fid[id(partner)], True)

    chunk = min(16, tok // 8)

    def rows_at(start, j):
        return pl.ds(pl.multiple_of(start + j * chunk, chunk), chunk)

    class Reduce:
        def __init__(self, lanes, base, size):
            self.lanes, self.base, self.size, self.arrive = lanes, base, size, {}
            self.rows, self.local = pl.ds(base, size), pl.ds(base // 2, size // 2)

        def d2d(self, i, xp, core):
            return pltpu.make_async_remote_copy(
                src_ref=O.at[xp, core, self.rows], dst_ref=DS.at[xp, self.rows], send_sem=rs_send.at[2 * self.lanes],
                recv_sem=rs_recv.at[(nx + 2) * self.lanes + i], device_id=fid[id(partner)], device_id_type=LOGICAL)

        def msg(self, k, d):
            half = self.size // 2
            lane = (nx + 2) * self.lanes + nx + (k > 0)
            off, side = (2, d) if k == 0 else (SIGN[d], d if k == 3 else 1 - d)
            size, slot, at = half, (0 if k == 0 else 2), 0
            if k in (1, 2):
                size, slot = half // 2, 1
                at = (k - 1) * size
            return size, pltpu.make_async_remote_copy(
                src_ref=O.at[chips[off % nx], c, pl.ds(self.base + side * half + at, size)],
                dst_ref=MS.at[d, slot, pl.ds(self.base // 2 + at, size)],
                send_sem=rs_send.at[2 * self.lanes + 1], recv_sem=rs_recv.at[lane], device_id=fid[id(dev(SIGN[d]))], device_id_type=LOGICAL)

        def post(self, k, d):
            size, copy = self.msg(k, d)
            copy.start()
            self.arrive[k, d] = clock.send(d, size * depth * 4)

        def take(self, later):
            yield max(self.arrive[k, d] for k in ((1, 2, 3) if later else (0,)) for d in BOTH)
            view = MS.at[:, pl.ds(later, 1 + later), self.local]
            wait_for(view, rs_recv.at[(nx + 2) * self.lanes + nx + later], fid[id(partner)])

        def combine(self, i, off):
            xp = chips[off % nx]
            yield self.arrive[i]
            self.d2d(i, xp, c).wait_recv()

            def add(j):
                rows = rows_at(self.base, j)
                O[xp, c, rows] += DS[xp, rows]
            loop(self.size // chunk, add)
            clock.busy(ADD)

        def near(self):
            for i, d in ((1, 0), (2, 1)):
                yield from self.combine(i, SIGN[d])
                self.post(1, d)

        def start(self):
            yield from self.combine(3, 2)
            for k in (0, 2):
                for d in BOTH:
                    self.post(k, d)
            yield from self.combine(0, 0)

        def mid(self):
            half = self.size // 2
            yield from self.take(0)
            for d in BOTH:
                def add(j):
                    rows = rows_at(self.base + d * half, j)
                    O[chips[SIGN[d] % nx], c, rows] += MS[d, 0, rows_at(self.base // 2, j)]
                loop(half // chunk, add)
                self.post(3, d)

        def end(self, body):
            half = self.size // 2
            yield from self.take(1)
            for side in BOTH:
                def step(j):
                    rows, local = rows_at(self.base + side * half, j), rows_at(self.base // 2, j)
                    body(rows, O[x, c, rows] + (MS[0, 2 - side, local] + MS[1, 1 + side, local]))
                loop(half // chunk, step)
            clock.busy(5 * ADD)
            wait_for(O.at[:, 0, self.rows], rs_send.at[2 * self.lanes], fid[id(partner)], True)
            wait_for(O.at[first(nx - 1), 0, self.rows], rs_send.at[2 * self.lanes + 1], fid[id(partner)], True)

        def pairs(self, gathers, body, cost, after_mid=None):
            def step(i):
                xp = wrap(x + i + i // 2 - 2 * (i // 3), nx)
                body(xp, self.rows)
                self.d2d(i, xp, 1 - c).start()

            def go(start, stop):
                repeat(start, stop, step)
                for i in range(start, stop):
                    clock.now += cost
                    self.arrive[i] = clock.send(CORES, self.size * depth * 4)
                clock.busy(0.0)

            go(0, 1)
            for gather in gathers:
                yield from gather.take(RELAY)
            go(1, 3)
            late = not all(gather.ready.get(FAR, self.arrive[2]) < self.arrive[2] for gather in gathers)
            if late:
                yield from self.near()
            for gather in gathers:
                yield from gather.take(FAR)
            go(3, nx)
            if not late:
                yield from self.near()

    def rms(hidden):
        return lax.rsqrt(jnp.mean(hidden * hidden, axis=-1, keepdims=True) + NORM_EPS)

    def down_grad(l):
        group = nf // 2
        zs = tile // (group * RS)

        def body(j, carry):
            lhs = GA[l, :, :, :, pl.ds(pl.multiple_of(j * tile, tile), tile)].reshape(-1, tile)
            for i in range(depth // tile):
                res = dot(lhs, DH[l % 2, :, :, pl.ds(i * tile, tile)].reshape(-1, tile), TN)
                for h in range(tile // LN):
                    col = i * (tile // LN) + h
                    for zi in range(zs):
                        rows = res[zi * group * RS:(zi + 1) * group * RS, h * LN:(h + 1) * LN]
                        G[l, col // 2, j * zs + zi, pl.ds(2 * nf + (col % 2) * group, group)] = rows.reshape(group, RS, LN)
            return carry
        lax.fori_loop(0, hid // tile, body, 0)

    def up_grad(l):
        fs = tile // (nz_rows * RS)

        def body(j, carry):
            lhs = N[l, :, :, pl.ds(pl.multiple_of(j * tile, tile), tile)].reshape(-1, tile)
            for m in BOTH:
                for i in range(hid // tile):
                    res = dot(lhs, DGU[m, :, :, :, pl.ds(i * tile, tile)].reshape(-1, tile), TN)
                    for h in range(tile // LN):
                        for fi in range(fs):
                            rows = res[fi * nz_rows * RS:(fi + 1) * nz_rows * RS, h * LN:(h + 1) * LN]
                            G[l, i * (tile // LN) + h, :, m * nf + j * fs + fi] = rows.reshape(nz_rows, RS, LN)
            return carry
        lax.fori_loop(0, depth // tile, body, 0)

    nz_rows = depth // nf // RS
    part = tok // 2
    fwd = [[Gather(g, N, l, g * part, part) for g in BOTH] for l in range(layers)]
    bwd = [Gather(2, DH, l % 2, 0, tok) for l in range(layers)]
    dy_task = bwd[last]

    def activations(l, xp, rows, cols):
        tokens = N[l, pl.ds(2 * xp, 2), rows].reshape(-1, depth)
        gate = dot(tokens, WB[l, 0, :, :, cols].reshape(depth, tile)).astype(BF16)
        up = dot(tokens, WB[l, 1, :, :, cols].reshape(depth, tile)).astype(BF16)
        return gate, up

    def flat(ref, *index):
        value = ref[index]
        return value.reshape(-1, value.shape[-1])

    def product(l, ref, lead, xp, rows):
        prod = flat(ref, *lead, xp, slice(None), rows)
        for j in range(depth // tile):
            cols = pl.ds(j * tile, tile)
            O[xp, :, rows, cols] = dot(prod, WD[l, :, cols]).reshape(2, rows.size, tile)

    def forward(l, xp, rows):
        shape = (2, rows.size, tile)
        for j in range(hid // tile):
            cols = pl.ds(j * tile, tile)
            gate, up = activations(l, xp, rows, cols)
            GA[l, xp, :, rows, cols] = gate.reshape(shape)
            UA[l, xp, :, rows, cols] = up.reshape(shape)
            DGU[0, xp, :, rows, cols] = (jax.nn.silu(gate.astype(F32)) * up.astype(F32)).astype(BF16).reshape(shape)
        product(l, DGU, (0,), xp, rows)

    def backward(l, xp, rows):
        cot = DH[l % 2, pl.ds(2 * xp, 2)].reshape(-1, depth)
        shape = (2, tok, tile)
        for j in range(hid // tile):
            cols = pl.ds(j * tile, tile)
            here = (l, xp, slice(None), slice(None), cols)
            gate, up = activations(l, xp, rows, cols) if l == last else (flat(GA, *here), flat(UA, *here))
            gate, up = gate.astype(F32), up.astype(F32)
            d_prod = dot(cot, WD[l, cols, :], NT).astype(BF16).astype(F32)
            sig = jax.nn.sigmoid(gate)
            GA[here] = (gate * sig * up).astype(BF16).reshape(shape)
            DGU[0, xp, :, :, cols] = (d_prod * up * sig * (1.0 + gate * (1.0 - sig))).astype(BF16).reshape(shape)
            DGU[1, xp, :, :, cols] = (d_prod * gate * sig).astype(BF16).reshape(shape)
        d_gate, d_up = flat(DGU, 0, xp), flat(DGU, 1, xp)
        block = depth // nf
        for j in range(depth // tile):
            sub = pl.ds(j * tile // block, tile // block)
            total = dot(d_gate, WB[l, 0, sub].reshape(tile, hid), NT) + dot(d_up, WB[l, 1, sub].reshape(tile, hid), NT)
            O[xp, :, :, pl.ds(j * tile, tile)] = total.reshape(shape)

    def normalize(l, rows, hidden):
        N[l, f, rows] = (hidden * rms(hidden) * gain_ref[l:l + 1]).astype(BF16)

    def half_task(g):
        for l in range(last):
            gather, reduce = fwd[l][g], Reduce(g, g * part, part)
            yield from gather.mid()
            if g and l == 0:
                wx_start(1)
                dy_task.start()
                clock.spawn(dy_task.mid())
                clock.spawn(dy_task.end())
            if g and l + 2 < layers:
                wx_start(l + 2)
            clock.spawn(gather.end())
            yield from gather.take(OWN)
            yield from weights_here(l)
            yield from reduce.pairs([gather], functools.partial(forward, l), FORWARD / len(BOTH))
            yield from reduce.start()
            yield from reduce.mid()

            def next_hidden(rows, total, l=l):
                hidden = (H[l, rows].astype(F32) + total).astype(BF16)
                H[l + 1, rows] = hidden
                normalize(l + 1, rows, hidden.astype(F32))
            yield from reduce.end(next_hidden)
            gather.drain()
            fwd[l + 1][g].start()
        yield from fwd[last][g].mid()
        yield from fwd[last][g].end()
        finished.add(g)

    finished = set()
    wx_start(0)
    x_copy.wait()
    for g in BOTH:
        def enter(j):
            rows = rows_at(g * part, j)
            normalize(0, rows, H[0, rows].astype(F32))
        loop(part // chunk, enter)
        clock.busy(ADD)
        fwd[0][g].start()
    wx_post(*straight)
    dy_copy.wait()
    clock.spawn(weights_task())
    for g in BOTH:
        clock.spawn(half_task(g))
    clock.until(lambda: FAR in fwd[last][0].ready)

    for l in reversed(range(layers)):
        reduce = Reduce(2, 0, tok)
        if l == last:
            gathers = fwd[l]
            clock.play(dy_task.take(RELAY, FAR, OWN))
            clock.play(weights_here(l))
        else:
            gathers = [bwd[l]]
            bwd[l].start()
            clock.spawn(bwd[l].mid())
            clock.spawn(bwd[l].end())
        for gather in gathers:
            clock.play(gather.take(OWN))
        clock.play(reduce.pairs(gathers, functools.partial(backward, l), FORWARD + BACKWARD if l == last else BACKWARD))
        clock.play(reduce.start())
        if l == 0:
            env.settle(last)
        down_grad(l)
        clock.busy(WEIGHT)
        env.begin_job(jobs[l, DOWN])
        up_grad(l)
        clock.busy(2 * WEIGHT)
        env.begin_job(jobs[l, GATE])
        env.begin_job(jobs[l, UP])
        clock.play(reduce.mid())
        bwd[l].drain()

        def next_cot(rows, total, l=l):
            d_normed = total.astype(BF16).astype(F32)
            hidden = H[l, rows].astype(F32)
            inv = rms(hidden)
            if l > 0:
                scaled = d_normed * gain_ref[l:l + 1]
                cot = DH[l % 2, f, rows].astype(F32)
                d_hidden = cot + inv * scaled - hidden * (inv * inv * inv) * jnp.mean(scaled * hidden, axis=-1, keepdims=True)
                DH[(l - 1) % 2, f, rows] = d_hidden.astype(BF16)
            gain_row[...] += jnp.sum(d_normed * hidden * inv, axis=0, keepdims=True)
        gain_row[...] = jnp.zeros((1, depth), F32)
        clock.play(reduce.end(next_cot))
        lanes = depth // LN
        for j in range(lanes):
            gain_buf[0, f, l * lanes + j:l * lanes + j + 1] = gain_row[:, j * LN:(j + 1) * LN]

    def gain_copy(stage, j):
        axis, pos, size = axes[stage]
        return pltpu.make_async_remote_copy(
            src_ref=gain_buf.at[stage, pos], dst_ref=gain_buf.at[stage, pos],
            send_sem=g_send.at[stage], recv_sem=g_recv.at[stage],
            device_id=env.device(axis, j), device_id_type=LOGICAL)

    def gain_send(stage):
        for j in range(1, axes[stage][2]):
            gain_copy(stage, j).start()
        clock.after(clock.now + 2 * EXCHANGE, functools.partial(gain_sum, stage))

    def gain_sum(stage):
        axis, pos, size = axes[stage]
        wait_for(gain_buf.at[stage, first(size - 1)], g_recv.at[stage], env.device(axis, 1))
        total = gain_buf[stage, 0]
        for i in range(1, size):
            total = total + gain_buf[stage, i]
        if stage == 2:
            gain_out[...] = total
        else:
            gain_buf[stage + 1, axes[stage + 1][1]] = total
            gain_send(stage + 1)

    gain_send(0)

    for target in (partner, dev(1), dev(-1)):
        pl.semaphore_signal(credit, device_id=fid[id(target)], device_id_type=LOGICAL)
    pl.semaphore_wait(credit, 3)
    reduce = Reduce(2, 0, tok)
    clock.play(reduce.pairs([], functools.partial(product, last, GA, (last,)), FORWARD))
    clock.play(reduce.start())
    clock.play(reduce.mid())

    def output(rows, total):
        H[0, rows] = (H[last, rows].astype(F32) + total).astype(BF16)
    clock.play(reduce.end(output))
    y_copy = pltpu.make_async_copy(H.at[0], y_ref, io_sem.at[2])
    y_copy.start()
    while clock.queue:
        clock.step()

    y_copy.wait()
    for gather in fwd[last]:
        gather.drain()
    for l, m, rows, lane in [straight[1:]] + [args for l in range(layers) for args in wx_sets(l)]:
        wait_for(WB.at[l, m, first(nf - 1), rows], wx_send.at[lane], env.device("fsdp", 1), True)
    for l in range(layers):
        for m in BOTH:
            if l:
                wz_copy(l, m).wait_send()
            wait_for(WB.at[l, m, :, first(3 * share(l, m).size)], wy_send.at[2 * l + m], env.device("replica", 1), True)
    for job in jobs.values():
        for phase in BOTH:
            job.wait_sends(1, phase)
    for stage, (axis, _, size) in enumerate(axes):
        wait_for(gain_buf.at[stage, first(size - 1)], g_send.at[stage], env.device(axis, 1), True)
    pltpu.make_async_copy(G, out_ref, out_sem).wait()


def fused_step(x, dy, wg, wu, wd, gain, dims):
    layers, ny, nz, nf, tok, depth, hid = dims
    nx = nf // 2
    vm, hbm = pl.BlockSpec(memory_space=pltpu.VMEM), pl.BlockSpec(memory_space=pl.ANY)
    dma = pltpu.SemaphoreType.DMA
    three, two, more = (dma((n,)) for n in (layers, 2 * layers, 2 * layers + 1))
    blocks = (layers, ny, nz, 3 * nf, RS, LN)
    lines = layers * depth // LN
    wide = max(nf, ny, nz)
    return pl.pallas_call(
        functools.partial(step_kernel, dims),
        out_shape=(jax.ShapeDtypeStruct((tok, depth), BF16), jax.ShapeDtypeStruct(blocks, F32), jax.ShapeDtypeStruct((lines, LN), F32)),
        in_specs=[hbm] * 5 + [vm],
        out_specs=(hbm, hbm, vm),
        scratch_shapes=[
            pltpu.VMEM((layers, 2, nf, depth // nf, hid), BF16),
            pltpu.VMEM((layers, hid, depth), BF16),
            pltpu.VMEM((layers, nf, tok, depth), BF16),
            pltpu.VMEM((layers, nx, 2, tok, hid), BF16),
            pltpu.VMEM((layers, nx, 2, tok, hid), BF16),
            pltpu.VMEM((2, nf, tok, depth), BF16),
            pltpu.VMEM((nx, 2, tok, depth), F32),
            pltpu.VMEM((nx, tok, depth), F32),
            pltpu.VMEM((2, 3, tok // 2, depth), F32),
            pltpu.VMEM((layers, tok, depth), BF16),
            pltpu.VMEM((2, nx, 2, tok, hid), BF16),
            pltpu.VMEM(blocks, F32),
            pltpu.VMEM(blocks[1:], F32),
            pltpu.VMEM((layers, 2 * nf, RS, LN), F32),
            pltpu.VMEM((3, wide, lines, LN), F32),
            pltpu.VMEM((1, depth), F32),
            three, dma((3 * (OWN + 1),)), two, dma((3 * (nx + 2),)),
            more, more, two, two, two, dma((4 * layers,)), more, three,
            dma((20 * layers,)), dma((10 * layers * (ny // 2 + nz // 2),)),
            two, two, three, three, dma, three,
            *[pltpu.SemaphoreType.REGULAR((layers, DOWN + 1))] * 2, pltpu.SemaphoreType.REGULAR,
        ],
        compiler_params=pltpu.CompilerParams(collective_id=0, has_side_effects=True, vmem_limit_bytes=67043328),
        name="fused_step",
    )(x, dy, wg, wu, wd, gain)


def unpack_kernel(g_ref, gate_ref, up_ref, down_ref):
    ny, nzb, units = g_ref.shape[:3]
    nf = units // 3
    for k in range(nzb):
        for i in range(ny):
            for m, ref in enumerate((gate_ref, up_ref)):
                for j in range(nf):
                    col = (j * ny + i) * LN
                    ref[k * RS:(k + 1) * RS, col:col + LN] = g_ref[i, k, m * nf + j]
            for h in BOTH:
                for r in range(nf // 2):
                    row, col = (k * (nf // 2) + r) * RS, (2 * i + h) * LN
                    down_ref[row:row + RS, col:col + LN] = g_ref[i, k, 2 * nf + h * (nf // 2) + r]


def unpack(out, dims, steps=4):
    layers, ny, nz, nf = dims
    nzb = nz // steps
    wide, tall = nf * ny * LN, (nf // 2) * RS
    return pl.pallas_call(
        unpack_kernel, grid=(layers, steps),
        in_specs=[pl.BlockSpec((None, ny, nzb, 3 * nf, RS, LN), lambda l, z: (l, 0, z, 0, 0, 0))],
        out_specs=[pl.BlockSpec((None, nzb * RS, wide), lambda l, z: (l, z, 0))] * 2
        + [pl.BlockSpec((None, nzb * tall, 2 * ny * LN), lambda l, z: (l, z, 0))],
        out_shape=[jax.ShapeDtypeStruct((layers, nz * RS, wide), F32)] * 2
        + [jax.ShapeDtypeStruct((layers, nz * tall, 2 * ny * LN), F32)],
        name="unpack")(out)


TOKEN_AXES = ("dp", "replica", "fsdp")


def solution(mesh):
    ny, nz, nf = mesh.shape["replica"], mesh.shape["dp"], mesh.shape["fsdp"]
    tok_spec, shard_spec, full_spec = P(TOKEN_AXES, None), P(None, "fsdp", None), P(None, None)

    def device_step(x, dy, wg, wu, wd, gain):
        layers, depth = gain.shape
        dims = (layers, ny, nz, nf)
        out, blocks, gain_sum = fused_step(x, dy, wg, wu, wd, gain, dims + (x.shape[0], depth, wd.shape[1]))
        dw_gate, dw_up, dw_down = unpack(blocks, dims)
        return out, dw_gate, dw_up, dw_down, gain_sum.reshape(gain.shape)

    return jax.shard_map(
        device_step, mesh=mesh, in_specs=(tok_spec, tok_spec, shard_spec, shard_spec, shard_spec, full_spec),
        out_specs=(tok_spec, shard_spec, shard_spec, shard_spec, full_spec), check_vma=False)
```

```python
import functools
import heapq
import jax
import jax.numpy as jnp
from jax import lax
from jax.sharding import PartitionSpec as P
from jax.experimental import pallas as pl
from jax.experimental.pallas import tpu as pltpu

F32 = jnp.float32
BF16 = jnp.bfloat16
LOGICAL = pl.DeviceIdType.LOGICAL
RS, LN = 16, 128
UNIT_BYTES = RS * LN * 4
NORM_EPS = 1e-6
NN = (((1,), (0,)), ((), ()))
NT = (((1,), (1,)), ((), ()))
TN = (((0,), (0,)), ((), ()))
LINK_RATE, CORE_RATE, HOP, CORE_HOP, STEP_COST, HBM_READ, ENTRY = 46.6e3, 500e3, 2.2, 0.9, 0.15, 1.1, 3.5
CORES = "cores"
BOTH, SIGN, BF16_BYTES = (0, 1), (1, -1), 2
FIRST, SECOND, PASS, RELAY, FAR, OWN = range(6)
DIRECT = "direct"
FORWARD, BACKWARD, WEIGHT, ADD, EXCHANGE = 0.7, 0.95, 0.9, 0.15, 5.0


def dot(a, b, dims=NN):
    return lax.dot_general(a, b, dims, preferred_element_type=F32)


def loop(count, work):
    repeat(0, count, work)


def repeat(start, stop, work):
    def step(i, carry):
        work(i)
        return carry
    lax.fori_loop(start, stop, step, 0)


def wait_for(view, sem, device, sent=False):
    copy = pltpu.make_async_remote_copy(
        src_ref=view, dst_ref=view, send_sem=sem, recv_sem=sem, device_id=device, device_id_type=LOGICAL)
    if sent:
        copy.wait_send()
    else:
        copy.wait_recv()


def first(count):
    return pl.ds(0, count)


def wrap(value, size):
    return lax.rem(value + 4 * size, size)


class Clock:
    def __init__(self):
        self.now, self.queue, self.count, self.links = 0.0, [], 0, {}

    def send(self, link, size):
        near = link == CORES
        start = max(self.now, self.links.get(link, 0.0))
        self.links[link] = start + size / (CORE_RATE if near else LINK_RATE)
        return self.links[link] + (CORE_HOP if near else HOP)

    def after(self, ready, work):
        self.count += 1
        heapq.heappush(self.queue, (ready, self.count, work))

    def step(self):
        ready, _, work = heapq.heappop(self.queue)
        self.now = max(self.now, ready) + STEP_COST
        work()

    def run(self, until):
        while self.queue and self.queue[0][0] <= until:
            self.step()

    def busy(self, spent):
        self.now += spent
        self.run(self.now)

    def idle(self, until):
        self.run(until)
        self.now = max(self.now, until)

    def play(self, task):
        for ready in task:
            self.idle(ready)

    def spawn(self, task):
        ready = next(task, None)
        if ready is not None:
            self.after(ready, functools.partial(self.spawn, task))

    def until(self, done):
        while not done():
            self.step()

    def known(self, times, key):
        while key not in times:
            yield self.now + STEP_COST
        yield times[key]


class Job:
    def __init__(self, env, layer, part):
        parts = LAST_SIZES if layer == env.last else PART_SIZES
        sizes, start = (parts[part], env.nf - parts[part]), part * env.nf
        before = sum(parts[:part])
        offsets = before, start - before
        self.split = sum(parts)
        swap = () if part == DOWN else (part,)
        self.env, self.layer, self.part, self.swap = env, layer, part, swap
        self.sizes, self.offsets, self.starts = sizes, offsets, (start, start + sizes[0])
        self.left, self.turned = len(BOTH), 0
        above = env.above(self)
        self.slots = dict(env.jobs[above].slots) if above else {}
        for gather in BOTH[1:] if above else BOTH:
            for phase in BOTH:
                for k in BOTH:
                    self.slots[gather, phase, k] = env.sends, env.receives
                    env.sends += 1
                    env.receives += self.half_ring(phase, k)

    def ring(self, phase, k):
        return ("replica", "dp")[phase ^ k]

    def half_ring(self, phase, k):
        return self.env.size[self.ring(phase, k)] // 2

    def block(self, phase, k, index, side=None):
        env, G, layer = self.env, self.env.G, self.layer
        start, size = self.starts[k], self.sizes[k]
        if side is not None:
            start, size = start + side * (size // 2), size // 2
        units = pl.ds(start, size)
        if phase == 0:
            return G.at[layer, index, :, units] if k == 0 else G.at[layer, :, index, units]
        return G.at[layer, env.y, index, units] if k == 0 else G.at[layer, index, env.z, units]

    def stage(self, phase, k, d, step, side=None):
        env = self.env
        ref, lead = (env.G, (0,)) if self.layer == env.last else (env.S, ())
        base = 0 if k == 0 else self.split
        offset, size = self.offsets[k], self.sizes[k]
        half_total = ((env.units - self.split) if k else self.split) // 2
        at = 2 * (step - 1) + d
        if step == 0:
            units = pl.ds(base + d * half_total + offset // 2, size // 2)
            at = env.nz - 2 if self.ring(phase, k) == "dp" else 2
        elif side is None:
            units = pl.ds(base + offset, size)
        else:
            units = pl.ds(base + offset + side * (size // 2), size // 2)
        every = slice(None)
        if phase == 0:
            place = (at, every) if k == 0 else (every, at)
        else:
            place = (env.ny - 1, at) if k == 0 else (at, env.nz - 1)
        return ref.at[(*lead, *place, units)]

    def many(self, phase, k, count):
        G, some, every = self.env.G, first(count), slice(None)
        units = pl.ds(self.starts[k], self.sizes[k])
        other = every if phase == 0 else 0
        place = (some, other) if phase == k else (other, some)
        return G.at[(self.layer, *place, units)]

    def copy(self, gather, phase, k, d, step, src, dst):
        env = self.env
        send, receive = self.slots[gather, phase, k]
        return pltpu.make_async_remote_copy(
            src_ref=src, dst_ref=dst, send_sem=env.send_sem.at[send], recv_sem=env.recv_sem.at[receive + step],
            device_id=env.device(self.ring(phase, k), SIGN[d]), device_id_type=LOGICAL)

    def take(self, gather, phase, k, step, blocks):
        receive = self.slots[gather, phase, k][1]
        wait_for(self.many(phase, k, blocks), self.env.recv_sem.at[receive + step], self.env.device(self.ring(phase, k), 1))

    def send_time(self, phase, k, d, units):
        env = self.env
        other = (env.nz if k == 0 else env.ny) if phase == 0 else 1
        return env.clock.send((self.ring(phase, k), d), units * other * UNIT_BYTES)

    def reduce_send(self, phase, k, step, early=False):
        size, ready = self.sizes[k], 0.0
        for d in BOTH:
            side = None if step > 1 else BOTH[d - 1] if early else d
            index = self.env.near(self.ring(phase, k), SIGN[d] * (self.half_ring(phase, k) - step))
            stage = self.stage(phase, k, d, step, None if step == 0 else side)
            self.copy(0, phase, k, d, step, self.block(phase, k, index, side), stage).start()
            ready = max(ready, self.send_time(phase, k, d, size if step > 1 else size // 2))
        if not early:
            self.env.clock.after(ready, functools.partial(self.reduce_step, phase, k, step))

    def reduce_start(self, phase, k):
        self.reduce_send(phase, k, 0)
        self.reduce_send(phase, k, 1, True)

    def start(self, phase, k):
        env = self.env
        if phase == 0 and k == 0 and env.above(self):
            pl.semaphore_wait(env.freed.at[env.above(self)], 4)
        self.reduce_start(phase, k)

    def reduce_step(self, phase, k, step):
        half = self.half_ring(phase, k)
        self.take(0, phase, k, step, len(BOTH) if step else 1)
        for d in BOTH:
            index = self.env.near(self.ring(phase, k), SIGN[d] * (half - 1 - step))
            self.block(phase, k, index, None if step else d)[...] += self.stage(phase, k, d, step)[...]
        if step + 1 < half:
            self.reduce_send(phase, k, step + 1)
        elif phase == 0:
            self.halfway()
            self.env.begin(self, 1, k)
        else:
            self.left -= 1
            if self.left == 0:
                self.reduced()

    def halfway(self):
        env, here = self.env, (self.layer, self.part)
        self.turned += 1
        if self.turned == len(BOTH):
            self.wait_sends(0, 0)
            if 0 < self.layer < env.last:
                self.tell(env.freed)
            env.half.add(here)
            env.begin_waiting()

    def tell(self, flags):
        for axis in ("replica", "dp"):
            for sign in SIGN:
                pl.semaphore_signal(flags.at[self.layer, self.part], device_id=self.env.device(axis, sign), device_id_type=LOGICAL)

    def wait_sends(self, gather, phase):
        for k in BOTH:
            ring = self.ring(phase, k)
            send = self.slots[gather, phase, k][0]
            wait_for(self.many(phase, k, self.env.size[ring] - 1), self.env.send_sem.at[send], self.env.device(ring, 1), True)

    def x_copy(self, m, peer, sender):
        env = self.env
        lane = 2 * self.layer + m
        return pltpu.make_async_remote_copy(
            src_ref=env.G.at[self.layer, env.y, env.z, m * env.nf + peer], dst_ref=env.R.at[self.layer, m * env.nf + sender],
            send_sem=env.x_send.at[lane], recv_sem=env.x_recv.at[lane],
            device_id=env.row + peer, device_id_type=LOGICAL)

    def reduced(self):
        env = self.env
        self.wait_sends(0, 1)
        self.tell(env.ready)
        for m in self.swap:
            repeat(1, env.nf, lambda j: self.x_copy(m, wrap(env.f + j, env.nf), env.f).start())
        env.reduced.add((self.layer, self.part))
        env.clock.after(env.clock.now + (EXCHANGE if self.swap else HOP), self.exchanged)

    def exchanged(self):
        env = self.env
        f, nf = env.f, env.nf
        for m in self.swap:
            env.R[self.layer, m * nf + f] = env.G[self.layer, env.y, env.z, m * nf + f]
        for m in self.swap:
            lane, view = 2 * self.layer + m, env.R.at[self.layer, first(nf - 1)]
            wait_for(view, env.x_send.at[lane], env.device("fsdp", 1), True)
            wait_for(view, env.x_recv.at[lane], env.device("fsdp", 1))
        for m in self.swap:
            env.G[self.layer, env.y, env.z, pl.ds(m * nf, nf)] = env.R[self.layer, pl.ds(m * nf, nf)]
        pl.semaphore_wait(env.ready.at[self.layer, self.part], 4)
        self.left = 2
        for k in BOTH:
            self.gather_send(1, k, 0)
        env.exchanged.add((self.layer, self.part))
        env.begin_waiting()

    def gather_send(self, phase, k, step):
        half, ready = self.half_ring(phase, k), 0.0
        for d in BOTH:
            side = d if step + 1 == half else None
            view = self.block(phase, k, self.env.near(self.ring(phase, k), -SIGN[d] * step), side)
            self.copy(1, phase, k, d, step, view, view).start()
            ready = max(ready, self.send_time(phase, k, d, self.sizes[k] if side is None else self.sizes[k] // 2))
        self.env.clock.after(ready, functools.partial(self.gather_step, phase, k, step))

    def gather_step(self, phase, k, step):
        env = self.env
        last = step + 1 == self.half_ring(phase, k)
        self.take(1, phase, k, step, 1 if last else len(BOTH))
        if not last:
            self.gather_send(phase, k, step + 1)
        elif phase == 1:
            self.gather_send(0, k, 0)
        else:
            self.left -= 1
            here = (self.layer, slice(None), slice(None), pl.ds(self.starts[k], self.sizes[k]))
            pltpu.make_async_copy(env.G.at[here], env.out_ref.at[here], env.out_sem).start()


class Env:
    def __init__(self, dims):
        self.exchanged, self.reduced, self.half, self.waiting, self.clock = set(), set(), set(), [], Clock()
        self.sends = self.receives = 0
        self.ny, self.nz, self.nf = dims[1:4]
        self.last = dims[0] - 1
        self.f, self.y, self.z = lax.axis_index("fsdp"), lax.axis_index("replica"), lax.axis_index("dp")
        self.size = {"fsdp": self.nf, "replica": self.ny, "dp": self.nz}
        self.pos = {"fsdp": self.f, "replica": self.y, "dp": self.z}
        stride = {"fsdp": 1, "replica": self.nf, "dp": self.nf * self.ny}
        me = self.f + stride["replica"] * self.y + stride["dp"] * self.z
        self.row = me - self.f
        self.shift = {a: [wrap(self.pos[a] + k, n) for k in range(n)] for a, n in self.size.items()}
        self.ids = {a: [me + (p - self.pos[a]) * stride[a] for p in self.shift[a]] for a in self.size}

    def near(self, axis, k):
        return self.shift[axis][k % self.size[axis]]

    def device(self, axis, k):
        return self.ids[axis][k % self.size[axis]]

    def above(self, job):
        return (job.layer + 1, job.part) if job.layer + 1 < self.last else None

    def begin(self, job, phase, k):
        self.waiting.append((job, phase, k))
        self.begin_waiting()

    def begin_job(self, job):
        for k in BOTH:
            self.begin(job, 0, k)

    def begin_waiting(self):
        for item in list(self.waiting):
            job, phase, k = item
            if item in self.waiting and (not self.above(job) or self.above(job) in (self.exchanged if phase else self.half)):
                self.waiting.remove(item)
                job.start(phase, k)

    def settle(self, layer):
        self.clock.until(lambda: {(layer, part) for part in (GATE, UP, DOWN)} <= self.reduced)


GATE, UP, DOWN = range(3)
PART_SIZES, LAST_SIZES = (4, 6, 6), (6, 4, 4)


def step_kernel(dims, x_ref, dy_ref, wg_ref, wu_ref, wd_ref, gain_ref, y_ref, out_ref, gain_out,
                WB, WD, N, GA, UA, DH, O, DS, MS, H, DGU, G, S, R, gain_buf, gain_row,
                ag_send, ag_recv, rs_send, rs_recv, wx_send, wx_recv, wz_send, wz_recv, wy_send, wy_recv, w_sem, wd_sem,
                j_send, j_recv, x_send, x_recv, g_send, g_recv, out_sem, io_sem, ready, freed, credit):
    layers, ny, nz, nf, tok, depth, hid = dims
    nx, q = nf // 2, depth // nf // ny
    tile = min(256, depth)
    last = layers - 1

    env = Env(dims)
    f, y, z = env.f, env.y, env.z
    x, c = f // 2, f % 2
    env.G, env.S, env.R, env.out_ref = G, S, R, out_ref
    env.send_sem, env.recv_sem = j_send, j_recv
    env.x_send, env.x_recv, env.ready, env.freed, env.out_sem = x_send, x_recv, ready, freed, out_sem
    env.units = 3 * nf
    clock = env.clock
    env.jobs = jobs = {}
    for l in reversed(range(layers)):
        for part in (GATE, UP, DOWN):
            jobs[l, part] = Job(env, l, part)

    chips = [wrap(x + k, nx) for k in range(nx)]
    same, opposite_core = [2 * p + c for p in chips], [2 * p + (1 - c) for p in chips]
    fid = {id(v): env.row + v for v in same + opposite_core}

    def dev(off, opposite=False):
        return (opposite_core if opposite else same)[off % nx]

    partner = dev(0, True)
    axes = [("fsdp", f, nf), ("replica", y, ny), ("dp", z, nz)]

    barrier = pltpu.get_barrier_semaphore()
    for axis, pos, size in axes:
        for j in range(1, size):
            pl.semaphore_signal(barrier, device_id=env.device(axis, j), device_id_type=LOGICAL)

    x_copy = pltpu.make_async_copy(x_ref, H.at[0], io_sem.at[0])
    dy_copy = pltpu.make_async_copy(dy_ref, DH.at[last % 2, f], io_sem.at[1])
    x_copy.start()
    dy_copy.start()
    wd_copies = [pltpu.make_async_copy(wd_ref.at[l], WD.at[l], wd_sem.at[l]) for l in range(layers)]
    weights = (wg_ref, wu_ref)
    y_at = [env.near("replica", k) for k in range(ny)]
    parts = (first(nf // 2), pl.ds(nf // 2, nf // 2))
    direct = pl.ds(ny * q // 2, ny * q // 2)
    direct_lane = 2 * layers
    shared = {}

    def share(l, m, hops=0):
        size = q // 2 if (l, m) == BOTH else q
        return pl.ds(y_at[hops % ny] * size, size)

    odd = lax.rem(z, 2)
    z_partner = env.ids["dp"][0] + (1 - 2 * odd) * nf * ny

    def fetched(l, m, other=False):
        if l == 0:
            return share(l, m)
        return pl.ds(y_at[0] * q + (1 - odd if other else odd) * (q // 2), q // 2)

    def wz_copy(l, m, other=False):
        view = WB.at[l, m, :, fetched(l, m, other)]
        return pltpu.make_async_remote_copy(
            src_ref=view, dst_ref=view, send_sem=wz_send.at[2 * l + m], recv_sem=wz_recv.at[2 * l + m],
            device_id=z_partner, device_id_type=LOGICAL)

    def own_rows(l, m, rows, sem):
        src = weights[m].at[l, rows, pl.ds(pl.multiple_of(f * hid, hid), hid)]
        return pltpu.make_async_copy(src, WB.at[l, m, f, rows], w_sem.at[sem])

    own_copies = {(l, m): own_rows(l, m, fetched(l, m), 2 * l + m) for l in range(layers) for m in BOTH}
    own_copies[DIRECT] = own_rows(*BOTH, direct, 2 * layers)
    for copy in own_copies.values():
        copy.start()
    for copy in wd_copies:
        copy.start()
    pl.semaphore_wait(barrier, nf + ny + nz - 3)
    clock.busy(ENTRY)

    def wx_copy(l, m, peer, sender, rows, lane):
        return pltpu.make_async_remote_copy(
            src_ref=weights[m].at[l, rows, pl.ds(pl.multiple_of(peer * hid, hid), hid)], dst_ref=WB.at[l, m, sender, rows],
            send_sem=wx_send.at[lane], recv_sem=wx_recv.at[lane], device_id=env.row + peer, device_id_type=LOGICAL)

    def wx_sets(l):
        return [(l, m, fetched(l, m), 2 * l + m) for m in BOTH]

    def wx_post(key, l, m, rows, lane):
        repeat(1, nf, lambda j: wx_copy(l, m, wrap(f + j, nf), f, rows, lane).start())
        for d in BOTH:
            shared[key] = clock.send(d, nx * rows.size * hid * BF16_BYTES) + HBM_READ

    def wx_take(key, l, m, rows, lane):
        yield from clock.known(shared, key)
        own_copies[key].wait()
        wait_for(WB.at[l, m, first(nf - 1), rows], wx_recv.at[lane], env.device("fsdp", 1))

    def wx_start(l):
        for args in wx_sets(l):
            wx_post(args[:2], *args)

    def wy_copy(l, m, kind, d, arrived=False):
        hops = (kind == PASS) + arrived
        lane = 2 * l + m
        part = parts[BOTH[d - (kind == SECOND)]]
        view = WB.at[l, m, part, share(l, m, -SIGN[d] * hops)]
        return pltpu.make_async_remote_copy(
            src_ref=view, dst_ref=view, send_sem=wy_send.at[lane], recv_sem=wy_recv.at[2 * lane + (kind > FIRST)],
            device_id=env.device("replica", SIGN[d]), device_id_type=LOGICAL)

    def wy_send_one(l, m, kind, d):
        wy_copy(l, m, kind, d).start()
        shared[l, m, kind, d] = clock.send(("replica", d), nf // 2 * share(l, m).size * hid * BF16_BYTES)

    def wy_take(l, m, later):
        for kind in (SECOND, PASS) if later else (FIRST,):
            for d in BOTH:
                yield from clock.known(shared, (l, m, kind, d))
        rows = first(share(l, m).size * (1 + later))
        wait_for(WB.at[l, m, :, rows], wy_recv.at[2 * (2 * l + m) + later], env.device("replica", 1))

    def weights_task():
        for l in range(layers):
            for args in wx_sets(l):
                yield from wx_take(args[:2], *args)
                if l:
                    wz_copy(*args[:2]).start()
                    yield clock.send(("dp", 0), nf * q // 2 * hid * BF16_BYTES)
                    wz_copy(*args[:2], True).wait_recv()
                for kind in (FIRST, SECOND):
                    for d in BOTH:
                        wy_send_one(*args[:2], kind, d)
            for m in BOTH:
                yield from wy_take(l, m, 0)
                for d in BOTH:
                    wy_send_one(l, m, PASS, d)

    def weights_here(l):
        while l in claimed and l not in arrived:
            yield clock.now + STEP_COST
        if l in arrived:
            return
        claimed.add(l)
        if l == 0:
            yield from wx_take(*straight)
        for m in BOTH:
            yield from wy_take(l, m, 1)
        wd_copies[l].wait()
        arrived.add(l)

    claimed, arrived = set(), set()
    straight = DIRECT, *BOTH, direct, direct_lane

    class Gather:
        def __init__(self, lanes, buf, slot, base, size):
            self.lanes, self.buf, self.slot, self.ready = lanes, buf, slot, {}
            self.whole = pl.ds(base, size)
            self.halves = (pl.ds(base, size // 2), pl.ds(base + size // 2, size // 2))

        def copy(self, kind, d):
            hops = (kind in (PASS, RELAY)) + (kind == FAR) * nx // len(BOTH)
            block = dev(-SIGN[d] * hops)
            rows = self.whole if kind in (RELAY, OWN) else self.halves[d - (kind == SECOND)]
            target = partner if kind in (RELAY, FAR, OWN) else dev(SIGN[d])
            view = self.buf.at[self.slot, block, rows]
            return rows.size, pltpu.make_async_remote_copy(
                src_ref=view, dst_ref=view, send_sem=ag_send.at[self.lanes], recv_sem=ag_recv.at[self.lanes * (OWN + 1) + kind],
                device_id=fid[id(target)], device_id_type=LOGICAL)

        def send(self, *kinds):
            for kind in kinds:
                ready = 0.0
                for d in BOTH[:1] if kind == OWN else BOTH:
                    size, copy = self.copy(kind, d)
                    copy.start()
                    ready = max(ready, clock.send(CORES if kind in (RELAY, FAR, OWN) else d, size * depth * BF16_BYTES))
                self.ready[kind] = ready

        def blocks(self, count):
            return self.buf.at[self.slot, first(count), self.whole]

        def take(self, *kinds):
            for kind in kinds:
                yield from clock.known(self.ready, kind)
                wait_for(self.blocks(2 if kind == RELAY else 1), ag_recv.at[self.lanes * (OWN + 1) + kind], fid[id(partner)])

        def start(self):
            self.send(FIRST, OWN, SECOND)

        def mid(self):
            for kind, onward in ((FIRST, PASS), (SECOND, RELAY)):
                yield from self.take(kind)
                self.send(onward)

        def end(self):
            yield from self.take(PASS)
            self.send(FAR)

        def drain(self):
            wait_for(self.blocks(nf - 1), ag_send.at[self.lanes], fid[id(partner)], True)

    chunk = min(16, tok // 8)

    def rows_at(start, j):
        return pl.ds(pl.multiple_of(start + j * chunk, chunk), chunk)

    class Reduce:
        def __init__(self, lanes, base, size):
            self.lanes, self.base, self.size, self.arrive = lanes, base, size, {}
            self.rows, self.local = pl.ds(base, size), pl.ds(base // 2, size // 2)

        def d2d(self, i, xp, core):
            return pltpu.make_async_remote_copy(
                src_ref=O.at[xp, core, self.rows], dst_ref=DS.at[xp, self.rows], send_sem=rs_send.at[2 * self.lanes],
                recv_sem=rs_recv.at[(nx + 2) * self.lanes + i], device_id=fid[id(partner)], device_id_type=LOGICAL)

        def msg(self, k, d):
            half = self.size // 2
            lane = (nx + 2) * self.lanes + nx + (k > 0)
            off, side = (2, d) if k == 0 else (SIGN[d], d if k == 3 else 1 - d)
            size, slot, at = half, (0 if k == 0 else 2), 0
            if k in (1, 2):
                size, slot = half // 2, 1
                at = (k - 1) * size
            return size, pltpu.make_async_remote_copy(
                src_ref=O.at[chips[off % nx], c, pl.ds(self.base + side * half + at, size)],
                dst_ref=MS.at[d, slot, pl.ds(self.base // 2 + at, size)],
                send_sem=rs_send.at[2 * self.lanes + 1], recv_sem=rs_recv.at[lane], device_id=fid[id(dev(SIGN[d]))], device_id_type=LOGICAL)

        def post(self, k, d):
            size, copy = self.msg(k, d)
            copy.start()
            self.arrive[k, d] = clock.send(d, size * depth * 4)

        def take(self, later):
            yield max(self.arrive[k, d] for k in ((1, 2, 3) if later else (0,)) for d in BOTH)
            view = MS.at[:, pl.ds(later, 1 + later), self.local]
            wait_for(view, rs_recv.at[(nx + 2) * self.lanes + nx + later], fid[id(partner)])

        def combine(self, i, off):
            xp = chips[off % nx]
            yield self.arrive[i]
            self.d2d(i, xp, c).wait_recv()

            def add(j):
                rows = rows_at(self.base, j)
                O[xp, c, rows] += DS[xp, rows]
            loop(self.size // chunk, add)
            clock.busy(ADD)

        def near(self):
            for i, d in ((1, 0), (2, 1)):
                yield from self.combine(i, SIGN[d])
                self.post(1, d)

        def start(self):
            yield from self.combine(3, 2)
            for k in (0, 2):
                for d in BOTH:
                    self.post(k, d)
            yield from self.combine(0, 0)

        def mid(self):
            half = self.size // 2
            yield from self.take(0)
            for d in BOTH:
                def add(j):
                    rows = rows_at(self.base + d * half, j)
                    O[chips[SIGN[d] % nx], c, rows] += MS[d, 0, rows_at(self.base // 2, j)]
                loop(half // chunk, add)
                self.post(3, d)

        def end(self, body):
            half = self.size // 2
            yield from self.take(1)
            for side in BOTH:
                def step(j):
                    rows, local = rows_at(self.base + side * half, j), rows_at(self.base // 2, j)
                    body(rows, O[x, c, rows] + (MS[0, 2 - side, local] + MS[1, 1 + side, local]))
                loop(half // chunk, step)
            clock.busy(5 * ADD)
            wait_for(O.at[:, 0, self.rows], rs_send.at[2 * self.lanes], fid[id(partner)], True)
            wait_for(O.at[first(nx - 1), 0, self.rows], rs_send.at[2 * self.lanes + 1], fid[id(partner)], True)

        def pairs(self, gathers, body, cost, after_mid=None):
            def step(i):
                xp = wrap(x + i + i // 2 - 2 * (i // 3), nx)
                body(xp, self.rows)
                self.d2d(i, xp, 1 - c).start()

            def go(start, stop):
                repeat(start, stop, step)
                for i in range(start, stop):
                    clock.now += cost
                    self.arrive[i] = clock.send(CORES, self.size * depth * 4)
                clock.busy(0.0)

            go(0, 1)
            for gather in gathers:
                yield from gather.take(RELAY)
            go(1, 3)
            late = not all(gather.ready.get(FAR, self.arrive[2]) < self.arrive[2] for gather in gathers)
            if late:
                yield from self.near()
            for gather in gathers:
                yield from gather.take(FAR)
            go(3, nx)
            if not late:
                yield from self.near()

    def rms(hidden):
        return lax.rsqrt(jnp.mean(hidden * hidden, axis=-1, keepdims=True) + NORM_EPS)

    def down_grad(l):
        group = nf // 2
        zs = tile // (group * RS)

        def body(j, carry):
            lhs = GA[l, :, :, :, pl.ds(pl.multiple_of(j * tile, tile), tile)].reshape(-1, tile)
            for i in range(depth // tile):
                res = dot(lhs, DH[l % 2, :, :, pl.ds(i * tile, tile)].reshape(-1, tile), TN)
                for h in range(tile // LN):
                    col = i * (tile // LN) + h
                    for zi in range(zs):
                        rows = res[zi * group * RS:(zi + 1) * group * RS, h * LN:(h + 1) * LN]
                        G[l, col // 2, j * zs + zi, pl.ds(2 * nf + (col % 2) * group, group)] = rows.reshape(group, RS, LN)
            return carry
        lax.fori_loop(0, hid // tile, body, 0)

    def up_grad(l):
        fs = tile // (nz_rows * RS)

        def body(j, carry):
            lhs = N[l, :, :, pl.ds(pl.multiple_of(j * tile, tile), tile)].reshape(-1, tile)
            for m in BOTH:
                for i in range(hid // tile):
                    res = dot(lhs, DGU[m, :, :, :, pl.ds(i * tile, tile)].reshape(-1, tile), TN)
                    for h in range(tile // LN):
                        for fi in range(fs):
                            rows = res[fi * nz_rows * RS:(fi + 1) * nz_rows * RS, h * LN:(h + 1) * LN]
                            G[l, i * (tile // LN) + h, :, m * nf + j * fs + fi] = rows.reshape(nz_rows, RS, LN)
            return carry
        lax.fori_loop(0, depth // tile, body, 0)

    nz_rows = depth // nf // RS
    part = tok // 2
    fwd = [[Gather(g, N, l, g * part, part) for g in BOTH] for l in range(layers)]
    bwd = [Gather(2, DH, l % 2, 0, tok) for l in range(layers)]
    dy_task = bwd[last]

    def activations(l, xp, rows, cols):
        tokens = N[l, pl.ds(2 * xp, 2), rows].reshape(-1, depth)
        gate = dot(tokens, WB[l, 0, :, :, cols].reshape(depth, tile)).astype(BF16)
        up = dot(tokens, WB[l, 1, :, :, cols].reshape(depth, tile)).astype(BF16)
        return gate, up

    def flat(ref, *index):
        value = ref[index]
        return value.reshape(-1, value.shape[-1])

    def product(l, ref, lead, xp, rows):
        prod = flat(ref, *lead, xp, slice(None), rows)
        for j in range(depth // tile):
            cols = pl.ds(j * tile, tile)
            O[xp, :, rows, cols] = dot(prod, WD[l, :, cols]).reshape(2, rows.size, tile)

    def forward(l, xp, rows):
        shape = (2, rows.size, tile)
        for j in range(hid // tile):
            cols = pl.ds(j * tile, tile)
            gate, up = activations(l, xp, rows, cols)
            GA[l, xp, :, rows, cols] = gate.reshape(shape)
            UA[l, xp, :, rows, cols] = up.reshape(shape)
            DGU[0, xp, :, rows, cols] = (jax.nn.silu(gate.astype(F32)) * up.astype(F32)).astype(BF16).reshape(shape)
        product(l, DGU, (0,), xp, rows)

    def backward(l, xp, rows):
        cot = DH[l % 2, pl.ds(2 * xp, 2)].reshape(-1, depth)
        shape = (2, tok, tile)
        for j in range(hid // tile):
            cols = pl.ds(j * tile, tile)
            here = (l, xp, slice(None), slice(None), cols)
            gate, up = activations(l, xp, rows, cols) if l == last else (flat(GA, *here), flat(UA, *here))
            gate, up = gate.astype(F32), up.astype(F32)
            d_prod = dot(cot, WD[l, cols, :], NT).astype(BF16).astype(F32)
            sig = jax.nn.sigmoid(gate)
            GA[here] = (gate * sig * up).astype(BF16).reshape(shape)
            DGU[0, xp, :, :, cols] = (d_prod * up * sig * (1.0 + gate * (1.0 - sig))).astype(BF16).reshape(shape)
            DGU[1, xp, :, :, cols] = (d_prod * gate * sig).astype(BF16).reshape(shape)
        d_gate, d_up = flat(DGU, 0, xp), flat(DGU, 1, xp)
        block = depth // nf
        for j in range(depth // tile):
            sub = pl.ds(j * tile // block, tile // block)
            total = dot(d_gate, WB[l, 0, sub].reshape(tile, hid), NT) + dot(d_up, WB[l, 1, sub].reshape(tile, hid), NT)
            O[xp, :, :, pl.ds(j * tile, tile)] = total.reshape(shape)

    def normalize(l, rows, hidden):
        N[l, f, rows] = (hidden * rms(hidden) * gain_ref[l:l + 1]).astype(BF16)

    def half_task(g):
        for l in range(last):
            gather, reduce = fwd[l][g], Reduce(g, g * part, part)
            yield from gather.mid()
            if g and l == 0:
                wx_start(1)
                dy_task.start()
                clock.spawn(dy_task.mid())
                clock.spawn(dy_task.end())
            if g and l + 2 < layers:
                wx_start(l + 2)
            clock.spawn(gather.end())
            yield from gather.take(OWN)
            yield from weights_here(l)
            yield from reduce.pairs([gather], functools.partial(forward, l), FORWARD / len(BOTH))
            yield from reduce.start()
            yield from reduce.mid()

            def next_hidden(rows, total, l=l):
                hidden = (H[l, rows].astype(F32) + total).astype(BF16)
                H[l + 1, rows] = hidden
                normalize(l + 1, rows, hidden.astype(F32))
            yield from reduce.end(next_hidden)
            gather.drain()
            fwd[l + 1][g].start()
        yield from fwd[last][g].mid()
        yield from fwd[last][g].end()
        finished.add(g)

    finished = set()
    wx_start(0)
    x_copy.wait()
    for g in BOTH:
        def enter(j):
            rows = rows_at(g * part, j)
            normalize(0, rows, H[0, rows].astype(F32))
        loop(part // chunk, enter)
        clock.busy(ADD)
        fwd[0][g].start()
    wx_post(*straight)
    dy_copy.wait()
    clock.spawn(weights_task())
    for g in BOTH:
        clock.spawn(half_task(g))
    clock.until(lambda: FAR in fwd[last][0].ready)

    for l in reversed(range(layers)):
        reduce = Reduce(2, 0, tok)
        if l == last:
            gathers = fwd[l]
            clock.play(dy_task.take(RELAY, FAR, OWN))
            clock.play(weights_here(l))
        else:
            gathers = [bwd[l]]
            bwd[l].start()
            clock.spawn(bwd[l].mid())
            clock.spawn(bwd[l].end())
        for gather in gathers:
            clock.play(gather.take(OWN))
        clock.play(reduce.pairs(gathers, functools.partial(backward, l), FORWARD + BACKWARD if l == last else BACKWARD))
        if l == 0:
            env.settle(last)
        down_grad(l)
        clock.busy(WEIGHT)
        env.begin_job(jobs[l, DOWN])
        clock.play(reduce.start())
        up_grad(l)
        clock.busy(2 * WEIGHT)
        env.begin_job(jobs[l, GATE])
        env.begin_job(jobs[l, UP])
        clock.play(reduce.mid())
        bwd[l].drain()

        def next_cot(rows, total, l=l):
            d_normed = total.astype(BF16).astype(F32)
            hidden = H[l, rows].astype(F32)
            inv = rms(hidden)
            if l > 0:
                scaled = d_normed * gain_ref[l:l + 1]
                cot = DH[l % 2, f, rows].astype(F32)
                d_hidden = cot + inv * scaled - hidden * (inv * inv * inv) * jnp.mean(scaled * hidden, axis=-1, keepdims=True)
                DH[(l - 1) % 2, f, rows] = d_hidden.astype(BF16)
            gain_row[...] += jnp.sum(d_normed * hidden * inv, axis=0, keepdims=True)
        gain_row[...] = jnp.zeros((1, depth), F32)
        clock.play(reduce.end(next_cot))
        lanes = depth // LN
        for j in range(lanes):
            gain_buf[0, f, l * lanes + j:l * lanes + j + 1] = gain_row[:, j * LN:(j + 1) * LN]

    def gain_copy(stage, j):
        axis, pos, size = axes[stage]
        return pltpu.make_async_remote_copy(
            src_ref=gain_buf.at[stage, pos], dst_ref=gain_buf.at[stage, pos],
            send_sem=g_send.at[stage], recv_sem=g_recv.at[stage],
            device_id=env.device(axis, j), device_id_type=LOGICAL)

    def gain_send(stage):
        for j in range(1, axes[stage][2]):
            gain_copy(stage, j).start()
        clock.after(clock.now + 2 * EXCHANGE, functools.partial(gain_sum, stage))

    def gain_sum(stage):
        axis, pos, size = axes[stage]
        wait_for(gain_buf.at[stage, first(size - 1)], g_recv.at[stage], env.device(axis, 1))
        total = gain_buf[stage, 0]
        for i in range(1, size):
            total = total + gain_buf[stage, i]
        if stage == 2:
            gain_out[...] = total
        else:
            gain_buf[stage + 1, axes[stage + 1][1]] = total
            gain_send(stage + 1)

    gain_send(0)

    for target in (partner, dev(1), dev(-1)):
        pl.semaphore_signal(credit, device_id=fid[id(target)], device_id_type=LOGICAL)
    pl.semaphore_wait(credit, 3)
    reduce = Reduce(2, 0, tok)
    clock.play(reduce.pairs([], functools.partial(product, last, GA, (last,)), FORWARD))
    clock.play(reduce.start())
    clock.play(reduce.mid())

    def output(rows, total):
        H[0, rows] = (H[last, rows].astype(F32) + total).astype(BF16)
    clock.play(reduce.end(output))
    y_copy = pltpu.make_async_copy(H.at[0], y_ref, io_sem.at[2])
    y_copy.start()
    while clock.queue:
        clock.step()

    y_copy.wait()
    for gather in fwd[last]:
        gather.drain()
    for l, m, rows, lane in [straight[1:]] + [args for l in range(layers) for args in wx_sets(l)]:
        wait_for(WB.at[l, m, first(nf - 1), rows], wx_send.at[lane], env.device("fsdp", 1), True)
    for l in range(layers):
        for m in BOTH:
            if l:
                wz_copy(l, m).wait_send()
            wait_for(WB.at[l, m, :, first(3 * share(l, m).size)], wy_send.at[2 * l + m], env.device("replica", 1), True)
    for job in jobs.values():
        for phase in BOTH:
            job.wait_sends(1, phase)
    for stage, (axis, _, size) in enumerate(axes):
        wait_for(gain_buf.at[stage, first(size - 1)], g_send.at[stage], env.device(axis, 1), True)
    pltpu.make_async_copy(G, out_ref, out_sem).wait()


def fused_step(x, dy, wg, wu, wd, gain, dims):
    layers, ny, nz, nf, tok, depth, hid = dims
    nx = nf // 2
    vm, hbm = pl.BlockSpec(memory_space=pltpu.VMEM), pl.BlockSpec(memory_space=pl.ANY)
    dma = pltpu.SemaphoreType.DMA
    three, two, more = (dma((n,)) for n in (layers, 2 * layers, 2 * layers + 1))
    blocks = (layers, ny, nz, 3 * nf, RS, LN)
    lines = layers * depth // LN
    wide = max(nf, ny, nz)
    return pl.pallas_call(
        functools.partial(step_kernel, dims),
        out_shape=(jax.ShapeDtypeStruct((tok, depth), BF16), jax.ShapeDtypeStruct(blocks, F32), jax.ShapeDtypeStruct((lines, LN), F32)),
        in_specs=[hbm] * 5 + [vm],
        out_specs=(hbm, hbm, vm),
        scratch_shapes=[
            pltpu.VMEM((layers, 2, nf, depth // nf, hid), BF16),
            pltpu.VMEM((layers, hid, depth), BF16),
            pltpu.VMEM((layers, nf, tok, depth), BF16),
            pltpu.VMEM((layers, nx, 2, tok, hid), BF16),
            pltpu.VMEM((layers, nx, 2, tok, hid), BF16),
            pltpu.VMEM((2, nf, tok, depth), BF16),
            pltpu.VMEM((nx, 2, tok, depth), F32),
            pltpu.VMEM((nx, tok, depth), F32),
            pltpu.VMEM((2, 3, tok // 2, depth), F32),
            pltpu.VMEM((layers, tok, depth), BF16),
            pltpu.VMEM((2, nx, 2, tok, hid), BF16),
            pltpu.VMEM(blocks, F32),
            pltpu.VMEM(blocks[1:], F32),
            pltpu.VMEM((layers, 2 * nf, RS, LN), F32),
            pltpu.VMEM((3, wide, lines, LN), F32),
            pltpu.VMEM((1, depth), F32),
            three, dma((3 * (OWN + 1),)), two, dma((3 * (nx + 2),)),
            more, more, two, two, two, dma((4 * layers,)), more, three,
            dma((20 * layers,)), dma((10 * layers * (ny // 2 + nz // 2),)),
            two, two, three, three, dma, three,
            *[pltpu.SemaphoreType.REGULAR((layers, DOWN + 1))] * 2, pltpu.SemaphoreType.REGULAR,
        ],
        compiler_params=pltpu.CompilerParams(collective_id=0, has_side_effects=True, vmem_limit_bytes=67043328),
        name="fused_step",
    )(x, dy, wg, wu, wd, gain)


def unpack_kernel(blocks_ref, gate_ref, up_ref, down_ref, blocks, gate, up, down, in_sem, out_sem):
    layers, ny, nz, units = blocks.shape[:4]
    nf = units // 3
    pairs, tall = nz // 2, nf // 2 * RS
    count = layers * pairs

    def load(i):
        here = (i // pairs, slice(None), pl.ds(i % pairs * 2, 2))
        return pltpu.make_async_copy(blocks_ref.at[here], blocks.at[here], in_sem.at[i])

    def stores(i):
        for ref, buf, rows in ((gate_ref, gate, RS), (up_ref, up, RS), (down_ref, down, tall)):
            here = (i // pairs, pl.ds(pl.multiple_of(i % pairs * (2 * rows), 2 * rows), 2 * rows))
            yield pltpu.make_async_copy(buf.at[here], ref.at[here], out_sem)

    loop(count, lambda i: load(i).start())

    def move(i):
        load(i).wait()
        l = i // pairs
        for k in BOTH:
            z = i % pairs * 2 + k
            rows = pl.ds(pl.multiple_of(z * RS, RS), RS)
            for y in range(ny):
                for j in range(nf):
                    cols = pl.ds((j * ny + y) * LN, LN)
                    gate[l, rows, cols] = blocks[l, y, z, j]
                    up[l, rows, cols] = blocks[l, y, z, nf + j]
                for j in range(nf):
                    h, r = j // (nf // 2), j % (nf // 2)
                    down[l, pl.ds(pl.multiple_of(z * tall + r * RS, RS), RS), pl.ds((2 * y + h) * LN, LN)] = blocks[l, y, z, 2 * nf + j]
        for copy in stores(i):
            copy.start()
    loop(count, move)
    for buf, ref in ((gate, gate_ref), (up, up_ref), (down, down_ref)):
        pltpu.make_async_copy(buf, ref, out_sem).wait()


def unpack(out, dims):
    layers, ny, nz, nf = dims
    wide, tall = (layers, nz * RS, nf * ny * LN), (layers, nz * nf // 2 * RS, 2 * ny * LN)
    shapes = (wide, wide, tall)
    hbm = pl.BlockSpec(memory_space=pl.ANY)
    return pl.pallas_call(
        unpack_kernel, in_specs=[hbm], out_specs=[hbm] * len(shapes),
        out_shape=[jax.ShapeDtypeStruct(shape, F32) for shape in shapes],
        scratch_shapes=[pltpu.VMEM(out.shape, F32), *[pltpu.VMEM(shape, F32) for shape in shapes],
                        pltpu.SemaphoreType.DMA((layers * nz // 2,)), pltpu.SemaphoreType.DMA],
        compiler_params=pltpu.CompilerParams(vmem_limit_bytes=48 * 2**20),
        name="unpack")(out)


TOKEN_AXES = ("dp", "replica", "fsdp")


def solution(mesh):
    ny, nz, nf = mesh.shape["replica"], mesh.shape["dp"], mesh.shape["fsdp"]
    tok_spec, shard_spec, full_spec = P(TOKEN_AXES, None), P(None, "fsdp", None), P(None, None)

    def device_step(x, dy, wg, wu, wd, gain):
        layers, depth = gain.shape
        dims = (layers, ny, nz, nf)
        out, blocks, gain_sum = fused_step(x, dy, wg, wu, wd, gain, dims + (x.shape[0], depth, wd.shape[1]))
        dw_gate, dw_up, dw_down = unpack(blocks, dims)
        return out, dw_gate, dw_up, dw_down, gain_sum.reshape(gain.shape)

    return jax.shard_map(
        device_step, mesh=mesh, in_specs=(tok_spec, tok_spec, shard_spec, shard_spec, shard_spec, full_spec),
        out_specs=(tok_spec, shard_spec, shard_spec, shard_spec, full_spec), check_vma=False)
```

```python
import functools
import heapq
import jax
import jax.numpy as jnp
from jax import lax
from jax.sharding import PartitionSpec as P
from jax.experimental import pallas as pl
from jax.experimental.pallas import tpu as pltpu

F32 = jnp.float32
BF16 = jnp.bfloat16
LOGICAL = pl.DeviceIdType.LOGICAL
RS, LN = 16, 128
UNIT_BYTES = RS * LN * 4
NORM_EPS = 1e-6
NN = (((1,), (0,)), ((), ()))
NT = (((1,), (1,)), ((), ()))
TN = (((0,), (0,)), ((), ()))
LINK_RATE, CORE_RATE, HOP, CORE_HOP, STEP_COST, HBM_READ, ENTRY = 46.6e3, 500e3, 2.2, 0.9, 0.15, 1.1, 3.5
CORES = "cores"
BOTH, SIGN, BF16_BYTES = (0, 1), (1, -1), 2
FIRST, SECOND, PASS, RELAY, FAR, OWN = range(6)
DIRECT = "direct"
FORWARD, BACKWARD, WEIGHT, ADD, EXCHANGE = 0.7, 0.95, 0.9, 0.15, 5.0


def dot(a, b, dims=NN):
    return lax.dot_general(a, b, dims, preferred_element_type=F32)


def loop(count, work):
    repeat(0, count, work)


def repeat(start, stop, work):
    def step(i, carry):
        work(i)
        return carry
    lax.fori_loop(start, stop, step, 0)


def wait_for(view, sem, device, sent=False):
    copy = pltpu.make_async_remote_copy(
        src_ref=view, dst_ref=view, send_sem=sem, recv_sem=sem, device_id=device, device_id_type=LOGICAL)
    if sent:
        copy.wait_send()
    else:
        copy.wait_recv()


def first(count):
    return pl.ds(0, count)


def wrap(value, size):
    return lax.rem(value + 4 * size, size)


class Clock:
    def __init__(self):
        self.now, self.queue, self.count, self.links = 0.0, [], 0, {}

    def send(self, link, size):
        near = link == CORES
        start = max(self.now, self.links.get(link, 0.0))
        self.links[link] = start + size / (CORE_RATE if near else LINK_RATE)
        return self.links[link] + (CORE_HOP if near else HOP)

    def after(self, ready, work):
        self.count += 1
        heapq.heappush(self.queue, (ready, self.count, work))

    def step(self):
        ready, _, work = heapq.heappop(self.queue)
        self.now = max(self.now, ready) + STEP_COST
        work()

    def run(self, until):
        while self.queue and self.queue[0][0] <= until:
            self.step()

    def busy(self, spent):
        self.now += spent
        self.run(self.now)

    def idle(self, until):
        self.run(until)
        self.now = max(self.now, until)

    def play(self, task):
        for ready in task:
            self.idle(ready)

    def spawn(self, task):
        ready = next(task, None)
        if ready is not None:
            self.after(ready, functools.partial(self.spawn, task))

    def until(self, done):
        while not done():
            self.step()

    def known(self, times, key):
        while key not in times:
            yield self.now + STEP_COST
        yield times[key]


class Job:
    def __init__(self, env, layer, part):
        parts = LAST_SIZES if layer == env.last else PART_SIZES
        sizes, start = (parts[part], env.nf - parts[part]), part * env.nf
        before = sum(parts[:part])
        offsets = before, start - before
        self.split = sum(parts)
        swap = () if part == DOWN else (part,)
        self.env, self.layer, self.part, self.swap = env, layer, part, swap
        self.sizes, self.offsets, self.starts = sizes, offsets, (start, start + sizes[0])
        self.left, self.turned = len(BOTH), 0
        above = env.above(self)
        self.slots = dict(env.jobs[above].slots) if above else {}
        for gather in BOTH[1:] if above else BOTH:
            for phase in BOTH:
                for k in BOTH:
                    self.slots[gather, phase, k] = env.sends, env.receives
                    env.sends += 1
                    env.receives += self.half_ring(phase, k)

    def ring(self, phase, k):
        return ("replica", "dp")[phase ^ k]

    def half_ring(self, phase, k):
        return self.env.size[self.ring(phase, k)] // 2

    def block(self, phase, k, index, side=None):
        env, G, layer = self.env, self.env.G, self.layer
        start, size = self.starts[k], self.sizes[k]
        if side is not None:
            start, size = start + side * (size // 2), size // 2
        units = pl.ds(start, size)
        if phase == 0:
            return G.at[layer, index, :, units] if k == 0 else G.at[layer, :, index, units]
        return G.at[layer, env.y, index, units] if k == 0 else G.at[layer, index, env.z, units]

    def stage(self, phase, k, d, step, side=None):
        env = self.env
        ref, lead = (env.G, (0,)) if self.layer == env.last else (env.S, ())
        base = 0 if k == 0 else self.split
        offset, size = self.offsets[k], self.sizes[k]
        half_total = ((env.units - self.split) if k else self.split) // 2
        at = 2 * (step - 1) + d
        if step == 0:
            units = pl.ds(base + d * half_total + offset // 2, size // 2)
            at = env.nz - 2 if self.ring(phase, k) == "dp" else 2
        elif side is None:
            units = pl.ds(base + offset, size)
        else:
            units = pl.ds(base + offset + side * (size // 2), size // 2)
        every = slice(None)
        if phase == 0:
            place = (at, every) if k == 0 else (every, at)
        else:
            place = (env.ny - 1, at) if k == 0 else (at, env.nz - 1)
        return ref.at[(*lead, *place, units)]

    def many(self, phase, k, count):
        G, some, every = self.env.G, first(count), slice(None)
        units = pl.ds(self.starts[k], self.sizes[k])
        other = every if phase == 0 else 0
        place = (some, other) if phase == k else (other, some)
        return G.at[(self.layer, *place, units)]

    def copy(self, gather, phase, k, d, step, src, dst):
        env = self.env
        send, receive = self.slots[gather, phase, k]
        return pltpu.make_async_remote_copy(
            src_ref=src, dst_ref=dst, send_sem=env.send_sem.at[send], recv_sem=env.recv_sem.at[receive + step],
            device_id=env.device(self.ring(phase, k), SIGN[d]), device_id_type=LOGICAL)

    def take(self, gather, phase, k, step, blocks):
        receive = self.slots[gather, phase, k][1]
        wait_for(self.many(phase, k, blocks), self.env.recv_sem.at[receive + step], self.env.device(self.ring(phase, k), 1))

    def send_time(self, phase, k, d, units):
        env = self.env
        other = (env.nz if k == 0 else env.ny) if phase == 0 else 1
        return env.clock.send((self.ring(phase, k), d), units * other * UNIT_BYTES)

    def reduce_send(self, phase, k, step, early=False):
        size, ready = self.sizes[k], 0.0
        for d in BOTH:
            side = None if step > 1 else BOTH[d - 1] if early else d
            index = self.env.near(self.ring(phase, k), SIGN[d] * (self.half_ring(phase, k) - step))
            stage = self.stage(phase, k, d, step, None if step == 0 else side)
            self.copy(0, phase, k, d, step, self.block(phase, k, index, side), stage).start()
            ready = max(ready, self.send_time(phase, k, d, size if step > 1 else size // 2))
        if not early:
            self.env.clock.after(ready, functools.partial(self.reduce_step, phase, k, step))

    def reduce_start(self, phase, k):
        self.reduce_send(phase, k, 0)
        self.reduce_send(phase, k, 1, True)

    def start(self, phase, k):
        env = self.env
        if phase == 0 and k == 0 and env.above(self):
            pl.semaphore_wait(env.freed.at[env.above(self)], 4)
        self.reduce_start(phase, k)

    def reduce_step(self, phase, k, step):
        half = self.half_ring(phase, k)
        self.take(0, phase, k, step, len(BOTH) if step else 1)
        for d in BOTH:
            index = self.env.near(self.ring(phase, k), SIGN[d] * (half - 1 - step))
            self.block(phase, k, index, None if step else d)[...] += self.stage(phase, k, d, step)[...]
        if step + 1 < half:
            self.reduce_send(phase, k, step + 1)
        elif phase == 0:
            self.halfway()
            self.env.begin(self, 1, k)
        else:
            self.left -= 1
            if self.left == 0:
                self.reduced()

    def halfway(self):
        env, here = self.env, (self.layer, self.part)
        self.turned += 1
        if self.turned == len(BOTH):
            self.wait_sends(0, 0)
            if 0 < self.layer < env.last:
                self.tell(env.freed)
            env.half.add(here)
            env.begin_waiting()

    def tell(self, flags):
        for axis in ("replica", "dp"):
            for sign in SIGN:
                pl.semaphore_signal(flags.at[self.layer, self.part], device_id=self.env.device(axis, sign), device_id_type=LOGICAL)

    def wait_sends(self, gather, phase):
        for k in BOTH:
            ring = self.ring(phase, k)
            send = self.slots[gather, phase, k][0]
            wait_for(self.many(phase, k, self.env.size[ring] - 1), self.env.send_sem.at[send], self.env.device(ring, 1), True)

    def x_copy(self, m, peer, sender):
        env = self.env
        lane = 2 * self.layer + m
        return pltpu.make_async_remote_copy(
            src_ref=env.G.at[self.layer, env.y, env.z, m * env.nf + peer], dst_ref=env.R.at[self.layer, m * env.nf + sender],
            send_sem=env.x_send.at[lane], recv_sem=env.x_recv.at[lane],
            device_id=env.row + peer, device_id_type=LOGICAL)

    def reduced(self):
        env = self.env
        self.wait_sends(0, 1)
        self.tell(env.ready)
        for m in self.swap:
            repeat(1, env.nf, lambda j: self.x_copy(m, wrap(env.f + j, env.nf), env.f).start())
        env.reduced.add((self.layer, self.part))
        env.clock.after(env.clock.now + (EXCHANGE if self.swap else HOP), self.exchanged)

    def exchanged(self):
        env = self.env
        f, nf = env.f, env.nf
        for m in self.swap:
            env.R[self.layer, m * nf + f] = env.G[self.layer, env.y, env.z, m * nf + f]
        for m in self.swap:
            lane, view = 2 * self.layer + m, env.R.at[self.layer, first(nf - 1)]
            wait_for(view, env.x_send.at[lane], env.device("fsdp", 1), True)
            wait_for(view, env.x_recv.at[lane], env.device("fsdp", 1))
        for m in self.swap:
            env.G[self.layer, env.y, env.z, pl.ds(m * nf, nf)] = env.R[self.layer, pl.ds(m * nf, nf)]
        pl.semaphore_wait(env.ready.at[self.layer, self.part], 4)
        self.left = 2
        for k in BOTH:
            self.gather_send(1, k, 0)
        env.exchanged.add((self.layer, self.part))
        env.begin_waiting()

    def gather_send(self, phase, k, step):
        half, ready = self.half_ring(phase, k), 0.0
        for d in BOTH:
            side = d if step + 1 == half else None
            view = self.block(phase, k, self.env.near(self.ring(phase, k), -SIGN[d] * step), side)
            self.copy(1, phase, k, d, step, view, view).start()
            ready = max(ready, self.send_time(phase, k, d, self.sizes[k] if side is None else self.sizes[k] // 2))
        self.env.clock.after(ready, functools.partial(self.gather_step, phase, k, step))

    def gather_step(self, phase, k, step):
        env = self.env
        last = step + 1 == self.half_ring(phase, k)
        self.take(1, phase, k, step, 1 if last else len(BOTH))
        if not last:
            self.gather_send(phase, k, step + 1)
        elif phase == 1:
            self.gather_send(0, k, 0)
        else:
            self.left -= 1
            here = (self.layer, slice(None), slice(None), pl.ds(self.starts[k], self.sizes[k]))
            pltpu.make_async_copy(env.G.at[here], env.out_ref.at[here], env.out_sem).start()


class Env:
    def __init__(self, dims):
        self.exchanged, self.reduced, self.half, self.waiting, self.clock = set(), set(), set(), [], Clock()
        self.sends = self.receives = 0
        self.ny, self.nz, self.nf = dims[1:4]
        self.last = dims[0] - 1
        self.f, self.y, self.z = lax.axis_index("fsdp"), lax.axis_index("replica"), lax.axis_index("dp")
        self.size = {"fsdp": self.nf, "replica": self.ny, "dp": self.nz}
        self.pos = {"fsdp": self.f, "replica": self.y, "dp": self.z}
        stride = {"fsdp": 1, "replica": self.nf, "dp": self.nf * self.ny}
        me = self.f + stride["replica"] * self.y + stride["dp"] * self.z
        self.row = me - self.f
        self.shift = {a: [wrap(self.pos[a] + k, n) for k in range(n)] for a, n in self.size.items()}
        self.ids = {a: [me + (p - self.pos[a]) * stride[a] for p in self.shift[a]] for a in self.size}

    def near(self, axis, k):
        return self.shift[axis][k % self.size[axis]]

    def device(self, axis, k):
        return self.ids[axis][k % self.size[axis]]

    def above(self, job):
        return (job.layer + 1, job.part) if job.layer + 1 < self.last else None

    def begin(self, job, phase, k):
        self.waiting.append((job, phase, k))
        self.begin_waiting()

    def begin_job(self, job):
        for k in BOTH:
            self.begin(job, 0, k)

    def begin_waiting(self):
        for item in list(self.waiting):
            job, phase, k = item
            if item in self.waiting and (not self.above(job) or self.above(job) in (self.exchanged if phase else self.half)):
                self.waiting.remove(item)
                job.start(phase, k)

    def settle(self, layer):
        self.clock.until(lambda: {(layer, part) for part in (GATE, UP, DOWN)} <= self.reduced)


GATE, UP, DOWN = range(3)
PART_SIZES, LAST_SIZES = (4, 4, 6), (6, 4, 6)


def step_kernel(dims, x_ref, dy_ref, wg_ref, wu_ref, wd_ref, gain_ref, y_ref, out_ref, gain_out,
                WB, WD, N, GA, UA, DH, O, DS, MS, H, DGU, G, S, R, gain_buf, gain_row,
                ag_send, ag_recv, rs_send, rs_recv, wx_send, wx_recv, wz_send, wz_recv, wy_send, wy_recv, w_sem, wd_sem,
                j_send, j_recv, x_send, x_recv, g_send, g_recv, out_sem, io_sem, ready, freed, credit):
    layers, ny, nz, nf, tok, depth, hid = dims
    nx, q = nf // 2, depth // nf // ny
    tile = min(256, depth)
    last = layers - 1

    env = Env(dims)
    f, y, z = env.f, env.y, env.z
    x, c = f // 2, f % 2
    env.G, env.S, env.R, env.out_ref = G, S, R, out_ref
    env.send_sem, env.recv_sem = j_send, j_recv
    env.x_send, env.x_recv, env.ready, env.freed, env.out_sem = x_send, x_recv, ready, freed, out_sem
    env.units = 3 * nf
    clock = env.clock
    env.jobs = jobs = {}
    for l in reversed(range(layers)):
        for part in (GATE, UP, DOWN):
            jobs[l, part] = Job(env, l, part)

    chips = [wrap(x + k, nx) for k in range(nx)]
    same, opposite_core = [2 * p + c for p in chips], [2 * p + (1 - c) for p in chips]
    fid = {id(v): env.row + v for v in same + opposite_core}

    def dev(off, opposite=False):
        return (opposite_core if opposite else same)[off % nx]

    partner = dev(0, True)
    axes = [("fsdp", f, nf), ("replica", y, ny), ("dp", z, nz)]

    barrier = pltpu.get_barrier_semaphore()
    for axis, pos, size in axes:
        for j in range(1, size):
            pl.semaphore_signal(barrier, device_id=env.device(axis, j), device_id_type=LOGICAL)

    x_copy = pltpu.make_async_copy(x_ref, H.at[0], io_sem.at[0])
    dy_copy = pltpu.make_async_copy(dy_ref, DH.at[last % 2, f], io_sem.at[1])
    x_copy.start()
    dy_copy.start()
    wd_copies = [pltpu.make_async_copy(wd_ref.at[l], WD.at[l], wd_sem.at[l]) for l in range(layers)]
    weights = (wg_ref, wu_ref)
    y_at = [env.near("replica", k) for k in range(ny)]
    parts = (first(nf // 2), pl.ds(nf // 2, nf // 2))
    direct = pl.ds(ny * q // 2, ny * q // 2)
    direct_lane = 2 * layers
    shared = {}

    def share(l, m, hops=0):
        size = q // 2 if (l, m) == BOTH else q
        return pl.ds(y_at[hops % ny] * size, size)

    odd = lax.rem(z, 2)
    z_partner = env.ids["dp"][0] + (1 - 2 * odd) * nf * ny

    def fetched(l, m, other=False):
        if l == 0:
            return share(l, m)
        return pl.ds(y_at[0] * q + (1 - odd if other else odd) * (q // 2), q // 2)

    def wz_copy(l, m, other=False):
        view = WB.at[l, m, :, fetched(l, m, other)]
        return pltpu.make_async_remote_copy(
            src_ref=view, dst_ref=view, send_sem=wz_send.at[2 * l + m], recv_sem=wz_recv.at[2 * l + m],
            device_id=z_partner, device_id_type=LOGICAL)

    def own_rows(l, m, rows, sem):
        src = weights[m].at[l, rows, pl.ds(pl.multiple_of(f * hid, hid), hid)]
        return pltpu.make_async_copy(src, WB.at[l, m, f, rows], w_sem.at[sem])

    own_copies = {(l, m): own_rows(l, m, fetched(l, m), 2 * l + m) for l in range(layers) for m in BOTH}
    own_copies[DIRECT] = own_rows(*BOTH, direct, 2 * layers)
    for copy in own_copies.values():
        copy.start()
    for copy in wd_copies:
        copy.start()
    pl.semaphore_wait(barrier, nf + ny + nz - 3)
    clock.busy(ENTRY)

    def wx_copy(l, m, peer, sender, rows, lane):
        return pltpu.make_async_remote_copy(
            src_ref=weights[m].at[l, rows, pl.ds(pl.multiple_of(peer * hid, hid), hid)], dst_ref=WB.at[l, m, sender, rows],
            send_sem=wx_send.at[lane], recv_sem=wx_recv.at[lane], device_id=env.row + peer, device_id_type=LOGICAL)

    def wx_sets(l):
        return [(l, m, fetched(l, m), 2 * l + m) for m in BOTH]

    def wx_post(key, l, m, rows, lane):
        repeat(1, nf, lambda j: wx_copy(l, m, wrap(f + j, nf), f, rows, lane).start())
        for d in BOTH:
            shared[key] = clock.send(d, nx * rows.size * hid * BF16_BYTES) + HBM_READ

    def wx_take(key, l, m, rows, lane):
        yield from clock.known(shared, key)
        own_copies[key].wait()
        wait_for(WB.at[l, m, first(nf - 1), rows], wx_recv.at[lane], env.device("fsdp", 1))

    def wx_start(l):
        for args in wx_sets(l):
            wx_post(args[:2], *args)

    def wy_copy(l, m, kind, d, arrived=False):
        hops = (kind == PASS) + arrived
        lane = 2 * l + m
        part = parts[BOTH[d - (kind == SECOND)]]
        view = WB.at[l, m, part, share(l, m, -SIGN[d] * hops)]
        return pltpu.make_async_remote_copy(
            src_ref=view, dst_ref=view, send_sem=wy_send.at[lane], recv_sem=wy_recv.at[2 * lane + (kind > FIRST)],
            device_id=env.device("replica", SIGN[d]), device_id_type=LOGICAL)

    def wy_send_one(l, m, kind, d):
        wy_copy(l, m, kind, d).start()
        shared[l, m, kind, d] = clock.send(("replica", d), nf // 2 * share(l, m).size * hid * BF16_BYTES)

    def wy_take(l, m, later):
        for kind in (SECOND, PASS) if later else (FIRST,):
            for d in BOTH:
                yield from clock.known(shared, (l, m, kind, d))
        rows = first(share(l, m).size * (1 + later))
        wait_for(WB.at[l, m, :, rows], wy_recv.at[2 * (2 * l + m) + later], env.device("replica", 1))

    def weights_task():
        for l in range(layers):
            for args in wx_sets(l):
                yield from wx_take(args[:2], *args)
                if l:
                    wz_copy(*args[:2]).start()
                    yield clock.send(("dp", 0), nf * q // 2 * hid * BF16_BYTES)
                    wz_copy(*args[:2], True).wait_recv()
                for kind in (FIRST, SECOND):
                    for d in BOTH:
                        wy_send_one(*args[:2], kind, d)
            for m in BOTH:
                yield from wy_take(l, m, 0)
                for d in BOTH:
                    wy_send_one(l, m, PASS, d)

    def weights_here(l):
        while l in claimed and l not in arrived:
            yield clock.now + STEP_COST
        if l in arrived:
            return
        claimed.add(l)
        if l == 0:
            yield from wx_take(*straight)
        for m in BOTH:
            yield from wy_take(l, m, 1)
        wd_copies[l].wait()
        arrived.add(l)

    claimed, arrived = set(), set()
    straight = DIRECT, *BOTH, direct, direct_lane

    class Gather:
        def __init__(self, lanes, buf, slot, base, size):
            self.lanes, self.buf, self.slot, self.ready = lanes, buf, slot, {}
            self.whole = pl.ds(base, size)
            self.halves = (pl.ds(base, size // 2), pl.ds(base + size // 2, size // 2))

        def copy(self, kind, d):
            hops = (kind in (PASS, RELAY)) + (kind == FAR) * nx // len(BOTH)
            block = dev(-SIGN[d] * hops)
            rows = self.whole if kind in (RELAY, OWN) else self.halves[d - (kind == SECOND)]
            target = partner if kind in (RELAY, FAR, OWN) else dev(SIGN[d])
            view = self.buf.at[self.slot, block, rows]
            return rows.size, pltpu.make_async_remote_copy(
                src_ref=view, dst_ref=view, send_sem=ag_send.at[self.lanes], recv_sem=ag_recv.at[self.lanes * (OWN + 1) + kind],
                device_id=fid[id(target)], device_id_type=LOGICAL)

        def send(self, *kinds):
            for kind in kinds:
                ready = 0.0
                for d in BOTH[:1] if kind == OWN else BOTH:
                    size, copy = self.copy(kind, d)
                    copy.start()
                    ready = max(ready, clock.send(CORES if kind in (RELAY, FAR, OWN) else d, size * depth * BF16_BYTES))
                self.ready[kind] = ready

        def blocks(self, count):
            return self.buf.at[self.slot, first(count), self.whole]

        def take(self, *kinds):
            for kind in kinds:
                yield from clock.known(self.ready, kind)
                wait_for(self.blocks(2 if kind == RELAY else 1), ag_recv.at[self.lanes * (OWN + 1) + kind], fid[id(partner)])

        def start(self):
            self.send(FIRST, OWN, SECOND)

        def mid(self):
            for kind, onward in ((FIRST, PASS), (SECOND, RELAY)):
                yield from self.take(kind)
                self.send(onward)

        def end(self):
            yield from self.take(PASS)
            self.send(FAR)

        def drain(self):
            wait_for(self.blocks(nf - 1), ag_send.at[self.lanes], fid[id(partner)], True)

    chunk = min(16, tok // 8)

    def rows_at(start, j):
        return pl.ds(pl.multiple_of(start + j * chunk, chunk), chunk)

    class Reduce:
        def __init__(self, lanes, base, size):
            self.lanes, self.base, self.size, self.arrive = lanes, base, size, {}
            self.rows, self.local = pl.ds(base, size), pl.ds(base // 2, size // 2)

        def d2d(self, i, xp, core):
            return pltpu.make_async_remote_copy(
                src_ref=O.at[xp, core, self.rows], dst_ref=DS.at[xp, self.rows], send_sem=rs_send.at[2 * self.lanes],
                recv_sem=rs_recv.at[(nx + 2) * self.lanes + i], device_id=fid[id(partner)], device_id_type=LOGICAL)

        def msg(self, k, d):
            half = self.size // 2
            lane = (nx + 2) * self.lanes + nx + (k > 0)
            off, side = (2, d) if k == 0 else (SIGN[d], d if k == 3 else 1 - d)
            size, slot, at = half, (0 if k == 0 else 2), 0
            if k in (1, 2):
                size, slot = half // 2, 1
                at = (k - 1) * size
            return size, pltpu.make_async_remote_copy(
                src_ref=O.at[chips[off % nx], c, pl.ds(self.base + side * half + at, size)],
                dst_ref=MS.at[d, slot, pl.ds(self.base // 2 + at, size)],
                send_sem=rs_send.at[2 * self.lanes + 1], recv_sem=rs_recv.at[lane], device_id=fid[id(dev(SIGN[d]))], device_id_type=LOGICAL)

        def post(self, k, d):
            size, copy = self.msg(k, d)
            copy.start()
            self.arrive[k, d] = clock.send(d, size * depth * 4)

        def take(self, later):
            yield max(self.arrive[k, d] for k in ((1, 2, 3) if later else (0,)) for d in BOTH)
            view = MS.at[:, pl.ds(later, 1 + later), self.local]
            wait_for(view, rs_recv.at[(nx + 2) * self.lanes + nx + later], fid[id(partner)])

        def combine(self, i, off):
            xp = chips[off % nx]
            yield self.arrive[i]
            self.d2d(i, xp, c).wait_recv()

            def add(j):
                rows = rows_at(self.base, j)
                O[xp, c, rows] += DS[xp, rows]
            loop(self.size // chunk, add)
            clock.busy(ADD)

        def near(self):
            for i, d in ((1, 0), (2, 1)):
                yield from self.combine(i, SIGN[d])
                self.post(1, d)

        def start(self):
            yield from self.combine(3, 2)
            for k in (0, 2):
                for d in BOTH:
                    self.post(k, d)
            yield from self.combine(0, 0)

        def mid(self):
            half = self.size // 2
            yield from self.take(0)
            for d in BOTH:
                def add(j):
                    rows = rows_at(self.base + d * half, j)
                    O[chips[SIGN[d] % nx], c, rows] += MS[d, 0, rows_at(self.base // 2, j)]
                loop(half // chunk, add)
                self.post(3, d)

        def end(self, body):
            half = self.size // 2
            yield from self.take(1)
            for side in BOTH:
                def step(j):
                    rows, local = rows_at(self.base + side * half, j), rows_at(self.base // 2, j)
                    body(rows, O[x, c, rows] + (MS[0, 2 - side, local] + MS[1, 1 + side, local]))
                loop(half // chunk, step)
            clock.busy(5 * ADD)
            wait_for(O.at[:, 0, self.rows], rs_send.at[2 * self.lanes], fid[id(partner)], True)
            wait_for(O.at[first(nx - 1), 0, self.rows], rs_send.at[2 * self.lanes + 1], fid[id(partner)], True)

        def pairs(self, gathers, body, cost, after_mid=None):
            def step(i):
                xp = wrap(x + i + i // 2 - 2 * (i // 3), nx)
                body(xp, self.rows)
                self.d2d(i, xp, 1 - c).start()

            def go(start, stop):
                repeat(start, stop, step)
                for i in range(start, stop):
                    clock.now += cost
                    self.arrive[i] = clock.send(CORES, self.size * depth * 4)
                clock.busy(0.0)

            go(0, 1)
            for gather in gathers:
                yield from gather.take(RELAY)
            go(1, 3)
            late = not all(gather.ready.get(FAR, self.arrive[2]) < self.arrive[2] for gather in gathers)
            if late:
                yield from self.near()
            for gather in gathers:
                yield from gather.take(FAR)
            go(3, nx)
            if not late:
                yield from self.near()

    def rms(hidden):
        return lax.rsqrt(jnp.mean(hidden * hidden, axis=-1, keepdims=True) + NORM_EPS)

    def down_grad(l):
        group = nf // 2
        zs = tile // (group * RS)

        def body(j, carry):
            lhs = GA[l, :, :, :, pl.ds(pl.multiple_of(j * tile, tile), tile)].reshape(-1, tile)
            for i in range(depth // tile):
                res = dot(lhs, DH[l % 2, :, :, pl.ds(i * tile, tile)].reshape(-1, tile), TN)
                for h in range(tile // LN):
                    col = i * (tile // LN) + h
                    for zi in range(zs):
                        rows = res[zi * group * RS:(zi + 1) * group * RS, h * LN:(h + 1) * LN]
                        G[l, col // 2, j * zs + zi, pl.ds(2 * nf + (col % 2) * group, group)] = rows.reshape(group, RS, LN)
            return carry
        lax.fori_loop(0, hid // tile, body, 0)

    def up_grad(l):
        fs = tile // (nz_rows * RS)

        def body(j, carry):
            lhs = N[l, :, :, pl.ds(pl.multiple_of(j * tile, tile), tile)].reshape(-1, tile)
            for m in BOTH:
                for i in range(hid // tile):
                    res = dot(lhs, DGU[m, :, :, :, pl.ds(i * tile, tile)].reshape(-1, tile), TN)
                    for h in range(tile // LN):
                        for fi in range(fs):
                            rows = res[fi * nz_rows * RS:(fi + 1) * nz_rows * RS, h * LN:(h + 1) * LN]
                            G[l, i * (tile // LN) + h, :, m * nf + j * fs + fi] = rows.reshape(nz_rows, RS, LN)
            return carry
        lax.fori_loop(0, depth // tile, body, 0)

    nz_rows = depth // nf // RS
    part = tok // 2
    fwd = [[Gather(g, N, l, g * part, part) for g in BOTH] for l in range(layers)]
    bwd = [Gather(2, DH, l % 2, 0, tok) for l in range(layers)]
    dy_task = bwd[last]

    def activations(l, xp, rows, cols):
        tokens = N[l, pl.ds(2 * xp, 2), rows].reshape(-1, depth)
        gate = dot(tokens, WB[l, 0, :, :, cols].reshape(depth, tile)).astype(BF16)
        up = dot(tokens, WB[l, 1, :, :, cols].reshape(depth, tile)).astype(BF16)
        return gate, up

    def flat(ref, *index):
        value = ref[index]
        return value.reshape(-1, value.shape[-1])

    def product(l, ref, lead, xp, rows):
        prod = flat(ref, *lead, xp, slice(None), rows)
        for j in range(depth // tile):
            cols = pl.ds(j * tile, tile)
            O[xp, :, rows, cols] = dot(prod, WD[l, :, cols]).reshape(2, rows.size, tile)

    def forward(l, xp, rows):
        shape = (2, rows.size, tile)
        for j in range(hid // tile):
            cols = pl.ds(j * tile, tile)
            gate, up = activations(l, xp, rows, cols)
            GA[l, xp, :, rows, cols] = gate.reshape(shape)
            UA[l, xp, :, rows, cols] = up.reshape(shape)
            DGU[0, xp, :, rows, cols] = (jax.nn.silu(gate.astype(F32)) * up.astype(F32)).astype(BF16).reshape(shape)
        product(l, DGU, (0,), xp, rows)

    def backward(l, xp, rows):
        cot = DH[l % 2, pl.ds(2 * xp, 2)].reshape(-1, depth)
        shape = (2, tok, tile)
        for j in range(hid // tile):
            cols = pl.ds(j * tile, tile)
            here = (l, xp, slice(None), slice(None), cols)
            gate, up = activations(l, xp, rows, cols) if l == last else (flat(GA, *here), flat(UA, *here))
            gate, up = gate.astype(F32), up.astype(F32)
            d_prod = dot(cot, WD[l, cols, :], NT).astype(BF16).astype(F32)
            sig = jax.nn.sigmoid(gate)
            GA[here] = (gate * sig * up).astype(BF16).reshape(shape)
            DGU[0, xp, :, :, cols] = (d_prod * up * sig * (1.0 + gate * (1.0 - sig))).astype(BF16).reshape(shape)
            DGU[1, xp, :, :, cols] = (d_prod * gate * sig).astype(BF16).reshape(shape)
        d_gate, d_up = flat(DGU, 0, xp), flat(DGU, 1, xp)
        block = depth // nf
        for j in range(depth // tile):
            sub = pl.ds(j * tile // block, tile // block)
            total = dot(d_gate, WB[l, 0, sub].reshape(tile, hid), NT) + dot(d_up, WB[l, 1, sub].reshape(tile, hid), NT)
            O[xp, :, :, pl.ds(j * tile, tile)] = total.reshape(shape)

    def normalize(l, rows, hidden):
        N[l, f, rows] = (hidden * rms(hidden) * gain_ref[l:l + 1]).astype(BF16)

    def half_task(g):
        for l in range(last):
            gather, reduce = fwd[l][g], Reduce(g, g * part, part)
            yield from gather.mid()
            if g and l == 0:
                wx_start(1)
                dy_task.start()
                clock.spawn(dy_task.mid())
                clock.spawn(dy_task.end())
            if g and l + 2 < layers:
                wx_start(l + 2)
            clock.spawn(gather.end())
            yield from gather.take(OWN)
            yield from weights_here(l)
            yield from reduce.pairs([gather], functools.partial(forward, l), FORWARD / len(BOTH))
            yield from reduce.start()
            yield from reduce.mid()

            def next_hidden(rows, total, l=l):
                hidden = (H[l, rows].astype(F32) + total).astype(BF16)
                H[l + 1, rows] = hidden
                normalize(l + 1, rows, hidden.astype(F32))
            yield from reduce.end(next_hidden)
            gather.drain()
            fwd[l + 1][g].start()
        yield from fwd[last][g].mid()
        yield from fwd[last][g].end()
        finished.add(g)

    finished = set()
    wx_start(0)
    x_copy.wait()
    for g in BOTH:
        def enter(j):
            rows = rows_at(g * part, j)
            normalize(0, rows, H[0, rows].astype(F32))
        loop(part // chunk, enter)
        clock.busy(ADD)
        fwd[0][g].start()
    wx_post(*straight)
    dy_copy.wait()
    clock.spawn(weights_task())
    for g in BOTH:
        clock.spawn(half_task(g))
    clock.until(lambda: FAR in fwd[last][0].ready)

    for l in reversed(range(layers)):
        reduce = Reduce(2, 0, tok)
        if l == last:
            gathers = fwd[l]
            clock.play(dy_task.take(RELAY, FAR, OWN))
            clock.play(weights_here(l))
        else:
            gathers = [bwd[l]]
            bwd[l].start()
            clock.spawn(bwd[l].mid())
            clock.spawn(bwd[l].end())
        for gather in gathers:
            clock.play(gather.take(OWN))
        clock.play(reduce.pairs(gathers, functools.partial(backward, l), FORWARD + BACKWARD if l == last else BACKWARD))
        clock.play(reduce.start())
        if l == 0:
            env.settle(last)
        down_grad(l)
        clock.busy(WEIGHT)
        env.begin_job(jobs[l, DOWN])
        up_grad(l)
        clock.busy(2 * WEIGHT)
        env.begin_job(jobs[l, GATE])
        env.begin_job(jobs[l, UP])
        clock.play(reduce.mid())
        bwd[l].drain()

        def next_cot(rows, total, l=l):
            d_normed = total.astype(BF16).astype(F32)
            hidden = H[l, rows].astype(F32)
            inv = rms(hidden)
            if l > 0:
                scaled = d_normed * gain_ref[l:l + 1]
                cot = DH[l % 2, f, rows].astype(F32)
                d_hidden = cot + inv * scaled - hidden * (inv * inv * inv) * jnp.mean(scaled * hidden, axis=-1, keepdims=True)
                DH[(l - 1) % 2, f, rows] = d_hidden.astype(BF16)
            gain_row[...] += jnp.sum(d_normed * hidden * inv, axis=0, keepdims=True)
        gain_row[...] = jnp.zeros((1, depth), F32)
        clock.play(reduce.end(next_cot))
        lanes = depth // LN
        for j in range(lanes):
            gain_buf[0, f, l * lanes + j:l * lanes + j + 1] = gain_row[:, j * LN:(j + 1) * LN]

    def gain_copy(stage, j):
        axis, pos, size = axes[stage]
        return pltpu.make_async_remote_copy(
            src_ref=gain_buf.at[stage, pos], dst_ref=gain_buf.at[stage, pos],
            send_sem=g_send.at[stage], recv_sem=g_recv.at[stage],
            device_id=env.device(axis, j), device_id_type=LOGICAL)

    def gain_send(stage):
        for j in range(1, axes[stage][2]):
            gain_copy(stage, j).start()
        clock.after(clock.now + 2 * EXCHANGE, functools.partial(gain_sum, stage))

    def gain_sum(stage):
        axis, pos, size = axes[stage]
        wait_for(gain_buf.at[stage, first(size - 1)], g_recv.at[stage], env.device(axis, 1))
        total = gain_buf[stage, 0]
        for i in range(1, size):
            total = total + gain_buf[stage, i]
        if stage == 2:
            gain_out[...] = total
        else:
            gain_buf[stage + 1, axes[stage + 1][1]] = total
            gain_send(stage + 1)

    gain_send(0)

    for target in (partner, dev(1), dev(-1)):
        pl.semaphore_signal(credit, device_id=fid[id(target)], device_id_type=LOGICAL)
    pl.semaphore_wait(credit, 3)
    reduce = Reduce(2, 0, tok)
    clock.play(reduce.pairs([], functools.partial(product, last, GA, (last,)), FORWARD))
    clock.play(reduce.start())
    clock.play(reduce.mid())

    def output(rows, total):
        H[0, rows] = (H[last, rows].astype(F32) + total).astype(BF16)
    clock.play(reduce.end(output))
    y_copy = pltpu.make_async_copy(H.at[0], y_ref, io_sem.at[2])
    y_copy.start()
    while clock.queue:
        clock.step()

    y_copy.wait()
    for gather in fwd[last]:
        gather.drain()
    for l, m, rows, lane in [straight[1:]] + [args for l in range(layers) for args in wx_sets(l)]:
        wait_for(WB.at[l, m, first(nf - 1), rows], wx_send.at[lane], env.device("fsdp", 1), True)
    for l in range(layers):
        for m in BOTH:
            if l:
                wz_copy(l, m).wait_send()
            wait_for(WB.at[l, m, :, first(3 * share(l, m).size)], wy_send.at[2 * l + m], env.device("replica", 1), True)
    for job in jobs.values():
        for phase in BOTH:
            job.wait_sends(1, phase)
    for stage, (axis, _, size) in enumerate(axes):
        wait_for(gain_buf.at[stage, first(size - 1)], g_send.at[stage], env.device(axis, 1), True)
    pltpu.make_async_copy(G, out_ref, out_sem).wait()


def fused_step(x, dy, wg, wu, wd, gain, dims):
    layers, ny, nz, nf, tok, depth, hid = dims
    nx = nf // 2
    vm, hbm = pl.BlockSpec(memory_space=pltpu.VMEM), pl.BlockSpec(memory_space=pl.ANY)
    dma = pltpu.SemaphoreType.DMA
    three, two, more = (dma((n,)) for n in (layers, 2 * layers, 2 * layers + 1))
    blocks = (layers, ny, nz, 3 * nf, RS, LN)
    lines = layers * depth // LN
    wide = max(nf, ny, nz)
    return pl.pallas_call(
        functools.partial(step_kernel, dims),
        out_shape=(jax.ShapeDtypeStruct((tok, depth), BF16), jax.ShapeDtypeStruct(blocks, F32), jax.ShapeDtypeStruct((lines, LN), F32)),
        in_specs=[hbm] * 5 + [vm],
        out_specs=(hbm, hbm, vm),
        scratch_shapes=[
            pltpu.VMEM((layers, 2, nf, depth // nf, hid), BF16),
            pltpu.VMEM((layers, hid, depth), BF16),
            pltpu.VMEM((layers, nf, tok, depth), BF16),
            pltpu.VMEM((layers, nx, 2, tok, hid), BF16),
            pltpu.VMEM((layers, nx, 2, tok, hid), BF16),
            pltpu.VMEM((2, nf, tok, depth), BF16),
            pltpu.VMEM((nx, 2, tok, depth), F32),
            pltpu.VMEM((nx, tok, depth), F32),
            pltpu.VMEM((2, 3, tok // 2, depth), F32),
            pltpu.VMEM((layers, tok, depth), BF16),
            pltpu.VMEM((2, nx, 2, tok, hid), BF16),
            pltpu.VMEM(blocks, F32),
            pltpu.VMEM(blocks[1:], F32),
            pltpu.VMEM((layers, 2 * nf, RS, LN), F32),
            pltpu.VMEM((3, wide, lines, LN), F32),
            pltpu.VMEM((1, depth), F32),
            three, dma((3 * (OWN + 1),)), two, dma((3 * (nx + 2),)),
            more, more, two, two, two, dma((4 * layers,)), more, three,
            dma((20 * layers,)), dma((10 * layers * (ny // 2 + nz // 2),)),
            two, two, three, three, dma, three,
            *[pltpu.SemaphoreType.REGULAR((layers, DOWN + 1))] * 2, pltpu.SemaphoreType.REGULAR,
        ],
        compiler_params=pltpu.CompilerParams(collective_id=0, has_side_effects=True, vmem_limit_bytes=67043328),
        name="fused_step",
    )(x, dy, wg, wu, wd, gain)


def unpack_kernel(blocks_ref, gate_ref, up_ref, down_ref, blocks, gate, up, down, in_sem, out_sem):
    layers, ny, nz, units = blocks.shape[:4]
    nf = units // 3
    pairs, tall = nz // 2, nf // 2 * RS
    count = layers * pairs

    def load(i):
        here = (i // pairs, slice(None), pl.ds(i % pairs * 2, 2))
        return pltpu.make_async_copy(blocks_ref.at[here], blocks.at[here], in_sem.at[i])

    def stores(i):
        for ref, buf, rows in ((gate_ref, gate, RS), (up_ref, up, RS), (down_ref, down, tall)):
            here = (i // pairs, pl.ds(pl.multiple_of(i % pairs * (2 * rows), 2 * rows), 2 * rows))
            yield pltpu.make_async_copy(buf.at[here], ref.at[here], out_sem)

    loop(count, lambda i: load(i).start())

    def move(i):
        load(i).wait()
        l = i // pairs
        for k in BOTH:
            z = i % pairs * 2 + k
            rows = pl.ds(pl.multiple_of(z * RS, RS), RS)
            for y in range(ny):
                for j in range(nf):
                    cols = pl.ds((j * ny + y) * LN, LN)
                    gate[l, rows, cols] = blocks[l, y, z, j]
                    up[l, rows, cols] = blocks[l, y, z, nf + j]
                for j in range(nf):
                    h, r = j // (nf // 2), j % (nf // 2)
                    down[l, pl.ds(pl.multiple_of(z * tall + r * RS, RS), RS), pl.ds((2 * y + h) * LN, LN)] = blocks[l, y, z, 2 * nf + j]
        for copy in stores(i):
            copy.start()
    loop(count, move)
    for buf, ref in ((gate, gate_ref), (up, up_ref), (down, down_ref)):
        pltpu.make_async_copy(buf, ref, out_sem).wait()


def unpack(out, dims):
    layers, ny, nz, nf = dims
    wide, tall = (layers, nz * RS, nf * ny * LN), (layers, nz * nf // 2 * RS, 2 * ny * LN)
    shapes = (wide, wide, tall)
    hbm = pl.BlockSpec(memory_space=pl.ANY)
    return pl.pallas_call(
        unpack_kernel, in_specs=[hbm], out_specs=[hbm] * len(shapes),
        out_shape=[jax.ShapeDtypeStruct(shape, F32) for shape in shapes],
        scratch_shapes=[pltpu.VMEM(out.shape, F32), *[pltpu.VMEM(shape, F32) for shape in shapes],
                        pltpu.SemaphoreType.DMA((layers * nz // 2,)), pltpu.SemaphoreType.DMA],
        compiler_params=pltpu.CompilerParams(vmem_limit_bytes=48 * 2**20),
        name="unpack")(out)


TOKEN_AXES = ("dp", "replica", "fsdp")


def solution(mesh):
    ny, nz, nf = mesh.shape["replica"], mesh.shape["dp"], mesh.shape["fsdp"]
    tok_spec, shard_spec, full_spec = P(TOKEN_AXES, None), P(None, "fsdp", None), P(None, None)

    def device_step(x, dy, wg, wu, wd, gain):
        layers, depth = gain.shape
        dims = (layers, ny, nz, nf)
        out, blocks, gain_sum = fused_step(x, dy, wg, wu, wd, gain, dims + (x.shape[0], depth, wd.shape[1]))
        dw_gate, dw_up, dw_down = unpack(blocks, dims)
        return out, dw_gate, dw_up, dw_down, gain_sum.reshape(gain.shape)

    return jax.shard_map(
        device_step, mesh=mesh, in_specs=(tok_spec, tok_spec, shard_spec, shard_spec, shard_spec, full_spec),
        out_specs=(tok_spec, shard_spec, shard_spec, shard_spec, full_spec), check_vma=False)
```

```python
import functools
import heapq
import jax
import jax.numpy as jnp
from jax import lax
from jax.sharding import PartitionSpec as P
from jax.experimental import pallas as pl
from jax.experimental.pallas import tpu as pltpu

F32 = jnp.float32
BF16 = jnp.bfloat16
LOGICAL = pl.DeviceIdType.LOGICAL
RS, LN = 16, 128
UNIT_BYTES = RS * LN * 4
NORM_EPS = 1e-6
NN = (((1,), (0,)), ((), ()))
NT = (((1,), (1,)), ((), ()))
TN = (((0,), (0,)), ((), ()))
LINK_RATE, CORE_RATE, HOP, CORE_HOP, STEP_COST, HBM_READ, ENTRY = 46.6e3, 500e3, 2.2, 0.9, 0.15, 1.1, 3.5
CORES = "cores"
BOTH, SIGN, BF16_BYTES = (0, 1), (1, -1), 2
FIRST, SECOND, PASS, RELAY, FAR, OWN = range(6)
DIRECT = "direct"
FORWARD, BACKWARD, WEIGHT, ADD, EXCHANGE = 0.7, 0.95, 0.9, 0.15, 5.0


def dot(a, b, dims=NN):
    return lax.dot_general(a, b, dims, preferred_element_type=F32)


def loop(count, work):
    repeat(0, count, work)


def repeat(start, stop, work):
    def step(i, carry):
        work(i)
        return carry
    lax.fori_loop(start, stop, step, 0)


def wait_for(view, sem, device, sent=False):
    copy = pltpu.make_async_remote_copy(
        src_ref=view, dst_ref=view, send_sem=sem, recv_sem=sem, device_id=device, device_id_type=LOGICAL)
    if sent:
        copy.wait_send()
    else:
        copy.wait_recv()


def first(count):
    return pl.ds(0, count)


def wrap(value, size):
    return lax.rem(value + 4 * size, size)


class Clock:
    def __init__(self):
        self.now, self.queue, self.count, self.links = 0.0, [], 0, {}

    def send(self, link, size):
        near = link == CORES
        start = max(self.now, self.links.get(link, 0.0))
        self.links[link] = start + size / (CORE_RATE if near else LINK_RATE)
        return self.links[link] + (CORE_HOP if near else HOP)

    def after(self, ready, work):
        self.count += 1
        heapq.heappush(self.queue, (ready, self.count, work))

    def step(self):
        ready, _, work = heapq.heappop(self.queue)
        self.now = max(self.now, ready) + STEP_COST
        work()

    def run(self, until):
        while self.queue and self.queue[0][0] <= until:
            self.step()

    def busy(self, spent):
        self.now += spent
        self.run(self.now)

    def idle(self, until):
        self.run(until)
        self.now = max(self.now, until)

    def play(self, task):
        for ready in task:
            self.idle(ready)

    def spawn(self, task):
        ready = next(task, None)
        if ready is not None:
            self.after(ready, functools.partial(self.spawn, task))

    def until(self, done):
        while not done():
            self.step()

    def known(self, times, key):
        while key not in times:
            yield self.now + STEP_COST
        yield times[key]


class Job:
    def __init__(self, env, layer, part):
        parts = LAST_SIZES if layer == env.last else PART_SIZES
        sizes, start = (parts[part], env.nf - parts[part]), part * env.nf
        before = sum(parts[:part])
        offsets = before, start - before
        self.split = sum(parts)
        swap = () if part == DOWN else (part,)
        self.env, self.layer, self.part, self.swap = env, layer, part, swap
        self.sizes, self.offsets, self.starts = sizes, offsets, (start, start + sizes[0])
        self.left, self.turned = len(BOTH), 0
        above = env.above(self)
        self.slots = dict(env.jobs[above].slots) if above else {}
        for gather in BOTH[1:] if above else BOTH:
            for phase in BOTH:
                for k in BOTH:
                    self.slots[gather, phase, k] = env.sends, env.receives
                    env.sends += 1
                    env.receives += self.half_ring(phase, k)

    def ring(self, phase, k):
        return ("replica", "dp")[phase ^ k]

    def half_ring(self, phase, k):
        return self.env.size[self.ring(phase, k)] // 2

    def block(self, phase, k, index, side=None):
        env, G, layer = self.env, self.env.G, self.layer
        start, size = self.starts[k], self.sizes[k]
        if side is not None:
            start, size = start + side * (size // 2), size // 2
        units = pl.ds(start, size)
        if phase == 0:
            return G.at[layer, index, :, units] if k == 0 else G.at[layer, :, index, units]
        return G.at[layer, env.y, index, units] if k == 0 else G.at[layer, index, env.z, units]

    def stage(self, phase, k, d, step, side=None):
        env = self.env
        ref, lead = (env.G, (0,)) if self.layer == env.last else (env.S, ())
        base = 0 if k == 0 else self.split
        offset, size = self.offsets[k], self.sizes[k]
        half_total = ((env.units - self.split) if k else self.split) // 2
        at = 2 * (step - 1) + d
        if step == 0:
            units = pl.ds(base + d * half_total + offset // 2, size // 2)
            at = env.nz - 2 if self.ring(phase, k) == "dp" else 2
        elif side is None:
            units = pl.ds(base + offset, size)
        else:
            units = pl.ds(base + offset + side * (size // 2), size // 2)
        every = slice(None)
        if phase == 0:
            place = (at, every) if k == 0 else (every, at)
        else:
            place = (env.ny - 1, at) if k == 0 else (at, env.nz - 1)
        return ref.at[(*lead, *place, units)]

    def many(self, phase, k, count):
        G, some, every = self.env.G, first(count), slice(None)
        units = pl.ds(self.starts[k], self.sizes[k])
        other = every if phase == 0 else 0
        place = (some, other) if phase == k else (other, some)
        return G.at[(self.layer, *place, units)]

    def copy(self, gather, phase, k, d, step, src, dst):
        env = self.env
        send, receive = self.slots[gather, phase, k]
        return pltpu.make_async_remote_copy(
            src_ref=src, dst_ref=dst, send_sem=env.send_sem.at[send], recv_sem=env.recv_sem.at[receive + step],
            device_id=env.device(self.ring(phase, k), SIGN[d]), device_id_type=LOGICAL)

    def take(self, gather, phase, k, step, blocks):
        receive = self.slots[gather, phase, k][1]
        wait_for(self.many(phase, k, blocks), self.env.recv_sem.at[receive + step], self.env.device(self.ring(phase, k), 1))

    def send_time(self, phase, k, d, units):
        env = self.env
        other = (env.nz if k == 0 else env.ny) if phase == 0 else 1
        return env.clock.send((self.ring(phase, k), d), units * other * UNIT_BYTES)

    def reduce_send(self, phase, k, step, early=False):
        size, ready = self.sizes[k], 0.0
        for d in BOTH:
            side = None if step > 1 else BOTH[d - 1] if early else d
            index = self.env.near(self.ring(phase, k), SIGN[d] * (self.half_ring(phase, k) - step))
            stage = self.stage(phase, k, d, step, None if step == 0 else side)
            self.copy(0, phase, k, d, step, self.block(phase, k, index, side), stage).start()
            ready = max(ready, self.send_time(phase, k, d, size if step > 1 else size // 2))
        if not early:
            self.env.clock.after(ready, functools.partial(self.reduce_step, phase, k, step))

    def reduce_start(self, phase, k):
        self.reduce_send(phase, k, 0)
        self.reduce_send(phase, k, 1, True)

    def start(self, phase, k):
        env = self.env
        if phase == 0 and k == 0 and env.above(self):
            pl.semaphore_wait(env.freed.at[env.above(self)], 4)
        self.reduce_start(phase, k)

    def reduce_step(self, phase, k, step):
        half = self.half_ring(phase, k)
        self.take(0, phase, k, step, len(BOTH) if step else 1)
        for d in BOTH:
            index = self.env.near(self.ring(phase, k), SIGN[d] * (half - 1 - step))
            self.block(phase, k, index, None if step else d)[...] += self.stage(phase, k, d, step)[...]
        if step + 1 < half:
            self.reduce_send(phase, k, step + 1)
        elif phase == 0:
            self.halfway()
            self.env.begin(self, 1, k)
        else:
            self.left -= 1
            if self.left == 0:
                self.reduced()

    def halfway(self):
        env, here = self.env, (self.layer, self.part)
        self.turned += 1
        if self.turned == len(BOTH):
            self.wait_sends(0, 0)
            if 0 < self.layer < env.last:
                self.tell(env.freed)
            env.half.add(here)
            env.begin_waiting()

    def tell(self, flags):
        for axis in ("replica", "dp"):
            for sign in SIGN:
                pl.semaphore_signal(flags.at[self.layer, self.part], device_id=self.env.device(axis, sign), device_id_type=LOGICAL)

    def wait_sends(self, gather, phase):
        for k in BOTH:
            ring = self.ring(phase, k)
            send = self.slots[gather, phase, k][0]
            wait_for(self.many(phase, k, self.env.size[ring] - 1), self.env.send_sem.at[send], self.env.device(ring, 1), True)

    def x_copy(self, m, peer, sender):
        env = self.env
        lane = 2 * self.layer + m
        return pltpu.make_async_remote_copy(
            src_ref=env.G.at[self.layer, env.y, env.z, m * env.nf + peer], dst_ref=env.R.at[self.layer, m * env.nf + sender],
            send_sem=env.x_send.at[lane], recv_sem=env.x_recv.at[lane],
            device_id=env.row + peer, device_id_type=LOGICAL)

    def reduced(self):
        env = self.env
        self.wait_sends(0, 1)
        self.tell(env.ready)
        for m in self.swap:
            repeat(1, env.nf, lambda j: self.x_copy(m, wrap(env.f + j, env.nf), env.f).start())
        env.reduced.add((self.layer, self.part))
        env.clock.after(env.clock.now + (EXCHANGE if self.swap else HOP), self.exchanged)

    def exchanged(self):
        env = self.env
        f, nf = env.f, env.nf
        for m in self.swap:
            env.R[self.layer, m * nf + f] = env.G[self.layer, env.y, env.z, m * nf + f]
        for m in self.swap:
            lane, view = 2 * self.layer + m, env.R.at[self.layer, first(nf - 1)]
            wait_for(view, env.x_send.at[lane], env.device("fsdp", 1), True)
            wait_for(view, env.x_recv.at[lane], env.device("fsdp", 1))
        for m in self.swap:
            env.G[self.layer, env.y, env.z, pl.ds(m * nf, nf)] = env.R[self.layer, pl.ds(m * nf, nf)]
        pl.semaphore_wait(env.ready.at[self.layer, self.part], 4)
        self.left = 2
        for k in BOTH:
            self.gather_send(1, k, 0)
        env.exchanged.add((self.layer, self.part))
        env.begin_waiting()

    def gather_send(self, phase, k, step):
        half, ready = self.half_ring(phase, k), 0.0
        for d in BOTH:
            side = d if step + 1 == half else None
            view = self.block(phase, k, self.env.near(self.ring(phase, k), -SIGN[d] * step), side)
            self.copy(1, phase, k, d, step, view, view).start()
            ready = max(ready, self.send_time(phase, k, d, self.sizes[k] if side is None else self.sizes[k] // 2))
        self.env.clock.after(ready, functools.partial(self.gather_step, phase, k, step))

    def gather_step(self, phase, k, step):
        env = self.env
        last = step + 1 == self.half_ring(phase, k)
        self.take(1, phase, k, step, 1 if last else len(BOTH))
        if not last:
            self.gather_send(phase, k, step + 1)
        elif phase == 1:
            self.gather_send(0, k, 0)
        else:
            self.left -= 1
            here = (self.layer, slice(None), slice(None), pl.ds(self.starts[k], self.sizes[k]))
            pltpu.make_async_copy(env.G.at[here], env.out_ref.at[here], env.out_sem).start()


class Env:
    def __init__(self, dims):
        self.exchanged, self.reduced, self.half, self.waiting, self.clock = set(), set(), set(), [], Clock()
        self.sends = self.receives = 0
        self.ny, self.nz, self.nf = dims[1:4]
        self.last = dims[0] - 1
        self.f, self.y, self.z = lax.axis_index("fsdp"), lax.axis_index("replica"), lax.axis_index("dp")
        self.size = {"fsdp": self.nf, "replica": self.ny, "dp": self.nz}
        self.pos = {"fsdp": self.f, "replica": self.y, "dp": self.z}
        stride = {"fsdp": 1, "replica": self.nf, "dp": self.nf * self.ny}
        me = self.f + stride["replica"] * self.y + stride["dp"] * self.z
        self.row = me - self.f
        self.shift = {a: [wrap(self.pos[a] + k, n) for k in range(n)] for a, n in self.size.items()}
        self.ids = {a: [me + (p - self.pos[a]) * stride[a] for p in self.shift[a]] for a in self.size}

    def near(self, axis, k):
        return self.shift[axis][k % self.size[axis]]

    def device(self, axis, k):
        return self.ids[axis][k % self.size[axis]]

    def above(self, job):
        return (job.layer + 1, job.part) if job.layer + 1 < self.last else None

    def begin(self, job, phase, k):
        self.waiting.append((job, phase, k))
        self.begin_waiting()

    def begin_job(self, job):
        for k in BOTH:
            self.begin(job, 0, k)

    def begin_waiting(self):
        for item in list(self.waiting):
            job, phase, k = item
            if item in self.waiting and (not self.above(job) or self.above(job) in (self.exchanged if phase else self.half)):
                self.waiting.remove(item)
                job.start(phase, k)

    def settle(self, layer):
        self.clock.until(lambda: {(layer, part) for part in (GATE, UP, DOWN)} <= self.reduced)


GATE, UP, DOWN = range(3)
PART_SIZES, LAST_SIZES = (4, 4, 6), (6, 4, 6)


def step_kernel(dims, x_ref, dy_ref, wg_ref, wu_ref, wd_ref, gain_ref, y_ref, out_ref, gain_out,
                WB, WD, N, GA, UA, DH, O, DS, MS, H, DGU, G, S, R, gain_buf, gain_row,
                ag_send, ag_recv, rs_send, rs_recv, wx_send, wx_recv, wz_send, wz_recv, wy_send, wy_recv, w_sem, wd_sem,
                j_send, j_recv, x_send, x_recv, g_send, g_recv, out_sem, io_sem, ready, freed, credit):
    layers, ny, nz, nf, tok, depth, hid = dims
    nx, q = nf // 2, depth // nf // ny
    tile = min(256, depth)
    last = layers - 1

    env = Env(dims)
    f, y, z = env.f, env.y, env.z
    x, c = f // 2, f % 2
    env.G, env.S, env.R, env.out_ref = G, S, R, out_ref
    env.send_sem, env.recv_sem = j_send, j_recv
    env.x_send, env.x_recv, env.ready, env.freed, env.out_sem = x_send, x_recv, ready, freed, out_sem
    env.units = 3 * nf
    clock = env.clock
    env.jobs = jobs = {}
    for l in reversed(range(layers)):
        for part in (GATE, UP, DOWN):
            jobs[l, part] = Job(env, l, part)

    chips = [wrap(x + k, nx) for k in range(nx)]
    same, opposite_core = [2 * p + c for p in chips], [2 * p + (1 - c) for p in chips]
    fid = {id(v): env.row + v for v in same + opposite_core}

    def dev(off, opposite=False):
        return (opposite_core if opposite else same)[off % nx]

    partner = dev(0, True)
    axes = [("fsdp", f, nf), ("replica", y, ny), ("dp", z, nz)]

    barrier = pltpu.get_barrier_semaphore()
    for axis, pos, size in axes:
        for j in range(1, size):
            pl.semaphore_signal(barrier, device_id=env.device(axis, j), device_id_type=LOGICAL)

    x_copy = pltpu.make_async_copy(x_ref, H.at[0], io_sem.at[0])
    dy_copy = pltpu.make_async_copy(dy_ref, DH.at[last % 2, f], io_sem.at[1])
    x_copy.start()
    dy_copy.start()
    wd_copies = [pltpu.make_async_copy(wd_ref.at[l], WD.at[l], wd_sem.at[l]) for l in range(layers)]
    weights = (wg_ref, wu_ref)
    y_at = [env.near("replica", k) for k in range(ny)]
    parts = (first(nf // 2), pl.ds(nf // 2, nf // 2))
    direct = pl.ds(ny * q // 2, ny * q // 2)
    direct_lane = 2 * layers
    shared = {}

    def share(l, m, hops=0):
        size = q // 2 if (l, m) == BOTH else q
        return pl.ds(y_at[hops % ny] * size, size)

    odd = lax.rem(z, 2)
    z_partner = env.ids["dp"][0] + (1 - 2 * odd) * nf * ny

    def fetched(l, m, other=False):
        if l == 0:
            return share(l, m)
        return pl.ds(y_at[0] * q + (1 - odd if other else odd) * (q // 2), q // 2)

    def wz_copy(l, m, other=False):
        view = WB.at[l, m, :, fetched(l, m, other)]
        return pltpu.make_async_remote_copy(
            src_ref=view, dst_ref=view, send_sem=wz_send.at[2 * l + m], recv_sem=wz_recv.at[2 * l + m],
            device_id=z_partner, device_id_type=LOGICAL)

    def own_rows(l, m, rows, sem):
        src = weights[m].at[l, rows, pl.ds(pl.multiple_of(f * hid, hid), hid)]
        return pltpu.make_async_copy(src, WB.at[l, m, f, rows], w_sem.at[sem])

    own_copies = {(l, m): own_rows(l, m, fetched(l, m), 2 * l + m) for l in range(layers) for m in BOTH}
    own_copies[DIRECT] = own_rows(*BOTH, direct, 2 * layers)
    for copy in own_copies.values():
        copy.start()
    for copy in wd_copies:
        copy.start()
    pl.semaphore_wait(barrier, nf + ny + nz - 3)
    clock.busy(ENTRY)

    def wx_copy(l, m, peer, sender, rows, lane):
        return pltpu.make_async_remote_copy(
            src_ref=weights[m].at[l, rows, pl.ds(pl.multiple_of(peer * hid, hid), hid)], dst_ref=WB.at[l, m, sender, rows],
            send_sem=wx_send.at[lane], recv_sem=wx_recv.at[lane], device_id=env.row + peer, device_id_type=LOGICAL)

    def wx_sets(l):
        return [(l, m, fetched(l, m), 2 * l + m) for m in BOTH]

    def wx_post(key, l, m, rows, lane):
        repeat(1, nf, lambda j: wx_copy(l, m, wrap(f + j, nf), f, rows, lane).start())
        for d in BOTH:
            shared[key] = clock.send(d, nx * rows.size * hid * BF16_BYTES) + HBM_READ

    def wx_take(key, l, m, rows, lane):
        yield from clock.known(shared, key)
        own_copies[key].wait()
        wait_for(WB.at[l, m, first(nf - 1), rows], wx_recv.at[lane], env.device("fsdp", 1))

    def wx_start(l):
        for args in wx_sets(l):
            wx_post(args[:2], *args)

    def wy_copy(l, m, kind, d, arrived=False):
        hops = (kind == PASS) + arrived
        lane = 2 * l + m
        part = parts[BOTH[d - (kind == SECOND)]]
        view = WB.at[l, m, part, share(l, m, -SIGN[d] * hops)]
        return pltpu.make_async_remote_copy(
            src_ref=view, dst_ref=view, send_sem=wy_send.at[lane], recv_sem=wy_recv.at[2 * lane + (kind > FIRST)],
            device_id=env.device("replica", SIGN[d]), device_id_type=LOGICAL)

    def wy_send_one(l, m, kind, d):
        wy_copy(l, m, kind, d).start()
        shared[l, m, kind, d] = clock.send(("replica", d), nf // 2 * share(l, m).size * hid * BF16_BYTES)

    def wy_take(l, m, later):
        for kind in (SECOND, PASS) if later else (FIRST,):
            for d in BOTH:
                yield from clock.known(shared, (l, m, kind, d))
        rows = first(share(l, m).size * (1 + later))
        wait_for(WB.at[l, m, :, rows], wy_recv.at[2 * (2 * l + m) + later], env.device("replica", 1))

    def weights_task():
        for l in range(layers):
            for args in wx_sets(l):
                yield from wx_take(args[:2], *args)
                if l:
                    wz_copy(*args[:2]).start()
                    yield clock.send(("dp", 0), nf * q // 2 * hid * BF16_BYTES)
                    wz_copy(*args[:2], True).wait_recv()
                for kind in (FIRST, SECOND):
                    for d in BOTH:
                        wy_send_one(*args[:2], kind, d)
            for m in BOTH:
                yield from wy_take(l, m, 0)
                for d in BOTH:
                    wy_send_one(l, m, PASS, d)

    def weights_here(l):
        while l in claimed and l not in arrived:
            yield clock.now + STEP_COST
        if l in arrived:
            return
        claimed.add(l)
        if l == 0:
            yield from wx_take(*straight)
        for m in BOTH:
            yield from wy_take(l, m, 1)
        wd_copies[l].wait()
        arrived.add(l)

    claimed, arrived = set(), set()
    straight = DIRECT, *BOTH, direct, direct_lane

    class Gather:
        def __init__(self, lanes, buf, slot, base, size):
            self.lanes, self.buf, self.slot, self.ready = lanes, buf, slot, {}
            self.whole = pl.ds(base, size)
            self.halves = (pl.ds(base, size // 2), pl.ds(base + size // 2, size // 2))

        def copy(self, kind, d):
            hops = (kind in (PASS, RELAY)) + (kind == FAR) * nx // len(BOTH)
            block = dev(-SIGN[d] * hops)
            rows = self.whole if kind in (RELAY, OWN) else self.halves[d - (kind == SECOND)]
            target = partner if kind in (RELAY, FAR, OWN) else dev(SIGN[d])
            view = self.buf.at[self.slot, block, rows]
            return rows.size, pltpu.make_async_remote_copy(
                src_ref=view, dst_ref=view, send_sem=ag_send.at[self.lanes], recv_sem=ag_recv.at[self.lanes * (OWN + 1) + kind],
                device_id=fid[id(target)], device_id_type=LOGICAL)

        def send(self, *kinds):
            for kind in kinds:
                ready = 0.0
                for d in BOTH[:1] if kind == OWN else BOTH:
                    size, copy = self.copy(kind, d)
                    copy.start()
                    ready = max(ready, clock.send(CORES if kind in (RELAY, FAR, OWN) else d, size * depth * BF16_BYTES))
                self.ready[kind] = ready

        def blocks(self, count):
            return self.buf.at[self.slot, first(count), self.whole]

        def take(self, *kinds):
            for kind in kinds:
                yield from clock.known(self.ready, kind)
                wait_for(self.blocks(2 if kind == RELAY else 1), ag_recv.at[self.lanes * (OWN + 1) + kind], fid[id(partner)])

        def start(self):
            self.send(FIRST, OWN, SECOND)

        def mid(self):
            for kind, onward in ((FIRST, PASS), (SECOND, RELAY)):
                yield from self.take(kind)
                self.send(onward)

        def end(self):
            yield from self.take(PASS)
            self.send(FAR)

        def drain(self):
            wait_for(self.blocks(nf - 1), ag_send.at[self.lanes], fid[id(partner)], True)

    chunk = min(16, tok // 8)

    def rows_at(start, j):
        return pl.ds(pl.multiple_of(start + j * chunk, chunk), chunk)

    class Reduce:
        def __init__(self, lanes, base, size):
            self.lanes, self.base, self.size, self.arrive = lanes, base, size, {}
            self.rows, self.local = pl.ds(base, size), pl.ds(base // 2, size // 2)

        def d2d(self, i, xp, core):
            return pltpu.make_async_remote_copy(
                src_ref=O.at[xp, core, self.rows], dst_ref=DS.at[xp, self.rows], send_sem=rs_send.at[2 * self.lanes],
                recv_sem=rs_recv.at[(nx + 2) * self.lanes + i], device_id=fid[id(partner)], device_id_type=LOGICAL)

        def msg(self, k, d):
            half = self.size // 2
            lane = (nx + 2) * self.lanes + nx + (k > 0)
            off, side = (2, d) if k == 0 else (SIGN[d], d if k == 3 else 1 - d)
            size, slot, at = half, (0 if k == 0 else 2), 0
            if k in (1, 2):
                size, slot = half // 2, 1
                at = (k - 1) * size
            return size, pltpu.make_async_remote_copy(
                src_ref=O.at[chips[off % nx], c, pl.ds(self.base + side * half + at, size)],
                dst_ref=MS.at[d, slot, pl.ds(self.base // 2 + at, size)],
                send_sem=rs_send.at[2 * self.lanes + 1], recv_sem=rs_recv.at[lane], device_id=fid[id(dev(SIGN[d]))], device_id_type=LOGICAL)

        def post(self, k, d):
            size, copy = self.msg(k, d)
            copy.start()
            self.arrive[k, d] = clock.send(d, size * depth * 4)

        def take(self, later):
            yield max(self.arrive[k, d] for k in ((1, 2, 3) if later else (0,)) for d in BOTH)
            view = MS.at[:, pl.ds(later, 1 + later), self.local]
            wait_for(view, rs_recv.at[(nx + 2) * self.lanes + nx + later], fid[id(partner)])

        def combine(self, i, off):
            xp = chips[off % nx]
            yield self.arrive[i]
            self.d2d(i, xp, c).wait_recv()

            def add(j):
                rows = rows_at(self.base, j)
                O[xp, c, rows] += DS[xp, rows]
            loop(self.size // chunk, add)
            clock.busy(ADD)

        def near(self):
            for i, d in ((1, 0), (2, 1)):
                yield from self.combine(i, SIGN[d])
                self.post(1, d)

        def start(self):
            yield from self.combine(3, 2)
            for k in (0, 2):
                for d in BOTH:
                    self.post(k, d)
            yield from self.combine(0, 0)

        def mid(self):
            half = self.size // 2
            yield from self.take(0)
            for d in BOTH:
                def add(j):
                    rows = rows_at(self.base + d * half, j)
                    O[chips[SIGN[d] % nx], c, rows] += MS[d, 0, rows_at(self.base // 2, j)]
                loop(half // chunk, add)
                self.post(3, d)

        def end(self, body):
            half = self.size // 2
            yield from self.take(1)
            for side in BOTH:
                def step(j):
                    rows, local = rows_at(self.base + side * half, j), rows_at(self.base // 2, j)
                    body(rows, O[x, c, rows] + (MS[0, 2 - side, local] + MS[1, 1 + side, local]))
                loop(half // chunk, step)
            clock.busy(5 * ADD)
            wait_for(O.at[:, 0, self.rows], rs_send.at[2 * self.lanes], fid[id(partner)], True)
            wait_for(O.at[first(nx - 1), 0, self.rows], rs_send.at[2 * self.lanes + 1], fid[id(partner)], True)

        def pairs(self, gathers, body, cost, after_mid=None):
            def step(i):
                xp = wrap(x + i + i // 2 - 2 * (i // 3), nx)
                body(xp, self.rows)
                self.d2d(i, xp, 1 - c).start()

            def go(start, stop):
                repeat(start, stop, step)
                for i in range(start, stop):
                    clock.now += cost
                    self.arrive[i] = clock.send(CORES, self.size * depth * 4)
                clock.busy(0.0)

            go(0, 1)
            for gather in gathers:
                yield from gather.take(RELAY)
            go(1, 3)
            late = not all(gather.ready.get(FAR, self.arrive[2]) < self.arrive[2] for gather in gathers)
            if late:
                yield from self.near()
            for gather in gathers:
                yield from gather.take(FAR)
            go(3, nx)
            if not late:
                yield from self.near()

    def rms(hidden):
        return lax.rsqrt(jnp.mean(hidden * hidden, axis=-1, keepdims=True) + NORM_EPS)

    def down_grad(l):
        group = nf // 2
        zs = tile // (group * RS)

        def body(j, carry):
            lhs = GA[l, :, :, :, pl.ds(pl.multiple_of(j * tile, tile), tile)].reshape(-1, tile)
            for i in range(depth // tile):
                res = dot(lhs, DH[l % 2, :, :, pl.ds(i * tile, tile)].reshape(-1, tile), TN)
                for h in range(tile // LN):
                    col = i * (tile // LN) + h
                    for zi in range(zs):
                        rows = res[zi * group * RS:(zi + 1) * group * RS, h * LN:(h + 1) * LN]
                        G[l, col // 2, j * zs + zi, pl.ds(2 * nf + (col % 2) * group, group)] = rows.reshape(group, RS, LN)
            return carry
        lax.fori_loop(0, hid // tile, body, 0)

    def up_grad(l):
        fs = tile // (nz_rows * RS)

        def body(j, carry):
            lhs = N[l, :, :, pl.ds(pl.multiple_of(j * tile, tile), tile)].reshape(-1, tile)
            for m in BOTH:
                for i in range(hid // tile):
                    res = dot(lhs, DGU[m, :, :, :, pl.ds(i * tile, tile)].reshape(-1, tile), TN)
                    for h in range(tile // LN):
                        for fi in range(fs):
                            rows = res[fi * nz_rows * RS:(fi + 1) * nz_rows * RS, h * LN:(h + 1) * LN]
                            G[l, i * (tile // LN) + h, :, m * nf + j * fs + fi] = rows.reshape(nz_rows, RS, LN)
            return carry
        lax.fori_loop(0, depth // tile, body, 0)

    nz_rows = depth // nf // RS
    part = tok // 2
    fwd = [[Gather(g, N, l, g * part, part) for g in BOTH] for l in range(layers)]
    bwd = [Gather(2, DH, l % 2, 0, tok) for l in range(layers)]
    dy_task = bwd[last]

    def activations(l, xp, rows, cols):
        tokens = N[l, pl.ds(2 * xp, 2), rows].reshape(-1, depth)
        gate = dot(tokens, WB[l, 0, :, :, cols].reshape(depth, tile)).astype(BF16)
        up = dot(tokens, WB[l, 1, :, :, cols].reshape(depth, tile)).astype(BF16)
        return gate, up

    def flat(ref, *index):
        value = ref[index]
        return value.reshape(-1, value.shape[-1])

    def product(l, ref, lead, xp, rows):
        prod = flat(ref, *lead, xp, slice(None), rows)
        for j in range(depth // tile):
            cols = pl.ds(j * tile, tile)
            O[xp, :, rows, cols] = dot(prod, WD[l, :, cols]).reshape(2, rows.size, tile)

    def forward(l, xp, rows):
        shape = (2, rows.size, tile)
        for j in range(hid // tile):
            cols = pl.ds(j * tile, tile)
            gate, up = activations(l, xp, rows, cols)
            GA[l, xp, :, rows, cols] = gate.reshape(shape)
            UA[l, xp, :, rows, cols] = up.reshape(shape)
            DGU[0, xp, :, rows, cols] = (jax.nn.silu(gate.astype(F32)) * up.astype(F32)).astype(BF16).reshape(shape)
        product(l, DGU, (0,), xp, rows)

    def backward(l, xp, rows):
        cot = DH[l % 2, pl.ds(2 * xp, 2)].reshape(-1, depth)
        shape = (2, tok, tile)
        for j in range(hid // tile):
            cols = pl.ds(j * tile, tile)
            here = (l, xp, slice(None), slice(None), cols)
            gate, up = activations(l, xp, rows, cols) if l == last else (flat(GA, *here), flat(UA, *here))
            gate, up = gate.astype(F32), up.astype(F32)
            d_prod = dot(cot, WD[l, cols, :], NT).astype(BF16).astype(F32)
            sig = jax.nn.sigmoid(gate)
            GA[here] = (gate * sig * up).astype(BF16).reshape(shape)
            DGU[0, xp, :, :, cols] = (d_prod * up * sig * (1.0 + gate * (1.0 - sig))).astype(BF16).reshape(shape)
            DGU[1, xp, :, :, cols] = (d_prod * gate * sig).astype(BF16).reshape(shape)
        d_gate, d_up = flat(DGU, 0, xp), flat(DGU, 1, xp)
        block = depth // nf
        for j in range(depth // tile):
            sub = pl.ds(j * tile // block, tile // block)
            total = dot(d_gate, WB[l, 0, sub].reshape(tile, hid), NT) + dot(d_up, WB[l, 1, sub].reshape(tile, hid), NT)
            O[xp, :, :, pl.ds(j * tile, tile)] = total.reshape(shape)

    def normalize(l, rows, hidden):
        N[l, f, rows] = (hidden * rms(hidden) * gain_ref[l:l + 1]).astype(BF16)

    def half_task(g):
        for l in range(last):
            gather, reduce = fwd[l][g], Reduce(g, g * part, part)
            yield from gather.mid()
            if g and l == 0:
                wx_start(1)
                dy_task.start()
                clock.spawn(dy_task.mid())
                clock.spawn(dy_task.end())
            if g and l + 2 < layers:
                wx_start(l + 2)
            clock.spawn(gather.end())
            yield from gather.take(OWN)
            yield from weights_here(l)
            yield from reduce.pairs([gather], functools.partial(forward, l), FORWARD / len(BOTH))
            yield from reduce.start()
            yield from reduce.mid()

            def next_hidden(rows, total, l=l):
                hidden = (H[l, rows].astype(F32) + total).astype(BF16)
                H[l + 1, rows] = hidden
                normalize(l + 1, rows, hidden.astype(F32))
            yield from reduce.end(next_hidden)
            gather.drain()
            fwd[l + 1][g].start()
        yield from fwd[last][g].mid()
        yield from fwd[last][g].end()
        finished.add(g)

    finished = set()
    wx_start(0)
    x_copy.wait()
    for g in BOTH:
        def enter(j):
            rows = rows_at(g * part, j)
            normalize(0, rows, H[0, rows].astype(F32))
        loop(part // chunk, enter)
        clock.busy(ADD)
        fwd[0][g].start()
    wx_post(*straight)
    dy_copy.wait()
    clock.spawn(weights_task())
    for g in BOTH:
        clock.spawn(half_task(g))
    clock.until(lambda: FAR in fwd[last][0].ready)

    for l in reversed(range(layers)):
        reduce = Reduce(2, 0, tok)
        if l == last:
            gathers = fwd[l]
            clock.play(dy_task.take(RELAY, FAR, OWN))
            clock.play(weights_here(l))
        else:
            gathers = [bwd[l]]
            bwd[l].start()
            clock.spawn(bwd[l].mid())
            clock.spawn(bwd[l].end())
        for gather in gathers:
            clock.play(gather.take(OWN))
        clock.play(reduce.pairs(gathers, functools.partial(backward, l), FORWARD + BACKWARD if l == last else BACKWARD))
        if l == 0:
            env.settle(last)
        down_grad(l)
        clock.busy(WEIGHT)
        env.begin_job(jobs[l, DOWN])
        clock.play(reduce.start())
        up_grad(l)
        clock.busy(2 * WEIGHT)
        env.begin_job(jobs[l, GATE])
        env.begin_job(jobs[l, UP])
        clock.play(reduce.mid())
        bwd[l].drain()

        def next_cot(rows, total, l=l):
            d_normed = total.astype(BF16).astype(F32)
            hidden = H[l, rows].astype(F32)
            inv = rms(hidden)
            if l > 0:
                scaled = d_normed * gain_ref[l:l + 1]
                cot = DH[l % 2, f, rows].astype(F32)
                d_hidden = cot + inv * scaled - hidden * (inv * inv * inv) * jnp.mean(scaled * hidden, axis=-1, keepdims=True)
                DH[(l - 1) % 2, f, rows] = d_hidden.astype(BF16)
            gain_row[...] += jnp.sum(d_normed * hidden * inv, axis=0, keepdims=True)
        gain_row[...] = jnp.zeros((1, depth), F32)
        clock.play(reduce.end(next_cot))
        lanes = depth // LN
        for j in range(lanes):
            gain_buf[0, f, l * lanes + j:l * lanes + j + 1] = gain_row[:, j * LN:(j + 1) * LN]

    def gain_copy(stage, j):
        axis, pos, size = axes[stage]
        return pltpu.make_async_remote_copy(
            src_ref=gain_buf.at[stage, pos], dst_ref=gain_buf.at[stage, pos],
            send_sem=g_send.at[stage], recv_sem=g_recv.at[stage],
            device_id=env.device(axis, j), device_id_type=LOGICAL)

    def gain_send(stage):
        for j in range(1, axes[stage][2]):
            gain_copy(stage, j).start()
        clock.after(clock.now + 2 * EXCHANGE, functools.partial(gain_sum, stage))

    def gain_sum(stage):
        axis, pos, size = axes[stage]
        wait_for(gain_buf.at[stage, first(size - 1)], g_recv.at[stage], env.device(axis, 1))
        total = gain_buf[stage, 0]
        for i in range(1, size):
            total = total + gain_buf[stage, i]
        if stage == 2:
            gain_out[...] = total
        else:
            gain_buf[stage + 1, axes[stage + 1][1]] = total
            gain_send(stage + 1)

    gain_send(0)

    for target in (partner, dev(1), dev(-1)):
        pl.semaphore_signal(credit, device_id=fid[id(target)], device_id_type=LOGICAL)
    pl.semaphore_wait(credit, 3)
    reduce = Reduce(2, 0, tok)
    clock.play(reduce.pairs([], functools.partial(product, last, GA, (last,)), FORWARD))
    clock.play(reduce.start())
    clock.play(reduce.mid())

    def output(rows, total):
        H[0, rows] = (H[last, rows].astype(F32) + total).astype(BF16)
    clock.play(reduce.end(output))
    y_copy = pltpu.make_async_copy(H.at[0], y_ref, io_sem.at[2])
    y_copy.start()
    while clock.queue:
        clock.step()

    y_copy.wait()
    for gather in fwd[last]:
        gather.drain()
    for l, m, rows, lane in [straight[1:]] + [args for l in range(layers) for args in wx_sets(l)]:
        wait_for(WB.at[l, m, first(nf - 1), rows], wx_send.at[lane], env.device("fsdp", 1), True)
    for l in range(layers):
        for m in BOTH:
            if l:
                wz_copy(l, m).wait_send()
            wait_for(WB.at[l, m, :, first(3 * share(l, m).size)], wy_send.at[2 * l + m], env.device("replica", 1), True)
    for job in jobs.values():
        for phase in BOTH:
            job.wait_sends(1, phase)
    for stage, (axis, _, size) in enumerate(axes):
        wait_for(gain_buf.at[stage, first(size - 1)], g_send.at[stage], env.device(axis, 1), True)
    pltpu.make_async_copy(G, out_ref, out_sem).wait()


def fused_step(x, dy, wg, wu, wd, gain, dims):
    layers, ny, nz, nf, tok, depth, hid = dims
    nx = nf // 2
    vm, hbm = pl.BlockSpec(memory_space=pltpu.VMEM), pl.BlockSpec(memory_space=pl.ANY)
    dma = pltpu.SemaphoreType.DMA
    three, two, more = (dma((n,)) for n in (layers, 2 * layers, 2 * layers + 1))
    blocks = (layers, ny, nz, 3 * nf, RS, LN)
    lines = layers * depth // LN
    wide = max(nf, ny, nz)
    return pl.pallas_call(
        functools.partial(step_kernel, dims),
        out_shape=(jax.ShapeDtypeStruct((tok, depth), BF16), jax.ShapeDtypeStruct(blocks, F32), jax.ShapeDtypeStruct((lines, LN), F32)),
        in_specs=[hbm] * 5 + [vm],
        out_specs=(hbm, hbm, vm),
        scratch_shapes=[
            pltpu.VMEM((layers, 2, nf, depth // nf, hid), BF16),
            pltpu.VMEM((layers, hid, depth), BF16),
            pltpu.VMEM((layers, nf, tok, depth), BF16),
            pltpu.VMEM((layers, nx, 2, tok, hid), BF16),
            pltpu.VMEM((layers, nx, 2, tok, hid), BF16),
            pltpu.VMEM((2, nf, tok, depth), BF16),
            pltpu.VMEM((nx, 2, tok, depth), F32),
            pltpu.VMEM((nx, tok, depth), F32),
            pltpu.VMEM((2, 3, tok // 2, depth), F32),
            pltpu.VMEM((layers, tok, depth), BF16),
            pltpu.VMEM((2, nx, 2, tok, hid), BF16),
            pltpu.VMEM(blocks, F32),
            pltpu.VMEM(blocks[1:], F32),
            pltpu.VMEM((layers, 2 * nf, RS, LN), F32),
            pltpu.VMEM((3, wide, lines, LN), F32),
            pltpu.VMEM((1, depth), F32),
            three, dma((3 * (OWN + 1),)), two, dma((3 * (nx + 2),)),
            more, more, two, two, two, dma((4 * layers,)), more, three,
            dma((20 * layers,)), dma((10 * layers * (ny // 2 + nz // 2),)),
            two, two, three, three, dma, three,
            *[pltpu.SemaphoreType.REGULAR((layers, DOWN + 1))] * 2, pltpu.SemaphoreType.REGULAR,
        ],
        compiler_params=pltpu.CompilerParams(collective_id=0, has_side_effects=True, vmem_limit_bytes=67043328),
        name="fused_step",
    )(x, dy, wg, wu, wd, gain)


def unpack_kernel(blocks_ref, gate_ref, up_ref, down_ref, blocks, gate, up, down, in_sem, out_sem):
    layers, ny, nz, units = blocks.shape[:4]
    nf = units // 3
    pairs, tall = nz // 2, nf // 2 * RS
    count = layers * pairs

    def load(i):
        here = (i // pairs, slice(None), pl.ds(i % pairs * 2, 2))
        return pltpu.make_async_copy(blocks_ref.at[here], blocks.at[here], in_sem.at[i])

    def stores(i):
        for ref, buf, rows in ((gate_ref, gate, RS), (up_ref, up, RS), (down_ref, down, tall)):
            here = (i // pairs, pl.ds(pl.multiple_of(i % pairs * (2 * rows), 2 * rows), 2 * rows))
            yield pltpu.make_async_copy(buf.at[here], ref.at[here], out_sem)

    loop(count, lambda i: load(i).start())

    def move(i):
        load(i).wait()
        l = i // pairs
        for k in BOTH:
            z = i % pairs * 2 + k
            rows = pl.ds(pl.multiple_of(z * RS, RS), RS)
            for y in range(ny):
                for j in range(nf):
                    cols = pl.ds((j * ny + y) * LN, LN)
                    gate[l, rows, cols] = blocks[l, y, z, j]
                    up[l, rows, cols] = blocks[l, y, z, nf + j]
                for j in range(nf):
                    h, r = j // (nf // 2), j % (nf // 2)
                    down[l, pl.ds(pl.multiple_of(z * tall + r * RS, RS), RS), pl.ds((2 * y + h) * LN, LN)] = blocks[l, y, z, 2 * nf + j]
        for copy in stores(i):
            copy.start()
    loop(count, move)
    for buf, ref in ((gate, gate_ref), (up, up_ref), (down, down_ref)):
        pltpu.make_async_copy(buf, ref, out_sem).wait()


def unpack(out, dims):
    layers, ny, nz, nf = dims
    wide, tall = (layers, nz * RS, nf * ny * LN), (layers, nz * nf // 2 * RS, 2 * ny * LN)
    shapes = (wide, wide, tall)
    hbm = pl.BlockSpec(memory_space=pl.ANY)
    return pl.pallas_call(
        unpack_kernel, in_specs=[hbm], out_specs=[hbm] * len(shapes),
        out_shape=[jax.ShapeDtypeStruct(shape, F32) for shape in shapes],
        scratch_shapes=[pltpu.VMEM(out.shape, F32), *[pltpu.VMEM(shape, F32) for shape in shapes],
                        pltpu.SemaphoreType.DMA((layers * nz // 2,)), pltpu.SemaphoreType.DMA],
        compiler_params=pltpu.CompilerParams(vmem_limit_bytes=48 * 2**20),
        name="unpack")(out)


TOKEN_AXES = ("dp", "replica", "fsdp")


def solution(mesh):
    ny, nz, nf = mesh.shape["replica"], mesh.shape["dp"], mesh.shape["fsdp"]
    tok_spec, shard_spec, full_spec = P(TOKEN_AXES, None), P(None, "fsdp", None), P(None, None)

    def device_step(x, dy, wg, wu, wd, gain):
        layers, depth = gain.shape
        dims = (layers, ny, nz, nf)
        out, blocks, gain_sum = fused_step(x, dy, wg, wu, wd, gain, dims + (x.shape[0], depth, wd.shape[1]))
        dw_gate, dw_up, dw_down = unpack(blocks, dims)
        return out, dw_gate, dw_up, dw_down, gain_sum.reshape(gain.shape)

    return jax.shard_map(
        device_step, mesh=mesh, in_specs=(tok_spec, tok_spec, shard_spec, shard_spec, shard_spec, full_spec),
        out_specs=(tok_spec, shard_spec, shard_spec, shard_spec, full_spec), check_vma=False)
```

```python
import functools
import heapq
import jax
import jax.numpy as jnp
from jax import lax
from jax.sharding import PartitionSpec as P
from jax.experimental import pallas as pl
from jax.experimental.pallas import tpu as pltpu

F32 = jnp.float32
BF16 = jnp.bfloat16
LOGICAL = pl.DeviceIdType.LOGICAL
RS, LN = 16, 128
UNIT_BYTES = RS * LN * 4
NORM_EPS = 1e-6
NN = (((1,), (0,)), ((), ()))
NT = (((1,), (1,)), ((), ()))
TN = (((0,), (0,)), ((), ()))
LINK_RATE, CORE_RATE, HOP, CORE_HOP, STEP_COST, HBM_READ, ENTRY = 46.6e3, 500e3, 2.2, 0.9, 0.15, 1.1, 3.5
CORES = "cores"
BOTH, SIGN, BF16_BYTES = (0, 1), (1, -1), 2
FIRST, SECOND, PASS, RELAY, FAR, OWN = range(6)
DIRECT = "direct"
FORWARD, BACKWARD, WEIGHT, ADD, EXCHANGE = 0.7, 0.95, 0.9, 0.15, 5.0


def dot(a, b, dims=NN):
    return lax.dot_general(a, b, dims, preferred_element_type=F32)


def loop(count, work):
    repeat(0, count, work)


def repeat(start, stop, work):
    def step(i, carry):
        work(i)
        return carry
    lax.fori_loop(start, stop, step, 0)


def wait_for(view, sem, device, sent=False):
    copy = pltpu.make_async_remote_copy(
        src_ref=view, dst_ref=view, send_sem=sem, recv_sem=sem, device_id=device, device_id_type=LOGICAL)
    if sent:
        copy.wait_send()
    else:
        copy.wait_recv()


def first(count):
    return pl.ds(0, count)


def wrap(value, size):
    return lax.rem(value + 4 * size, size)


class Clock:
    def __init__(self):
        self.now, self.queue, self.count, self.links = 0.0, [], 0, {}

    def send(self, link, size):
        near = link == CORES
        start = max(self.now, self.links.get(link, 0.0))
        self.links[link] = start + size / (CORE_RATE if near else LINK_RATE)
        return self.links[link] + (CORE_HOP if near else HOP)

    def after(self, ready, work):
        self.count += 1
        heapq.heappush(self.queue, (ready, self.count, work))

    def step(self):
        ready, _, work = heapq.heappop(self.queue)
        self.now = max(self.now, ready) + STEP_COST
        work()

    def run(self, until):
        while self.queue and self.queue[0][0] <= until:
            self.step()

    def busy(self, spent):
        self.now += spent
        self.run(self.now)

    def idle(self, until):
        self.run(until)
        self.now = max(self.now, until)

    def play(self, task):
        for ready in task:
            self.idle(ready)

    def spawn(self, task):
        ready = next(task, None)
        if ready is not None:
            self.after(ready, functools.partial(self.spawn, task))

    def until(self, done):
        while not done():
            self.step()

    def known(self, times, key):
        while key not in times:
            yield self.now + STEP_COST
        yield times[key]


class Job:
    def __init__(self, env, layer, part):
        parts = LAST_SIZES if layer == env.last else PART_SIZES
        sizes, start = (parts[part], env.nf - parts[part]), part * env.nf
        before = sum(parts[:part])
        offsets = before, start - before
        self.split = sum(parts)
        swap = () if part == DOWN else (part,)
        self.env, self.layer, self.part, self.swap = env, layer, part, swap
        self.sizes, self.offsets, self.starts = sizes, offsets, (start, start + sizes[0])
        self.left, self.turned, self.gathered = len(BOTH), 0, False
        above = env.above(self)
        self.before = env.jobs[env.last, part] if above else None
        if above:
            self.slots = {key: (self.before if key[0] else env.jobs[above]).slots[key] for key in self.before.slots}
            return
        self.slots = {}
        for gather in BOTH:
            for phase in BOTH:
                for k in BOTH:
                    self.slots[gather, phase, k] = env.sends, env.receives
                    env.sends += 1
                    env.receives += self.half_ring(phase, k)

    def ring(self, phase, k):
        return ("replica", "dp")[phase ^ k]

    def half_ring(self, phase, k):
        return self.env.size[self.ring(phase, k)] // 2

    def block(self, phase, k, index, side=None):
        env, G, layer = self.env, self.env.G, self.layer
        start, size = self.starts[k], self.sizes[k]
        if side is not None:
            start, size = start + side * (size // 2), size // 2
        units = pl.ds(start, size)
        if phase == 0:
            return G.at[layer, index, :, units] if k == 0 else G.at[layer, :, index, units]
        return G.at[layer, env.y, index, units] if k == 0 else G.at[layer, index, env.z, units]

    def stage(self, phase, k, d, step, side=None):
        env = self.env
        ref, lead = (env.G, (0,)) if self.layer == env.last else (env.S, ())
        base = 0 if k == 0 else self.split
        offset, size = self.offsets[k], self.sizes[k]
        half_total = ((env.units - self.split) if k else self.split) // 2
        at = 2 * (step - 1) + d
        if step == 0:
            units = pl.ds(base + d * half_total + offset // 2, size // 2)
            at = env.nz - 2 if self.ring(phase, k) == "dp" else 2
        elif side is None:
            units = pl.ds(base + offset, size)
        else:
            units = pl.ds(base + offset + side * (size // 2), size // 2)
        every = slice(None)
        if phase == 0:
            place = (at, every) if k == 0 else (every, at)
        else:
            place = (env.ny - 1, at) if k == 0 else (at, env.nz - 1)
        return ref.at[(*lead, *place, units)]

    def many(self, phase, k, count):
        G, some, every = self.env.G, first(count), slice(None)
        units = pl.ds(self.starts[k], self.sizes[k])
        other = every if phase == 0 else 0
        place = (some, other) if phase == k else (other, some)
        return G.at[(self.layer, *place, units)]

    def copy(self, gather, phase, k, d, step, src, dst):
        env = self.env
        send, receive = self.slots[gather, phase, k]
        return pltpu.make_async_remote_copy(
            src_ref=src, dst_ref=dst, send_sem=env.send_sem.at[send], recv_sem=env.recv_sem.at[receive + step],
            device_id=env.device(self.ring(phase, k), SIGN[d]), device_id_type=LOGICAL)

    def take(self, gather, phase, k, step, blocks):
        receive = self.slots[gather, phase, k][1]
        wait_for(self.many(phase, k, blocks), self.env.recv_sem.at[receive + step], self.env.device(self.ring(phase, k), 1))

    def send_time(self, phase, k, d, units):
        env = self.env
        other = (env.nz if k == 0 else env.ny) if phase == 0 else 1
        return env.clock.send((self.ring(phase, k), d), units * other * UNIT_BYTES)

    def reduce_send(self, phase, k, step, early=False):
        size, ready = self.sizes[k], 0.0
        for d in BOTH:
            side = None if step > 1 else BOTH[d - 1] if early else d
            index = self.env.near(self.ring(phase, k), SIGN[d] * (self.half_ring(phase, k) - step))
            stage = self.stage(phase, k, d, step, None if step == 0 else side)
            self.copy(0, phase, k, d, step, self.block(phase, k, index, side), stage).start()
            ready = max(ready, self.send_time(phase, k, d, size if step > 1 else size // 2))
        if not early:
            self.env.clock.after(ready, functools.partial(self.reduce_step, phase, k, step))

    def reduce_start(self, phase, k):
        self.reduce_send(phase, k, 0)
        self.reduce_send(phase, k, 1, True)

    def start(self, phase, k):
        env = self.env
        if phase == 0 and k == 0 and env.above(self):
            pl.semaphore_wait(env.freed.at[env.above(self)], 4)
        self.reduce_start(phase, k)

    def reduce_step(self, phase, k, step):
        half = self.half_ring(phase, k)
        self.take(0, phase, k, step, len(BOTH) if step else 1)
        for d in BOTH:
            index = self.env.near(self.ring(phase, k), SIGN[d] * (half - 1 - step))
            self.block(phase, k, index, None if step else d)[...] += self.stage(phase, k, d, step)[...]
        if step + 1 < half:
            self.reduce_send(phase, k, step + 1)
        elif phase == 0:
            self.halfway()
            self.env.begin(self, 1, k)
        else:
            self.left -= 1
            if self.left == 0:
                self.reduced()

    def halfway(self):
        env, here = self.env, (self.layer, self.part)
        self.turned += 1
        if self.turned == len(BOTH):
            self.wait_sends(0, 0)
            if 0 < self.layer < env.last:
                self.tell(env.freed)
            env.half.add(here)
            env.begin_waiting()

    def tell(self, flags):
        for axis in ("replica", "dp"):
            for sign in SIGN:
                pl.semaphore_signal(flags.at[self.layer, self.part], device_id=self.env.device(axis, sign), device_id_type=LOGICAL)

    def wait_sends(self, gather, phase):
        for k in BOTH:
            ring = self.ring(phase, k)
            send = self.slots[gather, phase, k][0]
            wait_for(self.many(phase, k, self.env.size[ring] - 1), self.env.send_sem.at[send], self.env.device(ring, 1), True)

    def x_copy(self, m, peer, sender):
        env = self.env
        lane = 2 * self.layer + m
        return pltpu.make_async_remote_copy(
            src_ref=env.G.at[self.layer, env.y, env.z, m * env.nf + peer], dst_ref=env.R.at[self.layer, m * env.nf + sender],
            send_sem=env.x_send.at[lane], recv_sem=env.x_recv.at[lane],
            device_id=env.row + peer, device_id_type=LOGICAL)

    def reduced(self):
        env = self.env
        self.wait_sends(0, 1)
        if self.before:
            env.clock.until(lambda: self.before.gathered)
            for phase in BOTH:
                self.before.wait_sends(1, phase)
        self.tell(env.ready)
        for m in self.swap:
            repeat(1, env.nf, lambda j: self.x_copy(m, wrap(env.f + j, env.nf), env.f).start())
        env.reduced.add((self.layer, self.part))
        env.clock.after(env.clock.now + (EXCHANGE if self.swap else HOP), self.exchanged)

    def exchanged(self):
        env = self.env
        f, nf = env.f, env.nf
        for m in self.swap:
            env.R[self.layer, m * nf + f] = env.G[self.layer, env.y, env.z, m * nf + f]
        for m in self.swap:
            lane, view = 2 * self.layer + m, env.R.at[self.layer, first(nf - 1)]
            wait_for(view, env.x_send.at[lane], env.device("fsdp", 1), True)
            wait_for(view, env.x_recv.at[lane], env.device("fsdp", 1))
        for m in self.swap:
            env.G[self.layer, env.y, env.z, pl.ds(m * nf, nf)] = env.R[self.layer, pl.ds(m * nf, nf)]
        pl.semaphore_wait(env.ready.at[self.layer, self.part], 4)
        self.left = 2
        for k in BOTH:
            self.gather_send(1, k, 0)
        env.exchanged.add((self.layer, self.part))
        env.begin_waiting()

    def gather_send(self, phase, k, step):
        half, ready = self.half_ring(phase, k), 0.0
        for d in BOTH:
            side = d if step + 1 == half else None
            view = self.block(phase, k, self.env.near(self.ring(phase, k), -SIGN[d] * step), side)
            self.copy(1, phase, k, d, step, view, view).start()
            ready = max(ready, self.send_time(phase, k, d, self.sizes[k] if side is None else self.sizes[k] // 2))
        self.env.clock.after(ready, functools.partial(self.gather_step, phase, k, step))

    def gather_step(self, phase, k, step):
        env = self.env
        last = step + 1 == self.half_ring(phase, k)
        self.take(1, phase, k, step, 1 if last else len(BOTH))
        if not last:
            self.gather_send(phase, k, step + 1)
        elif phase == 1:
            self.gather_send(0, k, 0)
        else:
            self.left -= 1
            self.gathered = self.left == 0
            here = (self.layer, slice(None), slice(None), pl.ds(self.starts[k], self.sizes[k]))
            pltpu.make_async_copy(env.G.at[here], env.out_ref.at[here], env.out_sem).start()


class Env:
    def __init__(self, dims):
        self.exchanged, self.reduced, self.half, self.waiting, self.clock = set(), set(), set(), [], Clock()
        self.sends = self.receives = 0
        self.ny, self.nz, self.nf = dims[1:4]
        self.last = dims[0] - 1
        self.f, self.y, self.z = lax.axis_index("fsdp"), lax.axis_index("replica"), lax.axis_index("dp")
        self.size = {"fsdp": self.nf, "replica": self.ny, "dp": self.nz}
        self.pos = {"fsdp": self.f, "replica": self.y, "dp": self.z}
        stride = {"fsdp": 1, "replica": self.nf, "dp": self.nf * self.ny}
        me = self.f + stride["replica"] * self.y + stride["dp"] * self.z
        self.row = me - self.f
        self.shift = {a: [wrap(self.pos[a] + k, n) for k in range(n)] for a, n in self.size.items()}
        self.ids = {a: [me + (p - self.pos[a]) * stride[a] for p in self.shift[a]] for a in self.size}

    def near(self, axis, k):
        return self.shift[axis][k % self.size[axis]]

    def device(self, axis, k):
        return self.ids[axis][k % self.size[axis]]

    def above(self, job):
        return (job.layer + 1, job.part) if job.layer + 1 < self.last else None

    def begin(self, job, phase, k):
        self.waiting.append((job, phase, k))
        self.begin_waiting()

    def begin_job(self, job):
        for k in BOTH:
            self.begin(job, 0, k)

    def begin_waiting(self):
        for item in list(self.waiting):
            job, phase, k = item
            if item in self.waiting and (not self.above(job) or self.above(job) in (self.exchanged if phase else self.half)):
                self.waiting.remove(item)
                job.start(phase, k)

    def settle(self, layer):
        self.clock.until(lambda: {(layer, part) for part in (GATE, UP, DOWN)} <= self.reduced)


GATE, UP, DOWN = range(3)
PART_SIZES, LAST_SIZES = (4, 4, 6), (6, 4, 6)


def step_kernel(dims, x_ref, dy_ref, wg_ref, wu_ref, wd_ref, gain_ref, y_ref, out_ref, gain_out,
                WB, WD, N, GA, UA, DH, O, DS, MS, H, DGU, G, S, R, gain_buf, gain_row,
                ag_send, ag_recv, rs_send, rs_recv, wx_send, wx_recv, wz_send, wz_recv, wy_send, wy_recv, w_sem, wd_sem,
                j_send, j_recv, x_send, x_recv, g_send, g_recv, out_sem, io_sem, ready, freed, credit):
    layers, ny, nz, nf, tok, depth, hid = dims
    nx, q = nf // 2, depth // nf // ny
    tile = min(256, depth)
    last = layers - 1

    env = Env(dims)
    f, y, z = env.f, env.y, env.z
    x, c = f // 2, f % 2
    env.G, env.S, env.R, env.out_ref = G, S, R, out_ref
    env.send_sem, env.recv_sem = j_send, j_recv
    env.x_send, env.x_recv, env.ready, env.freed, env.out_sem = x_send, x_recv, ready, freed, out_sem
    env.units = 3 * nf
    clock = env.clock
    env.jobs = jobs = {}
    for l in reversed(range(layers)):
        for part in (GATE, UP, DOWN):
            jobs[l, part] = Job(env, l, part)

    chips = [wrap(x + k, nx) for k in range(nx)]
    same, opposite_core = [2 * p + c for p in chips], [2 * p + (1 - c) for p in chips]
    fid = {id(v): env.row + v for v in same + opposite_core}

    def dev(off, opposite=False):
        return (opposite_core if opposite else same)[off % nx]

    partner = dev(0, True)
    axes = [("fsdp", f, nf), ("replica", y, ny), ("dp", z, nz)]

    barrier = pltpu.get_barrier_semaphore()
    for axis, pos, size in axes:
        for j in range(1, size):
            pl.semaphore_signal(barrier, device_id=env.device(axis, j), device_id_type=LOGICAL)

    x_copy = pltpu.make_async_copy(x_ref, H.at[0], io_sem.at[0])
    dy_copy = pltpu.make_async_copy(dy_ref, DH.at[last % 2, f], io_sem.at[1])
    x_copy.start()
    dy_copy.start()
    wd_copies = [pltpu.make_async_copy(wd_ref.at[l], WD.at[l], wd_sem.at[l]) for l in range(layers)]
    weights = (wg_ref, wu_ref)
    y_at = [env.near("replica", k) for k in range(ny)]
    parts = (first(nf // 2), pl.ds(nf // 2, nf // 2))
    direct = pl.ds(ny * q // 2, ny * q // 2)
    direct_lane = 2 * layers
    shared = {}

    def share(l, m, hops=0):
        size = q // 2 if (l, m) == BOTH else q
        return pl.ds(y_at[hops % ny] * size, size)

    odd = lax.rem(z, 2)
    z_partner = env.ids["dp"][0] + (1 - 2 * odd) * nf * ny

    def fetched(l, m, other=False):
        if l == 0:
            return share(l, m)
        return pl.ds(y_at[0] * q + (1 - odd if other else odd) * (q // 2), q // 2)

    def wz_copy(l, m, other=False):
        view = WB.at[l, m, :, fetched(l, m, other)]
        return pltpu.make_async_remote_copy(
            src_ref=view, dst_ref=view, send_sem=wz_send.at[2 * l + m], recv_sem=wz_recv.at[2 * l + m],
            device_id=z_partner, device_id_type=LOGICAL)

    def own_rows(l, m, rows, sem):
        src = weights[m].at[l, rows, pl.ds(pl.multiple_of(f * hid, hid), hid)]
        return pltpu.make_async_copy(src, WB.at[l, m, f, rows], w_sem.at[sem])

    own_copies = {(l, m): own_rows(l, m, fetched(l, m), 2 * l + m) for l in range(layers) for m in BOTH}
    own_copies[DIRECT] = own_rows(*BOTH, direct, 2 * layers)
    for copy in own_copies.values():
        copy.start()
    for copy in wd_copies:
        copy.start()
    pl.semaphore_wait(barrier, nf + ny + nz - 3)
    clock.busy(ENTRY)

    def wx_copy(l, m, peer, sender, rows, lane):
        return pltpu.make_async_remote_copy(
            src_ref=weights[m].at[l, rows, pl.ds(pl.multiple_of(peer * hid, hid), hid)], dst_ref=WB.at[l, m, sender, rows],
            send_sem=wx_send.at[lane], recv_sem=wx_recv.at[lane], device_id=env.row + peer, device_id_type=LOGICAL)

    def wx_sets(l):
        return [(l, m, fetched(l, m), 2 * l + m) for m in BOTH]

    def wx_post(key, l, m, rows, lane):
        repeat(1, nf, lambda j: wx_copy(l, m, wrap(f + j, nf), f, rows, lane).start())
        for d in BOTH:
            shared[key] = clock.send(d, nx * rows.size * hid * BF16_BYTES) + HBM_READ

    def wx_take(key, l, m, rows, lane):
        yield from clock.known(shared, key)
        own_copies[key].wait()
        wait_for(WB.at[l, m, first(nf - 1), rows], wx_recv.at[lane], env.device("fsdp", 1))

    def wx_start(l):
        for args in wx_sets(l):
            wx_post(args[:2], *args)

    def wy_copy(l, m, kind, d, arrived=False):
        hops = (kind == PASS) + arrived
        lane = 2 * l + m
        part = parts[BOTH[d - (kind == SECOND)]]
        view = WB.at[l, m, part, share(l, m, -SIGN[d] * hops)]
        return pltpu.make_async_remote_copy(
            src_ref=view, dst_ref=view, send_sem=wy_send.at[lane], recv_sem=wy_recv.at[2 * lane + (kind > FIRST)],
            device_id=env.device("replica", SIGN[d]), device_id_type=LOGICAL)

    def wy_send_one(l, m, kind, d):
        wy_copy(l, m, kind, d).start()
        shared[l, m, kind, d] = clock.send(("replica", d), nf // 2 * share(l, m).size * hid * BF16_BYTES)

    def wy_take(l, m, later):
        for kind in (SECOND, PASS) if later else (FIRST,):
            for d in BOTH:
                yield from clock.known(shared, (l, m, kind, d))
        rows = first(share(l, m).size * (1 + later))
        wait_for(WB.at[l, m, :, rows], wy_recv.at[2 * (2 * l + m) + later], env.device("replica", 1))

    def weights_task():
        for l in range(layers):
            for args in wx_sets(l):
                yield from wx_take(args[:2], *args)
                if l:
                    wz_copy(*args[:2]).start()
                    yield clock.send(("dp", 0), nf * q // 2 * hid * BF16_BYTES)
                    wz_copy(*args[:2], True).wait_recv()
                for kind in (FIRST, SECOND):
                    for d in BOTH:
                        wy_send_one(*args[:2], kind, d)
            for m in BOTH:
                yield from wy_take(l, m, 0)
                for d in BOTH:
                    wy_send_one(l, m, PASS, d)

    def weights_here(l):
        while l in claimed and l not in arrived:
            yield clock.now + STEP_COST
        if l in arrived:
            return
        claimed.add(l)
        if l == 0:
            yield from wx_take(*straight)
        for m in BOTH:
            yield from wy_take(l, m, 1)
        wd_copies[l].wait()
        arrived.add(l)

    claimed, arrived = set(), set()
    straight = DIRECT, *BOTH, direct, direct_lane

    class Gather:
        def __init__(self, lanes, buf, slot, base, size):
            self.lanes, self.buf, self.slot, self.ready = lanes, buf, slot, {}
            self.whole = pl.ds(base, size)
            self.halves = (pl.ds(base, size // 2), pl.ds(base + size // 2, size // 2))

        def copy(self, kind, d):
            hops = (kind in (PASS, RELAY)) + (kind == FAR) * nx // len(BOTH)
            block = dev(-SIGN[d] * hops)
            rows = self.whole if kind in (RELAY, OWN) else self.halves[d - (kind == SECOND)]
            target = partner if kind in (RELAY, FAR, OWN) else dev(SIGN[d])
            view = self.buf.at[self.slot, block, rows]
            return rows.size, pltpu.make_async_remote_copy(
                src_ref=view, dst_ref=view, send_sem=ag_send.at[self.lanes], recv_sem=ag_recv.at[self.lanes * (OWN + 1) + kind],
                device_id=fid[id(target)], device_id_type=LOGICAL)

        def send(self, *kinds):
            for kind in kinds:
                ready = 0.0
                for d in BOTH[:1] if kind == OWN else BOTH:
                    size, copy = self.copy(kind, d)
                    copy.start()
                    ready = max(ready, clock.send(CORES if kind in (RELAY, FAR, OWN) else d, size * depth * BF16_BYTES))
                self.ready[kind] = ready

        def blocks(self, count):
            return self.buf.at[self.slot, first(count), self.whole]

        def take(self, *kinds):
            for kind in kinds:
                yield from clock.known(self.ready, kind)
                wait_for(self.blocks(2 if kind == RELAY else 1), ag_recv.at[self.lanes * (OWN + 1) + kind], fid[id(partner)])

        def start(self):
            self.send(FIRST, OWN, SECOND)

        def mid(self):
            for kind, onward in ((FIRST, PASS), (SECOND, RELAY)):
                yield from self.take(kind)
                self.send(onward)

        def end(self):
            yield from self.take(PASS)
            self.send(FAR)

        def drain(self):
            wait_for(self.blocks(nf - 1), ag_send.at[self.lanes], fid[id(partner)], True)

    chunk = min(16, tok // 8)

    def rows_at(start, j):
        return pl.ds(pl.multiple_of(start + j * chunk, chunk), chunk)

    class Reduce:
        def __init__(self, lanes, base, size):
            self.lanes, self.base, self.size, self.arrive = lanes, base, size, {}
            self.rows, self.local = pl.ds(base, size), pl.ds(base // 2, size // 2)

        def d2d(self, i, xp, core):
            return pltpu.make_async_remote_copy(
                src_ref=O.at[xp, core, self.rows], dst_ref=DS.at[xp, self.rows], send_sem=rs_send.at[2 * self.lanes],
                recv_sem=rs_recv.at[(nx + 2) * self.lanes + i], device_id=fid[id(partner)], device_id_type=LOGICAL)

        def msg(self, k, d):
            half = self.size // 2
            lane = (nx + 2) * self.lanes + nx + (k > 0)
            off, side = (2, d) if k == 0 else (SIGN[d], d if k == 3 else 1 - d)
            size, slot, at = half, (0 if k == 0 else 2), 0
            if k in (1, 2):
                size, slot = half // 2, 1
                at = (k - 1) * size
            return size, pltpu.make_async_remote_copy(
                src_ref=O.at[chips[off % nx], c, pl.ds(self.base + side * half + at, size)],
                dst_ref=MS.at[d, slot, pl.ds(self.base // 2 + at, size)],
                send_sem=rs_send.at[2 * self.lanes + 1], recv_sem=rs_recv.at[lane], device_id=fid[id(dev(SIGN[d]))], device_id_type=LOGICAL)

        def post(self, k, d):
            size, copy = self.msg(k, d)
            copy.start()
            self.arrive[k, d] = clock.send(d, size * depth * 4)

        def take(self, later):
            yield max(self.arrive[k, d] for k in ((1, 2, 3) if later else (0,)) for d in BOTH)
            view = MS.at[:, pl.ds(later, 1 + later), self.local]
            wait_for(view, rs_recv.at[(nx + 2) * self.lanes + nx + later], fid[id(partner)])

        def combine(self, i, off):
            xp = chips[off % nx]
            yield self.arrive[i]
            self.d2d(i, xp, c).wait_recv()

            def add(j):
                rows = rows_at(self.base, j)
                O[xp, c, rows] += DS[xp, rows]
            loop(self.size // chunk, add)
            clock.busy(ADD)

        def near(self):
            for i, d in ((1, 0), (2, 1)):
                yield from self.combine(i, SIGN[d])
                self.post(1, d)

        def start(self):
            yield from self.combine(3, 2)
            for k in (0, 2):
                for d in BOTH:
                    self.post(k, d)
            yield from self.combine(0, 0)

        def mid(self):
            half = self.size // 2
            yield from self.take(0)
            for d in BOTH:
                def add(j):
                    rows = rows_at(self.base + d * half, j)
                    O[chips[SIGN[d] % nx], c, rows] += MS[d, 0, rows_at(self.base // 2, j)]
                loop(half // chunk, add)
                self.post(3, d)

        def end(self, body):
            half = self.size // 2
            yield from self.take(1)
            for side in BOTH:
                def step(j):
                    rows, local = rows_at(self.base + side * half, j), rows_at(self.base // 2, j)
                    body(rows, O[x, c, rows] + (MS[0, 2 - side, local] + MS[1, 1 + side, local]))
                loop(half // chunk, step)
            clock.busy(5 * ADD)
            wait_for(O.at[:, 0, self.rows], rs_send.at[2 * self.lanes], fid[id(partner)], True)
            wait_for(O.at[first(nx - 1), 0, self.rows], rs_send.at[2 * self.lanes + 1], fid[id(partner)], True)

        def pairs(self, gathers, body, cost, after_mid=None):
            def step(i):
                xp = wrap(x + i + i // 2 - 2 * (i // 3), nx)
                body(xp, self.rows)
                self.d2d(i, xp, 1 - c).start()

            def go(start, stop):
                repeat(start, stop, step)
                for i in range(start, stop):
                    clock.now += cost
                    self.arrive[i] = clock.send(CORES, self.size * depth * 4)
                clock.busy(0.0)

            go(0, 1)
            for gather in gathers:
                yield from gather.take(RELAY)
            go(1, 3)
            late = not all(gather.ready.get(FAR, self.arrive[2]) < self.arrive[2] for gather in gathers)
            if late:
                yield from self.near()
            for gather in gathers:
                yield from gather.take(FAR)
            go(3, nx)
            if not late:
                yield from self.near()

    def rms(hidden):
        return lax.rsqrt(jnp.mean(hidden * hidden, axis=-1, keepdims=True) + NORM_EPS)

    def down_grad(l):
        group = nf // 2
        zs = tile // (group * RS)

        def body(j, carry):
            lhs = GA[l, :, :, :, pl.ds(pl.multiple_of(j * tile, tile), tile)].reshape(-1, tile)
            for i in range(depth // tile):
                res = dot(lhs, DH[l % 2, :, :, pl.ds(i * tile, tile)].reshape(-1, tile), TN)
                for h in range(tile // LN):
                    col = i * (tile // LN) + h
                    for zi in range(zs):
                        rows = res[zi * group * RS:(zi + 1) * group * RS, h * LN:(h + 1) * LN]
                        G[l, col // 2, j * zs + zi, pl.ds(2 * nf + (col % 2) * group, group)] = rows.reshape(group, RS, LN)
            return carry
        lax.fori_loop(0, hid // tile, body, 0)

    def up_grad(l):
        fs = tile // (nz_rows * RS)

        def body(j, carry):
            lhs = N[l, :, :, pl.ds(pl.multiple_of(j * tile, tile), tile)].reshape(-1, tile)
            for m in BOTH:
                for i in range(hid // tile):
                    res = dot(lhs, DGU[m, :, :, :, pl.ds(i * tile, tile)].reshape(-1, tile), TN)
                    for h in range(tile // LN):
                        for fi in range(fs):
                            rows = res[fi * nz_rows * RS:(fi + 1) * nz_rows * RS, h * LN:(h + 1) * LN]
                            G[l, i * (tile // LN) + h, :, m * nf + j * fs + fi] = rows.reshape(nz_rows, RS, LN)
            return carry
        lax.fori_loop(0, depth // tile, body, 0)

    nz_rows = depth // nf // RS
    part = tok // 2
    fwd = [[Gather(g, N, l, g * part, part) for g in BOTH] for l in range(layers)]
    bwd = [Gather(2, DH, l % 2, 0, tok) for l in range(layers)]
    dy_task = bwd[last]

    def activations(l, xp, rows, cols):
        tokens = N[l, pl.ds(2 * xp, 2), rows].reshape(-1, depth)
        gate = dot(tokens, WB[l, 0, :, :, cols].reshape(depth, tile)).astype(BF16)
        up = dot(tokens, WB[l, 1, :, :, cols].reshape(depth, tile)).astype(BF16)
        return gate, up

    def flat(ref, *index):
        value = ref[index]
        return value.reshape(-1, value.shape[-1])

    def product(l, ref, lead, xp, rows):
        prod = flat(ref, *lead, xp, slice(None), rows)
        for j in range(depth // tile):
            cols = pl.ds(j * tile, tile)
            O[xp, :, rows, cols] = dot(prod, WD[l, :, cols]).reshape(2, rows.size, tile)

    def forward(l, xp, rows):
        shape = (2, rows.size, tile)
        for j in range(hid // tile):
            cols = pl.ds(j * tile, tile)
            gate, up = activations(l, xp, rows, cols)
            GA[l, xp, :, rows, cols] = gate.reshape(shape)
            UA[l, xp, :, rows, cols] = up.reshape(shape)
            DGU[0, xp, :, rows, cols] = (jax.nn.silu(gate.astype(F32)) * up.astype(F32)).astype(BF16).reshape(shape)
        product(l, DGU, (0,), xp, rows)

    def backward(l, xp, rows):
        cot = DH[l % 2, pl.ds(2 * xp, 2)].reshape(-1, depth)
        shape = (2, tok, tile)
        for j in range(hid // tile):
            cols = pl.ds(j * tile, tile)
            here = (l, xp, slice(None), slice(None), cols)
            gate, up = activations(l, xp, rows, cols) if l == last else (flat(GA, *here), flat(UA, *here))
            gate, up = gate.astype(F32), up.astype(F32)
            d_prod = dot(cot, WD[l, cols, :], NT).astype(BF16).astype(F32)
            sig = jax.nn.sigmoid(gate)
            GA[here] = (gate * sig * up).astype(BF16).reshape(shape)
            DGU[0, xp, :, :, cols] = (d_prod * up * sig * (1.0 + gate * (1.0 - sig))).astype(BF16).reshape(shape)
            DGU[1, xp, :, :, cols] = (d_prod * gate * sig).astype(BF16).reshape(shape)
        d_gate, d_up = flat(DGU, 0, xp), flat(DGU, 1, xp)
        block = depth // nf
        for j in range(depth // tile):
            sub = pl.ds(j * tile // block, tile // block)
            total = dot(d_gate, WB[l, 0, sub].reshape(tile, hid), NT) + dot(d_up, WB[l, 1, sub].reshape(tile, hid), NT)
            O[xp, :, :, pl.ds(j * tile, tile)] = total.reshape(shape)

    def normalize(l, rows, hidden):
        N[l, f, rows] = (hidden * rms(hidden) * gain_ref[l:l + 1]).astype(BF16)

    def half_task(g):
        for l in range(last):
            gather, reduce = fwd[l][g], Reduce(g, g * part, part)
            yield from gather.mid()
            if g and l == 0:
                wx_start(1)
                dy_task.start()
                clock.spawn(dy_task.mid())
                clock.spawn(dy_task.end())
            if g and l + 2 < layers:
                wx_start(l + 2)
            clock.spawn(gather.end())
            yield from gather.take(OWN)
            yield from weights_here(l)
            yield from reduce.pairs([gather], functools.partial(forward, l), FORWARD / len(BOTH))
            yield from reduce.start()
            yield from reduce.mid()

            def next_hidden(rows, total, l=l):
                hidden = (H[l, rows].astype(F32) + total).astype(BF16)
                H[l + 1, rows] = hidden
                normalize(l + 1, rows, hidden.astype(F32))
            yield from reduce.end(next_hidden)
            gather.drain()
            fwd[l + 1][g].start()
        yield from fwd[last][g].mid()
        yield from fwd[last][g].end()
        finished.add(g)

    finished = set()
    wx_start(0)
    x_copy.wait()
    for g in BOTH:
        def enter(j):
            rows = rows_at(g * part, j)
            normalize(0, rows, H[0, rows].astype(F32))
        loop(part // chunk, enter)
        clock.busy(ADD)
        fwd[0][g].start()
    wx_post(*straight)
    dy_copy.wait()
    clock.spawn(weights_task())
    for g in BOTH:
        clock.spawn(half_task(g))
    clock.until(lambda: FAR in fwd[last][0].ready)

    for l in reversed(range(layers)):
        reduce = Reduce(2, 0, tok)
        if l == last:
            gathers = fwd[l]
            clock.play(dy_task.take(RELAY, FAR, OWN))
            clock.play(weights_here(l))
        else:
            gathers = [bwd[l]]
            bwd[l].start()
            clock.spawn(bwd[l].mid())
            clock.spawn(bwd[l].end())
        for gather in gathers:
            clock.play(gather.take(OWN))
        clock.play(reduce.pairs(gathers, functools.partial(backward, l), FORWARD + BACKWARD if l == last else BACKWARD))
        if l == 0:
            env.settle(last)
        down_grad(l)
        clock.busy(WEIGHT)
        env.begin_job(jobs[l, DOWN])
        clock.play(reduce.start())
        up_grad(l)
        clock.busy(2 * WEIGHT)
        env.begin_job(jobs[l, GATE])
        env.begin_job(jobs[l, UP])
        clock.play(reduce.mid())
        bwd[l].drain()

        def next_cot(rows, total, l=l):
            d_normed = total.astype(BF16).astype(F32)
            hidden = H[l, rows].astype(F32)
            inv = rms(hidden)
            if l > 0:
                scaled = d_normed * gain_ref[l:l + 1]
                cot = DH[l % 2, f, rows].astype(F32)
                d_hidden = cot + inv * scaled - hidden * (inv * inv * inv) * jnp.mean(scaled * hidden, axis=-1, keepdims=True)
                DH[(l - 1) % 2, f, rows] = d_hidden.astype(BF16)
            gain_row[...] += jnp.sum(d_normed * hidden * inv, axis=0, keepdims=True)
        gain_row[...] = jnp.zeros((1, depth), F32)
        clock.play(reduce.end(next_cot))
        lanes = depth // LN
        for j in range(lanes):
            gain_buf[0, f, l * lanes + j:l * lanes + j + 1] = gain_row[:, j * LN:(j + 1) * LN]

    def gain_copy(stage, j):
        axis, pos, size = axes[stage]
        return pltpu.make_async_remote_copy(
            src_ref=gain_buf.at[stage, pos], dst_ref=gain_buf.at[stage, pos],
            send_sem=g_send.at[stage], recv_sem=g_recv.at[stage],
            device_id=env.device(axis, j), device_id_type=LOGICAL)

    def gain_send(stage):
        for j in range(1, axes[stage][2]):
            gain_copy(stage, j).start()
        clock.after(clock.now + 2 * EXCHANGE, functools.partial(gain_sum, stage))

    def gain_sum(stage):
        axis, pos, size = axes[stage]
        wait_for(gain_buf.at[stage, first(size - 1)], g_recv.at[stage], env.device(axis, 1))
        total = gain_buf[stage, 0]
        for i in range(1, size):
            total = total + gain_buf[stage, i]
        if stage == 2:
            gain_out[...] = total
        else:
            gain_buf[stage + 1, axes[stage + 1][1]] = total
            gain_send(stage + 1)

    gain_send(0)

    for target in (partner, dev(1), dev(-1)):
        pl.semaphore_signal(credit, device_id=fid[id(target)], device_id_type=LOGICAL)
    pl.semaphore_wait(credit, 3)
    reduce = Reduce(2, 0, tok)
    clock.play(reduce.pairs([], functools.partial(product, last, GA, (last,)), FORWARD))
    clock.play(reduce.start())
    clock.play(reduce.mid())

    def output(rows, total):
        H[0, rows] = (H[last, rows].astype(F32) + total).astype(BF16)
    clock.play(reduce.end(output))
    y_copy = pltpu.make_async_copy(H.at[0], y_ref, io_sem.at[2])
    y_copy.start()
    while clock.queue:
        clock.step()

    y_copy.wait()
    for gather in fwd[last]:
        gather.drain()
    for l, m, rows, lane in [straight[1:]] + [args for l in range(layers) for args in wx_sets(l)]:
        wait_for(WB.at[l, m, first(nf - 1), rows], wx_send.at[lane], env.device("fsdp", 1), True)
    for l in range(layers):
        for m in BOTH:
            if l:
                wz_copy(l, m).wait_send()
            wait_for(WB.at[l, m, :, first(3 * share(l, m).size)], wy_send.at[2 * l + m], env.device("replica", 1), True)
    for (l, _), job in jobs.items():
        for phase in BOTH if l < last else ():
            job.wait_sends(1, phase)
    for stage, (axis, _, size) in enumerate(axes):
        wait_for(gain_buf.at[stage, first(size - 1)], g_send.at[stage], env.device(axis, 1), True)
    pltpu.make_async_copy(G, out_ref, out_sem).wait()


def fused_step(x, dy, wg, wu, wd, gain, dims):
    layers, ny, nz, nf, tok, depth, hid = dims
    nx = nf // 2
    vm, hbm = pl.BlockSpec(memory_space=pltpu.VMEM), pl.BlockSpec(memory_space=pl.ANY)
    dma = pltpu.SemaphoreType.DMA
    three, two, more = (dma((n,)) for n in (layers, 2 * layers, 2 * layers + 1))
    blocks = (layers, ny, nz, 3 * nf, RS, LN)
    lines = layers * depth // LN
    wide = max(nf, ny, nz)
    return pl.pallas_call(
        functools.partial(step_kernel, dims),
        out_shape=(jax.ShapeDtypeStruct((tok, depth), BF16), jax.ShapeDtypeStruct(blocks, F32), jax.ShapeDtypeStruct((lines, LN), F32)),
        in_specs=[hbm] * 5 + [vm],
        out_specs=(hbm, hbm, vm),
        scratch_shapes=[
            pltpu.VMEM((layers, 2, nf, depth // nf, hid), BF16),
            pltpu.VMEM((layers, hid, depth), BF16),
            pltpu.VMEM((layers, nf, tok, depth), BF16),
            pltpu.VMEM((layers, nx, 2, tok, hid), BF16),
            pltpu.VMEM((layers, nx, 2, tok, hid), BF16),
            pltpu.VMEM((2, nf, tok, depth), BF16),
            pltpu.VMEM((nx, 2, tok, depth), F32),
            pltpu.VMEM((nx, tok, depth), F32),
            pltpu.VMEM((2, 3, tok // 2, depth), F32),
            pltpu.VMEM((layers, tok, depth), BF16),
            pltpu.VMEM((2, nx, 2, tok, hid), BF16),
            pltpu.VMEM(blocks, F32),
            pltpu.VMEM(blocks[1:], F32),
            pltpu.VMEM((layers, 2 * nf, RS, LN), F32),
            pltpu.VMEM((3, wide, lines, LN), F32),
            pltpu.VMEM((1, depth), F32),
            three, dma((3 * (OWN + 1),)), two, dma((3 * (nx + 2),)),
            more, more, two, two, two, dma((4 * layers,)), more, three,
            dma((16 * layers,)), dma((8 * layers * (ny // 2 + nz // 2),)),
            two, two, three, three, dma, three,
            *[pltpu.SemaphoreType.REGULAR((layers, DOWN + 1))] * 2, pltpu.SemaphoreType.REGULAR,
        ],
        compiler_params=pltpu.CompilerParams(collective_id=0, has_side_effects=True, vmem_limit_bytes=67043328),
        name="fused_step",
    )(x, dy, wg, wu, wd, gain)


def unpack_kernel(blocks_ref, gate_ref, up_ref, down_ref, blocks, gate, up, down, in_sem, out_sem):
    layers, ny, nz, units = blocks.shape[:4]
    nf = units // 3
    pairs, tall = nz // 2, nf // 2 * RS
    count = layers * pairs

    def load(i):
        here = (i // pairs, slice(None), pl.ds(i % pairs * 2, 2))
        return pltpu.make_async_copy(blocks_ref.at[here], blocks.at[here], in_sem.at[i])

    def stores(i):
        for ref, buf, rows in ((gate_ref, gate, RS), (up_ref, up, RS), (down_ref, down, tall)):
            here = (i // pairs, pl.ds(pl.multiple_of(i % pairs * (2 * rows), 2 * rows), 2 * rows))
            yield pltpu.make_async_copy(buf.at[here], ref.at[here], out_sem)

    loop(count, lambda i: load(i).start())

    def move(i):
        load(i).wait()
        l = i // pairs
        for k in BOTH:
            z = i % pairs * 2 + k
            rows = pl.ds(pl.multiple_of(z * RS, RS), RS)
            for y in range(ny):
                for j in range(nf):
                    cols = pl.ds((j * ny + y) * LN, LN)
                    gate[l, rows, cols] = blocks[l, y, z, j]
                    up[l, rows, cols] = blocks[l, y, z, nf + j]
                for j in range(nf):
                    h, r = j // (nf // 2), j % (nf // 2)
                    down[l, pl.ds(pl.multiple_of(z * tall + r * RS, RS), RS), pl.ds((2 * y + h) * LN, LN)] = blocks[l, y, z, 2 * nf + j]
        for copy in stores(i):
            copy.start()
    loop(count, move)
    for buf, ref in ((gate, gate_ref), (up, up_ref), (down, down_ref)):
        pltpu.make_async_copy(buf, ref, out_sem).wait()


def unpack(out, dims):
    layers, ny, nz, nf = dims
    wide, tall = (layers, nz * RS, nf * ny * LN), (layers, nz * nf // 2 * RS, 2 * ny * LN)
    shapes = (wide, wide, tall)
    hbm = pl.BlockSpec(memory_space=pl.ANY)
    return pl.pallas_call(
        unpack_kernel, in_specs=[hbm], out_specs=[hbm] * len(shapes),
        out_shape=[jax.ShapeDtypeStruct(shape, F32) for shape in shapes],
        scratch_shapes=[pltpu.VMEM(out.shape, F32), *[pltpu.VMEM(shape, F32) for shape in shapes],
                        pltpu.SemaphoreType.DMA((layers * nz // 2,)), pltpu.SemaphoreType.DMA],
        compiler_params=pltpu.CompilerParams(vmem_limit_bytes=48 * 2**20),
        name="unpack")(out)


TOKEN_AXES = ("dp", "replica", "fsdp")


def solution(mesh):
    ny, nz, nf = mesh.shape["replica"], mesh.shape["dp"], mesh.shape["fsdp"]
    tok_spec, shard_spec, full_spec = P(TOKEN_AXES, None), P(None, "fsdp", None), P(None, None)

    def device_step(x, dy, wg, wu, wd, gain):
        layers, depth = gain.shape
        dims = (layers, ny, nz, nf)
        out, blocks, gain_sum = fused_step(x, dy, wg, wu, wd, gain, dims + (x.shape[0], depth, wd.shape[1]))
        dw_gate, dw_up, dw_down = unpack(blocks, dims)
        return out, dw_gate, dw_up, dw_down, gain_sum.reshape(gain.shape)

    return jax.shard_map(
        device_step, mesh=mesh, in_specs=(tok_spec, tok_spec, shard_spec, shard_spec, shard_spec, full_spec),
        out_specs=(tok_spec, shard_spec, shard_spec, shard_spec, full_spec), check_vma=False)
```
